256 devices in a mesh: cells: 64 (over z, y, core), grp: 4 (over x).
Axes of the slice: x: 4, y: 4, z: 8, core: 2. Of those that a mesh axis runs over, the one named last changes fastest.
Arguments:
- latent_coordinates: float32 [50, 1048576], P(None, ('cells', 'grp')), may hold values from -40 to 40
- group_means: float32 [128, 50], replicated, may hold values from -4 to 4
- entropy_scaling: float32 [128], replicated, may hold values from 0.5 to 2
- sample_shrinkage_lambda: float32 [200], replicated, may hold values from 1311 to 10485
- sample_population: int32 [200], replicated, may hold values from 1 to 10485, 1048576 in all
Outputs:
- corrected: float32 [50, 1048576], P(None, ('cells', 'grp'))
- new_centroids: float32 [128, 50], P('cells')
The draws below stay inside these ranges and needn't reach their ends.
All inputs are finite; a program needn't handle non-finite values.
Results may differ from the reference program's by a relative error of at most 0.0003.
Values sent between devices are 32-bit elements; how exact they have to be, the bound alone decides.
A program may use at most 64 MiB of HBM per device.

```python
import math
import jax
import jax.numpy as jnp
import numpy as np
from jax import lax

PCS = 50
GROUP_NUMBER = 128
NB = 200
CELLS = 1048576
MOST = 10485


def centre_table(key):
    table = jax.random.normal(jax.random.fold_in(key, 11), (GROUP_NUMBER, PCS), jnp.float32) * 0.5
    return table


def draw_group_means(key, part):
    return jnp.clip(centre_table(key), -4.0, 4.0)


def draw_latent_coordinates(key, part):
    region_len = CELLS // NB
    shifts = jax.random.normal(jax.random.fold_in(key, 2), (PCS, NB + 1), jnp.float32)
    region = jnp.minimum(jnp.arange(CELLS) // region_len, NB)
    offset = shifts[:, region]
    noise = jax.random.normal(jax.random.fold_in(key, 1), (PCS, CELLS), jnp.float32)
    values = noise + offset
    return jnp.clip(values, -40.0, 40.0)


def split_up(count, total, most, skew):
    portions = [(1 << 20) // math.isqrt(rank ** skew) + 1 for rank in range(2, count + 1)]
    rest, given = total - most - (count - 1), [1] * (count - 1)
    while rest > 0:
        movable = [i for i in range(count - 1) if given[i] < most]
        whole, remaining = sum([portions[i] for i in movable]), rest
        for i in movable:
            more = min(most - given[i], max(1, remaining * portions[i] // whole), rest)
            given[i] = given[i] + more
            rest = rest - more
    return np.array([most] + given)


def ragged(rng, count, total, limit, lean):
    if count == 2:
        one = jax.random.randint(rng, (), max(1, total - limit), min(limit, total - 1) + 1)
        return jnp.stack([one, total - one])
    tallies = jnp.asarray(split_up(count, total, limit, lean), jnp.int32)
    twos = (count - 1) // 2
    giver, receiver = tallies[1:1 + 2 * twos:2], tallies[2:2 + 2 * twos:2]
    slack = jnp.minimum(giver - 1, limit - receiver)
    shifted = jax.random.randint(jax.random.fold_in(rng, 1), (twos,), 0, 1 << 20) % (slack + 1)
    tallies = tallies.at[1:1 + 2 * twos:2].set(giver - shifted).at[2:2 + 2 * twos:2].set(receiver + shifted)
    return tallies[jax.random.permutation(jax.random.fold_in(rng, 2), count)]


def setup_inputs(seed: int = 0) -> dict:
    key_list = jax.random.split(jax.random.key(seed), 6)
    latent_coordinates = draw_latent_coordinates(jax.random.fold_in(key_list[5], 71), 0)
    group_means = draw_group_means(jax.random.fold_in(key_list[5], 71), 0)
    entropy_scaling = jnp.clip(jnp.exp(jax.random.uniform(key_list[2], (GROUP_NUMBER,), jnp.float32, math.log(0.5), math.log(2.0))), 0.5, 2.0)
    sample_shrinkage_lambda = jnp.clip(jnp.exp(jax.random.uniform(key_list[3], (NB,), jnp.float32, math.log(1311.0), math.log(10485.0))), 1311.0, 10485.0)
    sample_population = ragged(key_list[4], NB, CELLS, MOST, 2).astype(jnp.int32)
    return {"latent_coordinates": latent_coordinates, "group_means": group_means, "entropy_scaling": entropy_scaling, "sample_shrinkage_lambda": sample_shrinkage_lambda, "sample_population": sample_population}


diversity = 2.0
intercept_ridge = 1.0
highest = lax.Precision.HIGHEST


def observation_affinity(latent_coordinates, group_means, entropy_scaling):
    pairwise_dots = jnp.dot(group_means, latent_coordinates, precision=highest, preferred_element_type=jnp.float32)
    quadratic_lengths = jnp.sum(group_means * group_means, axis=1)
    return (2.0 * pairwise_dots - quadratic_lengths[:, None]) / (2.0 * entropy_scaling[:, None])


def probabilistic_responsibility(group_affinity):
    top = jnp.max(group_affinity, axis=0, keepdims=True)
    raised = jnp.exp(group_affinity - top)
    return raised / jnp.sum(raised, axis=0, keepdims=True)


def reference(latent_coordinates, group_means, entropy_scaling, sample_shrinkage_lambda, sample_population):
    cells_total = latent_coordinates.shape[1]
    batch_ends = jnp.cumsum(sample_population).astype(jnp.int32)
    batch_starts = (batch_ends - sample_population).astype(jnp.int32)
    padded = jnp.pad(latent_coordinates, ((0, 0), (0, MOST)))
    window = lax.iota(jnp.int32, MOST)

    def batch_cells(start, size):
        contiguous_portion = lax.dynamic_slice(padded, (jnp.int32(0), start), (PCS, MOST))
        inside = (window < size).astype(jnp.float32)
        return contiguous_portion, inside

    def count_step(carry, item):
        start, size = item
        contiguous_portion, inside = batch_cells(start, size)
        expected_occupancy = probabilistic_responsibility(observation_affinity(contiguous_portion, group_means, entropy_scaling))
        return carry, jnp.sum(expected_occupancy * inside[None, :], axis=1)

    unused, counts_t = lax.scan(count_step, jnp.float32(0.0), (batch_starts, sample_population))
    counts = counts_t.T
    totals = jnp.sum(counts, axis=1)
    expected = sample_population.astype(jnp.float32)[None, :] * totals[:, None] / jnp.float32(cells_total)
    penalty = diversity * jnp.log((counts + 1.0) / (expected + 1.0))

    def assign_of(contiguous_portion, single_observation):
        return probabilistic_responsibility(observation_affinity(contiguous_portion, group_means, entropy_scaling) - single_observation[:, None])

    def moment_step(carry, item):
        start, size, single_observation = item
        contiguous_portion, inside = batch_cells(start, size)
        assign = assign_of(contiguous_portion, single_observation) * inside[None, :]
        augmented = jnp.concatenate([jnp.ones((1, MOST), jnp.float32), contiguous_portion], axis=0)
        return carry, jnp.einsum("kn,dn->kd", assign, augmented, precision=highest)

    unused, moments_t = lax.scan(moment_step, jnp.float32(0.0), (batch_starts, sample_population, penalty.T))
    moments = jnp.transpose(moments_t, (1, 2, 0))
    mass = moments[:, 0, :]
    sums = moments[:, 1:, :]
    shrink = sample_shrinkage_lambda[None, :] / (mass + sample_shrinkage_lambda[None, :])
    weight = jnp.sum(mass * shrink, axis=1)
    right_side = jnp.sum(sums * shrink[:, None, :], axis=2)
    intercept = right_side / (intercept_ridge + weight)[:, None]
    coefficients = (sums - mass[:, None, :] * intercept[:, :, None]) / (mass + sample_shrinkage_lambda[None, :])[:, None, :]
    new_centroids = jnp.sum(sums, axis=2) / (1.0 + jnp.sum(mass, axis=1))[:, None]

    def correct_step(carry, item):
        start, size, single_observation, coef = item
        contiguous_portion, inside = batch_cells(start, size)
        assign = assign_of(contiguous_portion, single_observation) * inside[None, :]
        moved = jnp.einsum("kd,kn->dn", coef, assign, precision=highest)
        current = lax.dynamic_slice(carry, (jnp.int32(0), start), (PCS, MOST))
        fresh = jnp.where(inside[None, :] > 0.0, contiguous_portion - moved, current)
        return lax.dynamic_update_slice(carry, fresh, (jnp.int32(0), start)), jnp.float32(0.0)

    result, unused = lax.scan(correct_step, padded, (batch_starts, sample_population, penalty.T, jnp.transpose(coefficients, (2, 0, 1))))
    return result[:, :cells_total], new_centroids
```

```python
import functools

import jax
import jax.numpy as jnp
from jax import lax
from jax.experimental import pallas as pl
from jax.experimental.pallas import tpu as pltpu
from jax.sharding import Mesh
from jax.sharding import PartitionSpec as P

CELLS = ("cells_0", "cells_1", "cells_2")
CELLS_GRP = ("cells_0", "cells_1", "cells_2", "grp")


diversity = 2.0
intercept_ridge = 1.0
highest = lax.Precision.HIGHEST


def split_up(array, dim, size):
    dims = array.shape
    parts = array.reshape(*dims[:dim], size, dims[dim] // size, *dims[dim + 1 :])
    return jnp.moveaxis(parts, dim, 0)


def summed_on_arrival(array, axis, dim):
    size = lax.axis_size(axis)
    parts = lax.all_to_all(split_up(array, dim, size), axis, 0, 0, tiled=True)
    return jnp.sum(parts, axis=0)


def sum_in_two_steps(array, axes, dim):
    far, near = axes
    parts = split_up(array, dim, lax.axis_size(far))
    nearer = summed_on_arrival(parts, near, dim + 1)
    arrived = lax.all_to_all(nearer, far, split_axis=0, concat_axis=0, tiled=True)
    return arrived.sum(axis=0)


def filled_up(lines, size):
    spare = -len(lines) % size
    return jnp.pad(lines, [(0, spare)] + [(0, 0)] * (lines.ndim - 1))


def sent_to_all(array, axis):
    size = lax.axis_size(axis)
    return lax.all_to_all(
        jnp.broadcast_to(array[None], (size, *array.shape)), axis, 0, 0, tiled=True
    )


def joined_along(parts, dim):
    parts = jnp.moveaxis(parts, 0, dim)
    dims = parts.shape
    return parts.reshape(*dims[:dim], dims[dim] * dims[dim + 1], *dims[dim + 2 :])


def gather_axes(array, axes, dim):
    far, near = axes
    leading = sent_to_all(array, far)
    parts = jnp.swapaxes(sent_to_all(leading, near), 0, 1)
    return joined_along(parts.reshape(-1, *array.shape), dim)


def total_of(array, axes):
    lines = array.reshape(-1)
    own = sum_in_two_steps(
        filled_up(lines, lax.axis_size(axes[0]) * lax.axis_size(axes[1])), axes, 0
    )
    whole = gather_axes(own, axes, 0)
    return whole[: len(lines)].reshape(array.shape)


def from_behind(block, axis, distance):
    devices = range(lax.axis_size(axis))
    route = [(i - distance, i) for i in devices if i - distance in devices]
    return lax.ppermute(block, axis, route)


def by_axis(array, axes):
    return functools.reduce(lax.psum, axes, array)


def observation_affinity(latent_coordinates, group_means, entropy_scaling):
    pairwise_dots = jnp.dot(
        group_means, latent_coordinates, precision=highest, preferred_element_type=jnp.float32
    )
    quadratic_lengths = jnp.sum(group_means * group_means, axis=1)
    return (2.0 * pairwise_dots - quadratic_lengths[:, None]) / (2.0 * entropy_scaling[:, None])


def probabilistic_responsibility(group_affinity):
    top = jnp.max(group_affinity, axis=0, keepdims=True)
    raised = jnp.exp(group_affinity - top)
    return raised / jnp.sum(raised, axis=0, keepdims=True)


def batch_parts(moments, ridge):
    mass = moments[:, 0, :]
    sums = moments[:, 1:, :]
    shrink = ridge[None, :] / (mass + ridge[None, :])
    weight = jnp.sum(mass * shrink, axis=1)
    right_side = jnp.sum(sums * shrink[:, None, :], axis=2)
    return (weight, right_side, jnp.sum(mass, axis=1), jnp.sum(sums, axis=2))


def slopes_of(moments, ridge, weight, right_side):
    mass = moments[:, 0, :]
    sums = moments[:, 1:, :]
    intercept = right_side / (intercept_ridge + weight)[:, None]
    return (sums - mass[:, None, :] * intercept[:, :, None]) / (mass + ridge[None, :])[:, None, :]


def wide_body(
    latent_coordinates, group_means, entropy_scaling, sample_shrinkage_lambda, sample_population
):
    local_cells = latent_coordinates.shape[1]
    num_pcs = latent_coordinates.shape[0]
    clusters = group_means.shape[0]
    batches = sample_population.shape[0]
    owned = clusters // lax.axis_size(CELLS)
    offset = (lax.axis_index(CELLS) * lax.axis_size("grp") + lax.axis_index("grp")) * local_cells
    batch_ends = jnp.cumsum(sample_population)
    batch_starts = batch_ends - sample_population
    cells_total = jnp.sum(sample_population).astype(jnp.float32)
    position = offset + lax.iota(jnp.int32, local_cells)
    batch_of = jnp.sum((batch_ends[:, None] <= position[None, :]).astype(jnp.int32), axis=0)
    first_batch = batch_of[0]
    last_batch = batch_of[local_cells - 1]
    group_affinity = observation_affinity(latent_coordinates, group_means, entropy_scaling)
    expected_occupancy = probabilistic_responsibility(group_affinity)

    def count_step(batch_id, running):
        in_batch = (batch_of == batch_id).astype(jnp.float32)
        single_observation = jnp.dot(
            expected_occupancy, in_batch, precision=highest, preferred_element_type=jnp.float32
        )
        return lax.dynamic_update_slice(
            running, single_observation[:, None], (jnp.int32(0), batch_id)
        )

    counts = lax.fori_loop(
        first_batch, last_batch + 1, count_step, jnp.zeros((clusters, batches), jnp.float32)
    )
    counts = total_of(counts, (("cells_0", "cells_1"), ("cells_2", "grp")))
    totals = jnp.sum(counts, axis=1)
    expected = sample_population.astype(jnp.float32)[None, :] * totals[:, None] / cells_total
    penalty = diversity * jnp.log((counts + 1.0) / (expected + 1.0))

    def penalty_step(batch_id, running):
        in_batch = (batch_of == batch_id).astype(jnp.float32)
        column = lax.dynamic_index_in_dim(penalty, batch_id, 1, keepdims=True)
        return running + column * in_batch[None, :]

    cell_penalty = lax.fori_loop(
        first_batch, last_batch + 1, penalty_step, jnp.zeros((clusters, local_cells), jnp.float32)
    )
    assign = probabilistic_responsibility(group_affinity - cell_penalty)
    augmented = jnp.concatenate(
        [jnp.ones((1, local_cells), jnp.float32), latent_coordinates], axis=0
    )

    def moment_step(batch_id, running):
        in_batch = (batch_of == batch_id).astype(jnp.float32)
        contiguous_portion = jnp.einsum(
            "kn,dn->kd", assign * in_batch[None, :], augmented, precision=highest
        )
        return lax.dynamic_update_slice(
            running, contiguous_portion[:, :, None], (jnp.int32(0), jnp.int32(0), batch_id)
        )

    moments = lax.fori_loop(
        first_batch,
        last_batch + 1,
        moment_step,
        jnp.zeros((clusters, num_pcs + 1, batches), jnp.float32),
    )
    devices_flat = lax.axis_size(CELLS) * lax.axis_size("grp")
    most_cells = 2 * local_cells * devices_flat // batches
    reach = (most_cells - 2) // local_cells + 1
    begins_here = (batch_starts >= offset) & (batch_starts < offset + local_cells)
    owner_mask = begins_here.astype(jnp.float32)
    head_owned = begins_here[first_batch]
    head_column = lax.dynamic_index_in_dim(moments, first_batch, 2, keepdims=False)
    sent_stats = jnp.where(head_owned, 0.0, 1.0) * head_column
    sent_tag = jnp.where(head_owned, 0.0, first_batch.astype(jnp.float32) + 1.0) * jnp.ones(
        (1,), jnp.float32
    )
    completed = moments
    for hop in range(1, reach + 1):
        got_stats, got_tag = from_behind((sent_stats, sent_tag), CELLS_GRP, -hop)
        got_id = jnp.maximum(got_tag[0].astype(jnp.int32) - 1, 0)
        accept = jnp.where((got_tag[0] > 0.5) & begins_here[got_id], 1.0, 0.0)
        single_observation = (
            lax.dynamic_index_in_dim(completed, got_id, 2, keepdims=False) + accept * got_stats
        )
        completed = lax.dynamic_update_slice(
            completed, single_observation[:, :, None], (jnp.int32(0), jnp.int32(0), got_id)
        )
    completed = completed * owner_mask[None, None, :]
    weight, right_side, mass_total, moment_total = jax.tree.map(
        lambda part: by_axis(part, CELLS_GRP), batch_parts(completed, sample_shrinkage_lambda)
    )
    coefficients = slopes_of(completed, sample_shrinkage_lambda, weight, right_side)
    every_centroid = moment_total / (1.0 + mass_total)[:, None]
    new_centroids = lax.dynamic_slice_in_dim(
        every_centroid, lax.axis_index(CELLS) * owned, owned, 0
    )
    tail_owned = begins_here[last_batch]
    tail_column = lax.dynamic_index_in_dim(coefficients, last_batch, 2, keepdims=False)
    tail_send = jnp.where(tail_owned, 1.0, 0.0) * tail_column
    tail_tag = jnp.where(tail_owned, last_batch.astype(jnp.float32) + 1.0, 0.0) * jnp.ones(
        (1,), jnp.float32
    )
    head_fix = jnp.zeros_like(tail_column)
    for hop in range(1, reach + 1):
        got_coef, got_tag = from_behind((tail_send, tail_tag), CELLS_GRP, hop)
        match = got_tag[0] == first_batch.astype(jnp.float32) + 1.0
        head_fix = jnp.where(match, got_coef, head_fix)
    own_head = lax.dynamic_index_in_dim(coefficients, first_batch, 2, keepdims=False)
    head_final = jnp.where(head_owned, own_head, head_fix)
    coefficients = lax.dynamic_update_slice(
        coefficients, head_final[:, :, None], (jnp.int32(0), jnp.int32(0), first_batch)
    )

    def correct_step(batch_id, running):
        in_batch = (batch_of == batch_id).astype(jnp.float32)
        slope_table = lax.dynamic_index_in_dim(coefficients, batch_id, 2, keepdims=False)
        moved = jnp.einsum("kd,kn->dn", slope_table, assign * in_batch[None, :], precision=highest)
        return running - moved

    corrected = lax.fori_loop(first_batch, last_batch + 1, correct_step, latent_coordinates)
    return (latent_coordinates - corrected, new_centroids)


SLOTS = 8
ROWS = 64
MOST = 10485
MESH = pl.DeviceIdType.MESH
bf16, f32 = jnp.bfloat16, jnp.float32


def two_pieces(value):
    first = value.astype(bf16)
    return first, (value - first.astype(f32)).astype(bf16)


def across(left, right):
    return lax.dot_general(left, right, (((1,), (1,)), ((), ())), preferred_element_type=f32)


def plain(left, right):
    return jnp.dot(left, right, preferred_element_type=f32)


def step_kernel(
    shape,
    cells_all,
    z_hbm,
    means_ref,
    soft_ref,
    ridge_ref,
    pop_ref,
    moved_ref,
    cent_ref,
    zf,
    zc,
    ex,
    pair,
    means_wide,
    acc,
    slopes,
    near_out,
    near_counts,
    near_mass,
    near_moments,
    ends_out,
    line_a,
    line_b,
    sums_out,
    sum_in,
    cent_out,
    cent_in,
    tile_out,
    tile_in,
    full_sums,
    load_sems,
    send_sems,
    recv_sems,
):
    nz, ny, nc, nx = shape
    near = nc * nx
    far = nz * ny
    count = near * far
    cells = zf.shape[1]
    pcs = means_ref.shape[1]
    clusters = means_ref.shape[0]
    batches = pop_ref.shape[1]
    rows_each = ROWS // near
    reach = (MOST - 2) // cells + 1
    offsets = [h for h in range(-reach, reach + 1) if h]
    me = (
        (lax.axis_index("cells_0") * ny + lax.axis_index("cells_1")) * nc
        + lax.axis_index("cells_2")
    ) * nx + lax.axis_index("grp")
    rank = lax.rem(me, near)
    block = lax.div(me, near)

    def place(q):
        return (
            lax.div(q, ny * nc * nx),
            lax.rem(lax.div(q, nc * nx), ny),
            lax.rem(lax.div(q, nx), nc),
            lax.rem(q, nx),
        )

    def mate(r):
        return block * near + lax.rem(rank + r, near)

    def peer(r):
        return lax.rem(block + r, far) * near + rank

    def neighbour(h):
        return lax.rem(me + (h + count), count)

    def push(src, dst, which, q):
        pltpu.make_async_remote_copy(
            src_ref=src,
            dst_ref=dst,
            send_sem=send_sems.at[which],
            recv_sem=recv_sems.at[which],
            device_id=place(q),
            device_id_type=MESH,
        ).start()

    def arrived(buffer, which):
        pltpu.make_async_copy(buffer, buffer, recv_sems.at[which]).wait()

    def left(buffer, which):
        pltpu.make_async_copy(buffer, buffer, send_sems.at[which]).wait()

    barrier = pltpu.get_barrier_semaphore()
    for r in range(1, near):
        pl.semaphore_signal(barrier, inc=1, device_id=place(mate(r)), device_id_type=MESH)
    for h in offsets:
        pl.semaphore_signal(barrier, inc=1, device_id=place(neighbour(h)), device_id_type=MESH)

    def greet(r, carry):
        pl.semaphore_signal(barrier, inc=1, device_id=place(peer(r)), device_id_type=MESH)
        return carry

    lax.fori_loop(1, far, greet, 0)

    loads = load_sems.shape[0]
    part = cells // loads
    for i in range(loads):
        columns = pl.ds(i * part, part)
        pltpu.make_async_copy(z_hbm.at[:, columns], zf.at[:, columns], load_sems.at[i]).start()

    means_wide[...] = jnp.zeros_like(means_wide)
    means_wide[:, 0:pcs] = means_ref[...]
    g = means_wide[...]
    square = lax.broadcasted_iota(jnp.int32, (clusters, clusters), 0)
    lane = lax.broadcasted_iota(jnp.int32, (clusters, clusters), 1)
    soft = jnp.sum(jnp.where(square == lane, soft_ref[...], 0.0), axis=1, keepdims=True)
    offset_of = -0.5 * jnp.sum(g * g, axis=1, keepdims=True) / soft
    weights = jnp.where(lane == pcs, offset_of, g / soft)
    w1 = weights.astype(bf16).astype(f32)
    w2 = (weights - w1).astype(bf16).astype(f32)
    o1 = offset_of.astype(bf16).astype(f32)
    o2 = (offset_of - o1).astype(bf16).astype(f32)
    w1 = jnp.where(lane == pcs + 1, offset_of - o1 - o2, w1)
    w1 = (w1 + pltpu.roll(w1, ROWS, 1)).astype(bf16)
    w2 = (w2 + pltpu.roll(w2, ROWS, 1)).astype(bf16)
    weights = jnp.concatenate([w1, w2], axis=1)

    pop = pop_ref[...].astype(f32)
    up = lax.broadcasted_iota(jnp.int32, (batches, batches), 0)
    down = lax.broadcasted_iota(jnp.int32, (batches, batches), 1)
    ends = jnp.dot(
        jnp.broadcast_to(pop, (8, batches)),
        (up <= down).astype(f32),
        precision=highest,
        preferred_element_type=f32,
    )[0:1]
    half = lax.broadcasted_iota(jnp.int32, (16, 1), 0)
    device = me + lax.rem(half, 8) - reach
    limit = device * cells + jnp.where(half >= 8, cells - 1, 0)
    spot = jnp.sum((ends <= limit.astype(f32)).astype(f32), axis=1, keepdims=True)
    spot = jnp.where(device < 0, -9.0, spot)
    first = {h: spot[h + reach : h + reach + 1] for h in offsets + [0]}
    last = {h: spot[8 + h + reach : 9 + h + reach] for h in offsets + [0]}
    slot = lax.broadcasted_iota(jnp.int32, (SLOTS, 1), 0).astype(f32)
    batch_id = first[0] + slot
    chosen = lax.broadcasted_iota(jnp.int32, (SLOTS, batches), 1).astype(f32) == batch_id
    held = jnp.sum(jnp.where(chosen, pop, 0.0), axis=1, keepdims=True)
    ridge = jnp.sum(jnp.where(chosen, ridge_ref[...], 0.0), axis=1, keepdims=True)
    ridge = jnp.where(batch_id < batches, ridge, 1.0)
    stop = jnp.sum(jnp.where(chosen, ends, 0.0), axis=1, keepdims=True) - (me * cells).astype(f32)
    start = stop - held
    tail = slot == last[0] - first[0]
    head = slot == 0.0
    behind = {h: (last[h] == first[0]).astype(f32) for h in offsets if h < 0}
    ahead = {h: (first[h] == last[0]).astype(f32) for h in offsets if h > 0}

    def inside(c, width, times):
        position = (
            lax.broadcasted_iota(jnp.int32, (SLOTS * times, width), 1) + c * width
        ).astype(f32)
        low = jnp.concatenate([start] * times, axis=0)
        high = jnp.concatenate([stop] * times, axis=0)
        return ((position >= low) & (position < high)).astype(f32)

    def completed(own, buffer, tail_row):
        before = jnp.zeros((1, clusters), f32)
        after = jnp.zeros((1, clusters), f32)
        for i, h in enumerate(offsets):
            if h < 0:
                before = before + behind[h] * buffer[i, 1:2, :]
            else:
                after = after + ahead[h] * buffer[i, 0:1, :]
        return own + jnp.where(head, before, 0.0) + jnp.where(tail, after, 0.0)

    def rows_of(*lines):
        row = lax.broadcasted_iota(jnp.int32, (8, clusters), 0)
        value = jnp.zeros((8, clusters), f32)
        for i, line in enumerate(lines):
            value = jnp.where(row == i, line, value)
        return value

    width = 512
    per_load = part // width

    for i in range(loads):
        columns = pl.ds(i * part, part)
        pltpu.make_async_copy(z_hbm.at[:, columns], zf.at[:, columns], load_sems.at[i]).wait()

    def prior_step(c, total):
        columns = pl.ds(pl.multiple_of(c * width, width), width)
        z1, z2 = two_pieces(
            jnp.concatenate(
                [
                    zf[:, columns],
                    jnp.ones((2, width), f32),
                    jnp.zeros((ROWS - 2 - pcs, width), f32),
                ],
                axis=0,
            )
        )
        zc[0:ROWS, columns] = z1
        zc[ROWS : 2 * ROWS, columns] = z2
        score = plain(weights, jnp.concatenate([z1, z2, z1, z2], axis=0))
        raised = jnp.exp(score - jnp.max(score, axis=0, keepdims=True))
        ex[:, columns] = raised
        p1, p2 = two_pieces(raised * (1.0 / jnp.sum(raised, axis=0, keepdims=True)))
        mask = inside(c, width, 2).astype(bf16)
        return total + across(mask, jnp.concatenate([p1, p2], axis=0))

    total = lax.fori_loop(
        0, cells // width, prior_step, jnp.zeros((2 * SLOTS, 2 * clusters), f32)
    )
    counts = total[0:SLOTS, 0:clusters] + total[0:SLOTS, clusters : 2 * clusters]
    own_total = jnp.sum(counts, axis=0, keepdims=True)
    near_out[0] = rows_of(
        counts[0:1], jnp.sum(jnp.where(tail, counts, 0.0), axis=0, keepdims=True), own_total
    )
    pl.semaphore_wait(barrier, near - 1 + far - 1 + len(offsets))
    for r in range(1, near):
        push(near_out.at[0], line_a.at[r - 1], 0, mate(r))
    for i, h in enumerate(offsets):
        push(near_out.at[0], near_counts.at[len(offsets) - 1 - i], 1, neighbour(h))
    arrived(line_a, 0)
    block_total = own_total
    for r in range(near - 1):
        block_total = block_total + line_a[r, 2:3, :]
    tile_out[0] = jnp.broadcast_to(block_total, (8, clusters))

    def send_line(r, carry):
        push(tile_out.at[0], line_b.at[r - 1], 2, peer(r))
        return carry

    lax.fori_loop(1, far, send_line, 0)
    arrived(near_counts, 1)
    full_counts = completed(counts, near_counts, 1)
    arrived(line_b, 2)
    totals = block_total + jnp.sum(line_b[...], axis=0)[0:1]
    expected = held * totals * (1.0 / cells_all)
    ratio = (expected + 1.0) / (full_counts + 1.0)
    factor = ratio * ratio
    f1 = factor.astype(bf16).astype(f32)
    f2 = (factor - f1).astype(bf16).astype(f32)
    f3 = factor - f1 - f2
    factor = jnp.concatenate([f1, f2, f3, jnp.zeros_like(f3)], axis=0).T.astype(bf16)

    acc[...] = jnp.zeros_like(acc)

    def moment_step(c, carry):
        columns = pl.ds(pl.multiple_of(c * width, width), width)
        mask = inside(c, width, 4).astype(bf16)
        weighed = ex[:, columns] * plain(factor, mask)
        a1, a2 = two_pieces(weighed * (1.0 / jnp.sum(weighed, axis=0, keepdims=True)))
        pair[0:clusters, columns] = a1
        pair[clusters : 2 * clusters, columns] = a2
        z = zc[:, columns]
        both = jnp.concatenate([a1, a2], axis=0)
        lined = jnp.concatenate([z * mask[s : s + 1, :] for s in range(SLOTS)], axis=0)
        acc[...] += across(lined, both)
        return carry

    lax.fori_loop(0, cells // width, moment_step, 0)
    moments = []
    for s in range(SLOTS):
        top = acc[2 * ROWS * s : 2 * ROWS * s + ROWS, :]
        low = acc[2 * ROWS * s + ROWS : 2 * ROWS * (s + 1), :]
        moments.append(
            top[:, 0:clusters] + top[:, clusters:] + low[:, 0:clusters] + low[:, clusters:]
        )
    mass = rows_of(*[moments[s][pcs : pcs + 1] for s in range(SLOTS)])
    near_out[1] = rows_of(
        mass[0:1], jnp.sum(jnp.where(tail, mass, 0.0), axis=0, keepdims=True)
    )
    for i, h in enumerate(offsets):
        push(near_out.at[1], near_mass.at[len(offsets) - 1 - i], 3, neighbour(h))
    whole = moments[0]
    tail_moment = moments[0] * tail[0:1].astype(f32)
    for s in range(1, SLOTS):
        whole = whole + moments[s]
        tail_moment = tail_moment + moments[s] * tail[s : s + 1].astype(f32)
    ends_out[0] = moments[0][0:56]
    ends_out[1] = tail_moment[0:56]
    for t in range(near):
        cent_out[t] = whole[t * rows_each : (t + 1) * rows_each]
    for r in range(1, near):
        push(cent_out.at[lax.rem(rank + r, near)], cent_in.at[r - 1], 4, mate(r))
    arrived(near_mass, 3)
    full_mass = completed(mass, near_mass, 1)
    shrink = ridge / (full_mass + ridge)
    right = moments[0] * shrink[0:1]
    for s in range(1, SLOTS):
        right = right + moments[s] * shrink[s : s + 1]
    for t in range(near):
        sums_out[t] = right[t * rows_each : (t + 1) * rows_each]
    for r in range(1, near):
        push(sums_out.at[lax.rem(rank + r, near)], sum_in.at[r - 1], 5, mate(r))
    for i, h in enumerate(offsets):
        push(ends_out.at[int(h > 0)], near_moments.at[len(offsets) - 1 - i], 6, neighbour(h))
    arrived(cent_in, 4)
    cent_tile = cent_out[rank]
    for r in range(near - 1):
        cent_tile = cent_tile + cent_in[r]
    tile_out[1] = cent_tile
    arrived(sum_in, 5)
    sum_tile = sums_out[rank]
    for r in range(near - 1):
        sum_tile = sum_tile + sum_in[r]
    tile_out[2] = sum_tile

    def send_sum(r, carry):
        push(tile_out.at[2], tile_in.at[1, r - 1], 8, peer(r))
        return carry

    def send_cent(r, carry):
        push(tile_out.at[1], tile_in.at[0, r - 1], 7, peer(r))
        return carry

    lax.fori_loop(1, far, send_sum, 0)
    lax.fori_loop(1, far, send_cent, 0)

    arrived(near_moments, 6)
    before = jnp.zeros((56, clusters), f32)
    after = jnp.zeros((56, clusters), f32)
    for i, h in enumerate(offsets):
        if h < 0:
            before = before + behind[h] * near_moments[i]
        else:
            after = after + ahead[h] * near_moments[i]

    arrived(tile_in.at[1], 8)
    full_sums[1, 0] = sum_tile + jnp.sum(tile_in[1], axis=0)
    for r in range(1, near):
        push(full_sums.at[1, 0], full_sums.at[1, r], 10, mate(r))
    arrived(tile_in.at[0], 7)
    full_sums[0, 0] = cent_tile + jnp.sum(tile_in[0], axis=0)
    for r in range(1, near):
        push(full_sums.at[0, 0], full_sums.at[0, r], 9, mate(r))

    def gathered(which):
        return jnp.concatenate(
            [full_sums[which, lax.rem(rank + (near - t), near)] for t in range(near)], axis=0
        )

    arrived(full_sums.at[1, pl.ds(1, near - 1)], 10)
    right = gathered(1)
    intercept = (right / (1.0 + right[pcs : pcs + 1]))[0:56]
    for s in range(SLOTS):
        moment = moments[s][0:56] + after * tail[s : s + 1].astype(f32)
        if s == 0:
            moment = moment + before
        line = full_mass[s : s + 1]
        slope = (moment - line * intercept) / (line + ridge[s : s + 1])
        c1, c2 = two_pieces(jnp.concatenate([slope, jnp.zeros((8, clusters), f32)], axis=0))
        slopes[ROWS * s : ROWS * (s + 1), :] = jnp.concatenate([c1, c1, c2], axis=1)

    def moved_step(c, carry):
        columns = pl.ds(pl.multiple_of(c * width, width), width)
        both = pair[:, columns]
        every = plain(slopes[...], jnp.concatenate([both, both[0:clusters]], axis=0))
        mask = inside(c, width, 1)
        moved = every[0:ROWS] * mask[0:1]
        for s in range(1, SLOTS):
            moved = moved + every[ROWS * s : ROWS * (s + 1)] * mask[s : s + 1]
        moved_ref[:, columns] = moved[0:pcs]
        return carry

    lax.fori_loop(0, cells // width, moved_step, 0)

    arrived(full_sums.at[0, pl.ds(1, near - 1)], 9)
    centre = gathered(0)
    centre = (centre / (1.0 + centre[pcs : pcs + 1])).T
    owned = cent_ref.shape[0]
    cells_at = lax.div(me, nx)
    row = lax.broadcasted_iota(jnp.int32, (clusters, ROWS), 0)
    for j in range(owned):
        line = jnp.sum(jnp.where(row == cells_at * owned + j, centre, 0.0), axis=0, keepdims=True)
        cent_ref[j : j + 1, :] = line[:, 0:pcs]

    left(line_a, 0)
    left(near_counts, 1)
    left(line_b, 2)
    left(near_mass, 3)
    left(cent_in, 4)
    left(sum_in, 5)
    left(near_moments, 6)
    left(tile_in.at[0], 7)
    left(tile_in.at[1], 8)
    left(full_sums.at[0, pl.ds(1, near - 1)], 9)
    left(full_sums.at[1, pl.ds(1, near - 1)], 10)


def narrow_body(
    shape, latent_coordinates, group_means, entropy_scaling, sample_shrinkage_lambda, sample_population
):
    pcs, cells = latent_coordinates.shape
    clusters = group_means.shape[0]
    batches = sample_population.shape[0]
    nz, ny, nc, nx = shape
    near, far = nc * nx, nz * ny
    rows_each = ROWS // near
    reach = (MOST - 2) // cells + 1
    owned = clusters // (nz * ny * nc)
    vmem = pl.BlockSpec(memory_space=pltpu.VMEM)
    scratch = [
        pltpu.VMEM((pcs, cells), f32),
        pltpu.VMEM((2 * ROWS, cells), bf16),
        pltpu.VMEM((clusters, cells), f32),
        pltpu.VMEM((2 * clusters, cells), bf16),
        pltpu.VMEM((clusters, clusters), f32),
        pltpu.VMEM((SLOTS * 2 * ROWS, 2 * clusters), f32),
        pltpu.VMEM((SLOTS * ROWS, 3 * clusters), bf16),
        pltpu.VMEM((2, 8, clusters), f32),
        pltpu.VMEM((2 * reach, 8, clusters), f32),
        pltpu.VMEM((2 * reach, 8, clusters), f32),
        pltpu.VMEM((2 * reach, 56, clusters), f32),
        pltpu.VMEM((2, 56, clusters), f32),
        pltpu.VMEM((near - 1, 8, clusters), f32),
        pltpu.VMEM((far - 1, 8, clusters), f32),
        pltpu.VMEM((near, rows_each, clusters), f32),
        pltpu.VMEM((near - 1, rows_each, clusters), f32),
        pltpu.VMEM((near, rows_each, clusters), f32),
        pltpu.VMEM((near - 1, rows_each, clusters), f32),
        pltpu.VMEM((3, rows_each, clusters), f32),
        pltpu.VMEM((2, far - 1, rows_each, clusters), f32),
        pltpu.VMEM((2, near, rows_each, clusters), f32),
        pltpu.SemaphoreType.DMA((4,)),
        pltpu.SemaphoreType.DMA((11,)),
        pltpu.SemaphoreType.DMA((11,)),
    ]
    return pl.pallas_call(
        functools.partial(step_kernel, shape, float(cells * near * far)),
        out_shape=(
            jax.ShapeDtypeStruct((pcs, cells), f32),
            jax.ShapeDtypeStruct((owned, pcs), f32),
        ),
        in_specs=[pl.BlockSpec(memory_space=pl.ANY)] + [vmem] * 4,
        out_specs=(vmem, vmem),
        scratch_shapes=scratch,
        compiler_params=pltpu.CompilerParams(
            collective_id=0, has_side_effects=True, vmem_limit_bytes=40 * 1024 * 1024
        ),
    )(
        latent_coordinates,
        group_means,
        entropy_scaling.reshape(1, clusters),
        sample_shrinkage_lambda.reshape(1, batches),
        sample_population.reshape(1, batches),
    )


def body(
    shape, latent_coordinates, group_means, entropy_scaling, sample_shrinkage_lambda, sample_population
):
    cells = latent_coordinates.shape[1]
    batches = sample_population.shape[0]
    inner = SLOTS - 1
    window = sample_population[: batches - inner + 1]
    for i in range(1, inner):
        window = window + sample_population[i : batches - inner + 1 + i]
    few = jnp.min(window) >= cells - 1
    moved, new_centroids = lax.cond(
        few,
        functools.partial(narrow_body, shape),
        wide_body,
        latent_coordinates,
        group_means,
        entropy_scaling,
        sample_shrinkage_lambda,
        sample_population,
    )
    return (latent_coordinates - moved, new_centroids)


def solution(mesh):
    shape = (mesh.shape["cells"] // 8, 4, 2, mesh.shape["grp"])
    finer = Mesh(mesh.devices.reshape(shape), ("cells_0", "cells_1", "cells_2", "grp"))
    return jax.shard_map(
        functools.partial(body, shape),
        mesh=finer,
        in_specs=(P(None, CELLS_GRP), P(), P(), P(), P()),
        out_specs=(P(None, CELLS_GRP), P(CELLS, None)),
        check_vma=False,
    )
```

```python
import functools

import jax
import jax.numpy as jnp
from jax import lax
from jax.experimental import pallas as pl
from jax.experimental.pallas import tpu as pltpu
from jax.sharding import Mesh
from jax.sharding import PartitionSpec as P

CELLS = ("cells_0", "cells_1", "cells_2")
CELLS_GRP = ("cells_0", "cells_1", "cells_2", "grp")


diversity = 2.0
intercept_ridge = 1.0
highest = lax.Precision.HIGHEST


def split_up(array, dim, size):
    dims = array.shape
    parts = array.reshape(*dims[:dim], size, dims[dim] // size, *dims[dim + 1 :])
    return jnp.moveaxis(parts, dim, 0)


def summed_on_arrival(array, axis, dim):
    size = lax.axis_size(axis)
    parts = lax.all_to_all(split_up(array, dim, size), axis, 0, 0, tiled=True)
    return jnp.sum(parts, axis=0)


def sum_in_two_steps(array, axes, dim):
    far, near = axes
    parts = split_up(array, dim, lax.axis_size(far))
    nearer = summed_on_arrival(parts, near, dim + 1)
    arrived = lax.all_to_all(nearer, far, split_axis=0, concat_axis=0, tiled=True)
    return arrived.sum(axis=0)


def filled_up(lines, size):
    spare = -len(lines) % size
    return jnp.pad(lines, [(0, spare)] + [(0, 0)] * (lines.ndim - 1))


def sent_to_all(array, axis):
    size = lax.axis_size(axis)
    return lax.all_to_all(
        jnp.broadcast_to(array[None], (size, *array.shape)), axis, 0, 0, tiled=True
    )


def joined_along(parts, dim):
    parts = jnp.moveaxis(parts, 0, dim)
    dims = parts.shape
    return parts.reshape(*dims[:dim], dims[dim] * dims[dim + 1], *dims[dim + 2 :])


def gather_axes(array, axes, dim):
    far, near = axes
    leading = sent_to_all(array, far)
    parts = jnp.swapaxes(sent_to_all(leading, near), 0, 1)
    return joined_along(parts.reshape(-1, *array.shape), dim)


def total_of(array, axes):
    lines = array.reshape(-1)
    own = sum_in_two_steps(
        filled_up(lines, lax.axis_size(axes[0]) * lax.axis_size(axes[1])), axes, 0
    )
    whole = gather_axes(own, axes, 0)
    return whole[: len(lines)].reshape(array.shape)


def from_behind(block, axis, distance):
    devices = range(lax.axis_size(axis))
    route = [(i - distance, i) for i in devices if i - distance in devices]
    return lax.ppermute(block, axis, route)


def by_axis(array, axes):
    return functools.reduce(lax.psum, axes, array)


def observation_affinity(latent_coordinates, group_means, entropy_scaling):
    pairwise_dots = jnp.dot(
        group_means, latent_coordinates, precision=highest, preferred_element_type=jnp.float32
    )
    quadratic_lengths = jnp.sum(group_means * group_means, axis=1)
    return (2.0 * pairwise_dots - quadratic_lengths[:, None]) / (2.0 * entropy_scaling[:, None])


def probabilistic_responsibility(group_affinity):
    top = jnp.max(group_affinity, axis=0, keepdims=True)
    raised = jnp.exp(group_affinity - top)
    return raised / jnp.sum(raised, axis=0, keepdims=True)


def batch_parts(moments, ridge):
    mass = moments[:, 0, :]
    sums = moments[:, 1:, :]
    shrink = ridge[None, :] / (mass + ridge[None, :])
    weight = jnp.sum(mass * shrink, axis=1)
    right_side = jnp.sum(sums * shrink[:, None, :], axis=2)
    return (weight, right_side, jnp.sum(mass, axis=1), jnp.sum(sums, axis=2))


def slopes_of(moments, ridge, weight, right_side):
    mass = moments[:, 0, :]
    sums = moments[:, 1:, :]
    intercept = right_side / (intercept_ridge + weight)[:, None]
    return (sums - mass[:, None, :] * intercept[:, :, None]) / (mass + ridge[None, :])[:, None, :]


def wide_body(
    latent_coordinates, group_means, entropy_scaling, sample_shrinkage_lambda, sample_population
):
    local_cells = latent_coordinates.shape[1]
    num_pcs = latent_coordinates.shape[0]
    clusters = group_means.shape[0]
    batches = sample_population.shape[0]
    owned = clusters // lax.axis_size(CELLS)
    offset = (lax.axis_index(CELLS) * lax.axis_size("grp") + lax.axis_index("grp")) * local_cells
    batch_ends = jnp.cumsum(sample_population)
    batch_starts = batch_ends - sample_population
    cells_total = jnp.sum(sample_population).astype(jnp.float32)
    position = offset + lax.iota(jnp.int32, local_cells)
    batch_of = jnp.sum((batch_ends[:, None] <= position[None, :]).astype(jnp.int32), axis=0)
    first_batch = batch_of[0]
    last_batch = batch_of[local_cells - 1]
    group_affinity = observation_affinity(latent_coordinates, group_means, entropy_scaling)
    expected_occupancy = probabilistic_responsibility(group_affinity)

    def count_step(batch_id, running):
        in_batch = (batch_of == batch_id).astype(jnp.float32)
        single_observation = jnp.dot(
            expected_occupancy, in_batch, precision=highest, preferred_element_type=jnp.float32
        )
        return lax.dynamic_update_slice(
            running, single_observation[:, None], (jnp.int32(0), batch_id)
        )

    counts = lax.fori_loop(
        first_batch, last_batch + 1, count_step, jnp.zeros((clusters, batches), jnp.float32)
    )
    counts = total_of(counts, (("cells_0", "cells_1"), ("cells_2", "grp")))
    totals = jnp.sum(counts, axis=1)
    expected = sample_population.astype(jnp.float32)[None, :] * totals[:, None] / cells_total
    penalty = diversity * jnp.log((counts + 1.0) / (expected + 1.0))

    def penalty_step(batch_id, running):
        in_batch = (batch_of == batch_id).astype(jnp.float32)
        column = lax.dynamic_index_in_dim(penalty, batch_id, 1, keepdims=True)
        return running + column * in_batch[None, :]

    cell_penalty = lax.fori_loop(
        first_batch, last_batch + 1, penalty_step, jnp.zeros((clusters, local_cells), jnp.float32)
    )
    assign = probabilistic_responsibility(group_affinity - cell_penalty)
    augmented = jnp.concatenate(
        [jnp.ones((1, local_cells), jnp.float32), latent_coordinates], axis=0
    )

    def moment_step(batch_id, running):
        in_batch = (batch_of == batch_id).astype(jnp.float32)
        contiguous_portion = jnp.einsum(
            "kn,dn->kd", assign * in_batch[None, :], augmented, precision=highest
        )
        return lax.dynamic_update_slice(
            running, contiguous_portion[:, :, None], (jnp.int32(0), jnp.int32(0), batch_id)
        )

    moments = lax.fori_loop(
        first_batch,
        last_batch + 1,
        moment_step,
        jnp.zeros((clusters, num_pcs + 1, batches), jnp.float32),
    )
    devices_flat = lax.axis_size(CELLS) * lax.axis_size("grp")
    most_cells = 2 * local_cells * devices_flat // batches
    reach = (most_cells - 2) // local_cells + 1
    begins_here = (batch_starts >= offset) & (batch_starts < offset + local_cells)
    owner_mask = begins_here.astype(jnp.float32)
    head_owned = begins_here[first_batch]
    head_column = lax.dynamic_index_in_dim(moments, first_batch, 2, keepdims=False)
    sent_stats = jnp.where(head_owned, 0.0, 1.0) * head_column
    sent_tag = jnp.where(head_owned, 0.0, first_batch.astype(jnp.float32) + 1.0) * jnp.ones(
        (1,), jnp.float32
    )
    completed = moments
    for hop in range(1, reach + 1):
        got_stats, got_tag = from_behind((sent_stats, sent_tag), CELLS_GRP, -hop)
        got_id = jnp.maximum(got_tag[0].astype(jnp.int32) - 1, 0)
        accept = jnp.where((got_tag[0] > 0.5) & begins_here[got_id], 1.0, 0.0)
        single_observation = (
            lax.dynamic_index_in_dim(completed, got_id, 2, keepdims=False) + accept * got_stats
        )
        completed = lax.dynamic_update_slice(
            completed, single_observation[:, :, None], (jnp.int32(0), jnp.int32(0), got_id)
        )
    completed = completed * owner_mask[None, None, :]
    weight, right_side, mass_total, moment_total = jax.tree.map(
        lambda part: by_axis(part, CELLS_GRP), batch_parts(completed, sample_shrinkage_lambda)
    )
    coefficients = slopes_of(completed, sample_shrinkage_lambda, weight, right_side)
    every_centroid = moment_total / (1.0 + mass_total)[:, None]
    new_centroids = lax.dynamic_slice_in_dim(
        every_centroid, lax.axis_index(CELLS) * owned, owned, 0
    )
    tail_owned = begins_here[last_batch]
    tail_column = lax.dynamic_index_in_dim(coefficients, last_batch, 2, keepdims=False)
    tail_send = jnp.where(tail_owned, 1.0, 0.0) * tail_column
    tail_tag = jnp.where(tail_owned, last_batch.astype(jnp.float32) + 1.0, 0.0) * jnp.ones(
        (1,), jnp.float32
    )
    head_fix = jnp.zeros_like(tail_column)
    for hop in range(1, reach + 1):
        got_coef, got_tag = from_behind((tail_send, tail_tag), CELLS_GRP, hop)
        match = got_tag[0] == first_batch.astype(jnp.float32) + 1.0
        head_fix = jnp.where(match, got_coef, head_fix)
    own_head = lax.dynamic_index_in_dim(coefficients, first_batch, 2, keepdims=False)
    head_final = jnp.where(head_owned, own_head, head_fix)
    coefficients = lax.dynamic_update_slice(
        coefficients, head_final[:, :, None], (jnp.int32(0), jnp.int32(0), first_batch)
    )

    def correct_step(batch_id, running):
        in_batch = (batch_of == batch_id).astype(jnp.float32)
        slope_table = lax.dynamic_index_in_dim(coefficients, batch_id, 2, keepdims=False)
        moved = jnp.einsum("kd,kn->dn", slope_table, assign * in_batch[None, :], precision=highest)
        return running + moved

    corrected = lax.fori_loop(first_batch, last_batch + 1, correct_step, jnp.zeros_like(latent_coordinates))
    return (latent_coordinates - corrected, new_centroids)


SLOTS = 8
ROWS = 64
MOST = 10485
LOGICAL = pl.DeviceIdType.LOGICAL
TILE = 256
CLOSE = 4
bf16, f32 = jnp.bfloat16, jnp.float32


def two_pieces(value):
    first = value.astype(bf16)
    return first, (value - first.astype(f32)).astype(bf16)


def across(left, right):
    return lax.dot_general(left, right, (((1,), (1,)), ((), ())), preferred_element_type=f32)


def plain(left, right):
    return jnp.dot(left, right, preferred_element_type=f32)


def step_kernel(
    shape,
    cells_all,
    z_hbm,
    means_ref,
    soft_ref,
    ridge_ref,
    pop_ref,
    zf,
    pair,
    slopes,
    starts_ref,
    flag_ref,
    cent_ref,
    zc,
    ex,
    means_wide,
    pieces,
    near_out,
    near_counts,
    near_mass,
    near_moments,
    ends_out,
    line_a,
    line_b,
    sums_out,
    sum_in,
    cent_out,
    cent_in,
    tile_out,
    tile_in,
    full_sums,
    load_sems,
    send_sems,
    recv_sems,
):
    nz, ny, nc, nx = shape
    near = nc * nx
    far = nz * ny
    count = near * far
    cells = zf.shape[1]
    pcs, clusters = means_ref.shape
    batches = pop_ref.shape[1]
    rows_each = ROWS // near
    width = 512
    reach = (MOST - 2) // cells + 1
    offsets = [h for h in range(-reach, reach + 1) if h]
    me = (
        (lax.axis_index("cells_0") * ny + lax.axis_index("cells_1")) * nc
        + lax.axis_index("cells_2")
    ) * nx + lax.axis_index("grp")
    rank = lax.rem(me, near)
    block = lax.div(me, near)

    def mate(r):
        return block * near + lax.rem(rank + r, near)

    def peer(r):
        return lax.rem(block + r, far) * near + rank

    def neighbour(h):
        return lax.rem(me + (h + count), count)

    def push(src, dst, which, q):
        pltpu.make_async_remote_copy(
            src_ref=src,
            dst_ref=dst,
            send_sem=send_sems.at[which],
            recv_sem=recv_sems.at[which],
            device_id=q,
            device_id_type=LOGICAL,
        ).start()

    def arrived(buffer, which):
        pltpu.make_async_copy(buffer, buffer, recv_sems.at[which]).wait()

    def left(buffer, which):
        pltpu.make_async_copy(buffer, buffer, send_sems.at[which]).wait()

    loads = load_sems.shape[0]
    part = cells // loads
    for i in range(loads):
        columns = pl.ds(i * part, part)
        pltpu.make_async_copy(z_hbm.at[0, :, columns], zf.at[:, columns], load_sems.at[i]).start()

    barrier = pltpu.get_barrier_semaphore()
    for r in range(1, near):
        pl.semaphore_signal(barrier, inc=1, device_id=mate(r), device_id_type=LOGICAL)
    for h in offsets:
        pl.semaphore_signal(barrier, inc=1, device_id=neighbour(h), device_id_type=LOGICAL)

    def greet(r, carry):
        pl.semaphore_signal(barrier, inc=1, device_id=peer(r), device_id_type=LOGICAL)
        return carry

    lax.fori_loop(1, far, greet, 0)

    means_wide[...] = jnp.zeros_like(means_wide)
    means_wide[0:pcs, :] = means_ref[...]
    g = means_wide[...].T
    square = lax.broadcasted_iota(jnp.int32, (clusters, clusters), 0)
    lane = lax.broadcasted_iota(jnp.int32, (clusters, clusters), 1)
    soft = jnp.sum(jnp.where(square == lane, soft_ref[...], 0.0), axis=1, keepdims=True)
    offset_of = -0.5 * jnp.sum(g * g, axis=1, keepdims=True) / soft
    weights = jnp.where(lane == pcs, offset_of, g / soft)
    w1 = weights.astype(bf16).astype(f32)
    w2 = (weights - w1).astype(bf16).astype(f32)
    o1 = offset_of.astype(bf16).astype(f32)
    o2 = (offset_of - o1).astype(bf16).astype(f32)
    w1 = jnp.where(lane == pcs + 1, offset_of - o1 - o2, w1)
    w1 = (w1 + pltpu.roll(w1, ROWS, 1)).astype(bf16)
    w2 = (w2 + pltpu.roll(w2, ROWS, 1)).astype(bf16)
    weights = jnp.concatenate([w1, w2], axis=1)

    pop = pop_ref[...]
    up = lax.broadcasted_iota(jnp.int32, (batches, batches), 0)
    down = lax.broadcasted_iota(jnp.int32, (batches, batches), 1)
    column = jnp.sum(jnp.where(up == down, pop, 0), axis=1, keepdims=True)
    ends = jnp.sum(jnp.where(up <= down, column, 0), axis=0, keepdims=True)
    half = lax.broadcasted_iota(jnp.int32, (16, 1), 0)
    device = me + lax.rem(half, 8) - reach
    limit = device * cells + jnp.where(half >= 8, cells - 1, 0)
    spot = jnp.sum(jnp.where(ends <= limit, 1, 0), axis=1, keepdims=True)
    spot = jnp.where(device < 0, -9, spot)
    first = {h: spot[h + reach : h + reach + 1] for h in offsets + [0]}
    last = {h: spot[8 + h + reach : 9 + h + reach] for h in offsets + [0]}
    slot = lax.broadcasted_iota(jnp.int32, (SLOTS, 1), 0)
    batch_id = first[0] + slot
    batch_lane = lax.broadcasted_iota(jnp.int32, (SLOTS, batches), 1)
    chosen = batch_lane == batch_id
    held = jnp.sum(jnp.where(chosen, pop, 0), axis=1, keepdims=True)
    ridge = jnp.sum(jnp.where(chosen, ridge_ref[...], 0.0), axis=1, keepdims=True)
    ridge = jnp.where(batch_id < batches, ridge, 1.0)
    stop = jnp.sum(jnp.where(batch_lane <= batch_id, pop, 0), axis=1, keepdims=True) - me * cells
    start = stop - held
    held = held.astype(f32)
    starts_ref[...] = jnp.broadcast_to(jnp.where(batch_id < batches, start, 2 * cells), (SLOTS, 128))
    tail = slot == last[0] - first[0]
    head = slot == 0
    behind = {h: (last[h] == first[0]).astype(f32) for h in offsets if h < 0}
    ahead = {h: (first[h] == last[0]).astype(f32) for h in offsets if h > 0}

    crowded = jnp.zeros((1, 1), jnp.int32)
    for inner, room in ((SLOTS - 1, cells), (CLOSE - 1, width)):
        window = jnp.sum(
            jnp.where((up >= down) & (up < down + inner), column, 0), axis=0, keepdims=True
        )
        window = jnp.where((window < room - 1) & (batch_lane[0:1] <= batches - inner), 1, 0)
        crowded = crowded + jnp.sum(window, axis=1, keepdims=True)
    flag_ref[...] = jnp.broadcast_to(crowded, (1, 128))

    def inside(c, width, times):
        position = lax.broadcasted_iota(jnp.int32, (SLOTS * times, width), 1) + c * width
        low = jnp.concatenate([start] * times, axis=0)
        high = jnp.concatenate([stop] * times, axis=0)
        return ((position >= low) & (position < high)).astype(f32)

    def completed(own, buffer, tail_row):
        before = jnp.zeros((1, clusters), f32)
        after = jnp.zeros((1, clusters), f32)
        for i, h in enumerate(offsets):
            if h < 0:
                before = before + behind[h] * buffer[i, 1:2, :]
            else:
                after = after + ahead[h] * buffer[i, 0:1, :]
        return own + jnp.where(head, before, 0.0) + jnp.where(tail, after, 0.0)

    def rows_of(*lines):
        row = lax.broadcasted_iota(jnp.int32, (8, clusters), 0)
        value = jnp.zeros((8, clusters), f32)
        for i, line in enumerate(lines):
            value = jnp.where(row == i, line, value)
        return value


    for i in range(loads):
        columns = pl.ds(i * part, part)
        pltpu.make_async_copy(z_hbm.at[0, :, columns], zf.at[:, columns], load_sems.at[i]).wait()

    def prior_step(c, total):
        columns = pl.ds(pl.multiple_of(c * width, width), width)
        z1, z2 = two_pieces(
            jnp.concatenate(
                [
                    zf[:, columns],
                    jnp.ones((2, width), f32),
                    jnp.zeros((ROWS - 2 - pcs, width), f32),
                ],
                axis=0,
            )
        )
        zc[0:ROWS, columns] = z1
        zc[ROWS : 2 * ROWS, columns] = z2
        score = plain(weights, jnp.concatenate([z1, z2, z1, z2], axis=0))
        raised = jnp.exp(score - jnp.max(score, axis=0, keepdims=True))
        ex[:, columns] = raised
        p1, p2 = two_pieces(raised * (1.0 / jnp.sum(raised, axis=0, keepdims=True)))
        mask = inside(c, width, 2).astype(bf16)
        return total + across(mask, jnp.concatenate([p1, p2], axis=0))

    total = lax.fori_loop(
        0, cells // width, prior_step, jnp.zeros((2 * SLOTS, 2 * clusters), f32)
    )
    counts = total[0:SLOTS, 0:clusters] + total[0:SLOTS, clusters : 2 * clusters]
    own_total = jnp.sum(counts, axis=0, keepdims=True)
    near_out[0] = rows_of(
        counts[0:1], jnp.sum(jnp.where(tail, counts, 0.0), axis=0, keepdims=True), own_total
    )
    pl.semaphore_wait(barrier, near - 1 + far - 1 + len(offsets))
    for r in range(1, near):
        push(near_out.at[0], line_a.at[r - 1], 0, mate(r))
    for i, h in enumerate(offsets):
        push(near_out.at[0], near_counts.at[len(offsets) - 1 - i], 1, neighbour(h))
    arrived(line_a, 0)
    block_total = own_total
    for r in range(near - 1):
        block_total = block_total + line_a[r, 2:3, :]
    tile_out[0] = jnp.broadcast_to(block_total, (8, clusters))

    def send_line(r, carry):
        push(tile_out.at[0], line_b.at[r - 1], 2, peer(r))
        return carry

    lax.fori_loop(1, far, send_line, 0)
    arrived(near_counts, 1)
    full_counts = completed(counts, near_counts, 1)
    arrived(line_b, 2)
    totals = block_total + jnp.sum(line_b[...], axis=0)[0:1]
    expected = held * totals * (1.0 / cells_all)
    ratio = (expected + 1.0) / (full_counts + 1.0)
    factor = ratio * ratio
    f1 = factor.astype(bf16).astype(f32)
    f2 = (factor - f1).astype(bf16).astype(f32)
    f3 = factor - f1 - f2
    factor = jnp.concatenate([f1, f2, f3, jnp.zeros_like(f3)], axis=0).T.astype(bf16)

    def summed(value):
        top, low = value[0:ROWS], value[ROWS : 2 * ROWS]
        return top[:, 0:clusters] + top[:, clusters:] + low[:, 0:clusters] + low[:, clusters:]

    def moment_step(c, carry):
        columns = pl.ds(pl.multiple_of(c * width, width), width)
        mask = inside(c, width, 4)
        weighed = ex[:, columns] * plain(factor, mask.astype(bf16))
        a1, a2 = two_pieces(weighed * (1.0 / jnp.sum(weighed, axis=0, keepdims=True)))
        both = jnp.concatenate([a1, a2], axis=0)
        pair[:, columns] = both
        z = zc[:, columns]
        kind = jnp.sum(mask[0:SLOTS] * slot.astype(f32), axis=0, keepdims=True)
        kind = kind - base_of(c).astype(f32)
        lined = [z * (kind == j).astype(f32).astype(bf16) for j in range(CLOSE)]
        value = across(jnp.concatenate(lined, axis=0), both)
        for j in range(CLOSE):
            pieces[c, j] = summed(value[2 * ROWS * j : 2 * ROWS * (j + 1)])
        return carry

    def base_of(c):
        return jnp.sum(
            jnp.where((start <= c * width) & (slot > 0) & (batch_id < batches), 1, 0),
            axis=0,
            keepdims=True,
        )

    lax.fori_loop(0, cells // width, moment_step, 0)
    moments = [jnp.zeros((ROWS, clusters), f32) for s in range(SLOTS)]
    for c in range(cells // width):
        base = base_of(c)
        for s in range(SLOTS):
            for j in range(min(s + 1, CLOSE)):
                moments[s] = moments[s] + jnp.where(base + j == s, 1.0, 0.0) * pieces[c, j]
    whole = moments[0]
    for s in range(1, SLOTS):
        whole = whole + moments[s]
    mass = rows_of(*[moments[s][pcs : pcs + 1] for s in range(SLOTS)])
    near_out[1] = rows_of(
        mass[0:1], jnp.sum(jnp.where(tail, mass, 0.0), axis=0, keepdims=True)
    )
    for i, h in enumerate(offsets):
        push(near_out.at[1], near_mass.at[len(offsets) - 1 - i], 3, neighbour(h))
    tail_moment = moments[0] * tail[0:1].astype(f32)
    for s in range(1, SLOTS):
        tail_moment = tail_moment + moments[s] * tail[s : s + 1].astype(f32)
    ends_out[0] = moments[0][0:56]
    ends_out[1] = tail_moment[0:56]
    for t in range(near):
        cent_out[t] = whole[t * rows_each : (t + 1) * rows_each]
    for r in range(1, near):
        push(cent_out.at[lax.rem(rank + r, near)], cent_in.at[r - 1], 4, mate(r))
    arrived(near_mass, 3)
    full_mass = completed(mass, near_mass, 1)
    shrink = ridge / (full_mass + ridge)
    right = moments[0] * shrink[0:1]
    for s in range(1, SLOTS):
        right = right + moments[s] * shrink[s : s + 1]
    for t in range(near):
        sums_out[t] = right[t * rows_each : (t + 1) * rows_each]
    for r in range(1, near):
        push(sums_out.at[lax.rem(rank + r, near)], sum_in.at[r - 1], 5, mate(r))
    for i, h in enumerate(offsets):
        push(ends_out.at[int(h > 0)], near_moments.at[len(offsets) - 1 - i], 6, neighbour(h))
    arrived(cent_in, 4)
    cent_tile = cent_out[rank]
    for r in range(near - 1):
        cent_tile = cent_tile + cent_in[r]
    tile_out[1] = cent_tile
    arrived(sum_in, 5)
    sum_tile = sums_out[rank]
    for r in range(near - 1):
        sum_tile = sum_tile + sum_in[r]
    tile_out[2] = sum_tile

    def send_sum(r, carry):
        push(tile_out.at[2], tile_in.at[1, r - 1], 8, peer(r))
        return carry

    def send_cent(r, carry):
        push(tile_out.at[1], tile_in.at[0, r - 1], 7, peer(r))
        return carry

    lax.fori_loop(1, far, send_sum, 0)
    lax.fori_loop(1, far, send_cent, 0)

    arrived(near_moments, 6)
    before = jnp.zeros((56, clusters), f32)
    after = jnp.zeros((56, clusters), f32)
    for i, h in enumerate(offsets):
        if h < 0:
            before = before + behind[h] * near_moments[i]
        else:
            after = after + ahead[h] * near_moments[i]

    arrived(tile_in.at[1], 8)
    full_sums[1, 0] = sum_tile + jnp.sum(tile_in[1], axis=0)
    for r in range(1, near):
        push(full_sums.at[1, 0], full_sums.at[1, r], 10, mate(r))
    arrived(tile_in.at[0], 7)
    full_sums[0, 0] = cent_tile + jnp.sum(tile_in[0], axis=0)
    for r in range(1, near):
        push(full_sums.at[0, 0], full_sums.at[0, r], 9, mate(r))

    def gathered(which):
        return jnp.concatenate(
            [full_sums[which, lax.rem(rank + (near - t), near)] for t in range(near)], axis=0
        )

    arrived(full_sums.at[1, pl.ds(1, near - 1)], 10)
    right = gathered(1)
    intercept = (right / (1.0 + right[pcs : pcs + 1]))[0:56]
    for s in range(SLOTS):
        moment = moments[s][0:56] + after * tail[s : s + 1].astype(f32)
        if s == 0:
            moment = moment + before
        line = full_mass[s : s + 1]
        slope = (moment - line * intercept) / (line + ridge[s : s + 1])
        c1, c2 = two_pieces(jnp.concatenate([slope, jnp.zeros((8, clusters), f32)], axis=0))
        slopes[ROWS * s : ROWS * (s + 1), :] = jnp.concatenate([c1, c1, c2], axis=1)

    arrived(full_sums.at[0, pl.ds(1, near - 1)], 9)
    centre = gathered(0)
    centre = (centre / (1.0 + centre[pcs : pcs + 1])).T
    owned = cent_ref.shape[0]
    cells_at = lax.div(me, nx)
    row = lax.broadcasted_iota(jnp.int32, (clusters, ROWS), 0)
    for j in range(owned):
        line = jnp.sum(jnp.where(row == cells_at * owned + j, centre, 0.0), axis=0, keepdims=True)
        cent_ref[j : j + 1, :] = line[:, 0:pcs]

    left(line_a, 0)
    left(near_counts, 1)
    left(line_b, 2)
    left(near_mass, 3)
    left(cent_in, 4)
    left(sum_in, 5)
    left(near_moments, 6)
    left(tile_in.at[0], 7)
    left(tile_in.at[1], 8)
    left(full_sums.at[0, pl.ds(1, near - 1)], 9)
    left(full_sums.at[1, pl.ds(1, near - 1)], 10)


def correct_kernel(
    zf, pair, slopes, starts_ref, cent_ref, out_hbm, cent_hbm, held, starts, out_sems
):
    pcs, cells = zf.shape
    clusters = pair.shape[0] // 2
    loads = out_sems.shape[0] - 1
    part = cells // loads
    cent = pltpu.make_async_copy(cent_ref, cent_hbm, out_sems.at[loads])
    cent.start()
    begin = [jnp.max(starts_ref[s : s + 1, :]) for s in range(SLOTS)]
    for s in range(SLOTS):
        starts[s] = begin[s]
    outs = []
    lane = lax.broadcasted_iota(jnp.int32, (1, TILE), 1)
    for i in range(loads):
        for t in range(i * part // TILE, (i + 1) * part // TILE):
            columns = slice(t * TILE, (t + 1) * TILE)
            base = sum((begin[s] <= t * TILE).astype(jnp.int32) for s in range(1, SLOTS))
            final = sum((begin[s] < (t + 1) * TILE).astype(jnp.int32) for s in range(1, SLOTS))
            border = jnp.int32(2 * cells)
            for s in range(1, SLOTS):
                border = jnp.where(
                    begin[s] > t * TILE, jnp.minimum(border, begin[s]), border
                )
            following = jnp.minimum(base + 1, SLOTS - 1)
            both = pair[:, columns]
            both = jnp.concatenate([both, both[0:clusters]], axis=0)

            def slope_of(j):
                return slopes[pl.ds(pl.multiple_of(j * ROWS, ROWS), ROWS), :]

            moved = plain(jnp.concatenate([slope_of(base), slope_of(following)], axis=0), both)
            moved = jnp.where(lane < border - t * TILE, moved[0:ROWS], moved[ROWS:])
            held[:, columns] = zf[:, columns] - moved[0:pcs]

            @pl.when(final > base + 1)
            def _():
                def more(j, carry):
                    other = zf[:, columns] - plain(slope_of(j), both)[0:pcs]
                    held[:, columns] = jnp.where(
                        lane >= starts[j] - t * TILE, other, held[:, columns]
                    )
                    return carry

                lax.fori_loop(base + 2, final + 1, more, 0)

        columns = pl.ds(i * part, part)
        outs.append(pltpu.make_async_copy(held.at[:, columns], out_hbm.at[:, columns], out_sems.at[i]))
        outs[-1].start()
    for copy in outs:
        copy.wait()
    cent.wait()


def narrow_body(
    shape, latent_coordinates, group_means, entropy_scaling, sample_shrinkage_lambda, sample_population
):
    pcs, cells = latent_coordinates.shape
    clusters = group_means.shape[0]
    batches = sample_population.shape[0]
    nz, ny, nc, nx = shape
    near, far = nc * nx, nz * ny
    rows_each = ROWS // near
    reach = (MOST - 2) // cells + 1
    owned = clusters // (nz * ny * nc)
    vmem = pl.BlockSpec(memory_space=pltpu.VMEM)
    scratch = [
        pltpu.VMEM((2 * ROWS, cells), bf16),
        pltpu.VMEM((clusters, cells), f32),
        pltpu.VMEM((clusters, clusters), f32),
        pltpu.VMEM((cells // 512, CLOSE, ROWS, clusters), f32),
        pltpu.VMEM((2, 8, clusters), f32),
        pltpu.VMEM((2 * reach, 8, clusters), f32),
        pltpu.VMEM((2 * reach, 8, clusters), f32),
        pltpu.VMEM((2 * reach, 56, clusters), f32),
        pltpu.VMEM((2, 56, clusters), f32),
        pltpu.VMEM((near - 1, 8, clusters), f32),
        pltpu.VMEM((far - 1, 8, clusters), f32),
        pltpu.VMEM((near, rows_each, clusters), f32),
        pltpu.VMEM((near - 1, rows_each, clusters), f32),
        pltpu.VMEM((near, rows_each, clusters), f32),
        pltpu.VMEM((near - 1, rows_each, clusters), f32),
        pltpu.VMEM((3, rows_each, clusters), f32),
        pltpu.VMEM((2, far - 1, rows_each, clusters), f32),
        pltpu.VMEM((2, near, rows_each, clusters), f32),
        pltpu.SemaphoreType.DMA((4,)),
        pltpu.SemaphoreType.DMA((11,)),
        pltpu.SemaphoreType.DMA((11,)),
    ]
    return pl.pallas_call(
        functools.partial(step_kernel, shape, float(cells * near * far)),
        out_shape=(
            pltpu.VMEM((pcs, cells), f32),
            pltpu.VMEM((2 * clusters, cells), bf16),
            pltpu.VMEM((SLOTS * ROWS, 3 * clusters), bf16),
            pltpu.VMEM((SLOTS, 128), jnp.int32),
            pltpu.VMEM((1, 128), jnp.int32),
            pltpu.VMEM((owned, pcs), f32),
        ),
        in_specs=[pl.BlockSpec(memory_space=pl.ANY)] + [vmem] * 4,
        out_specs=(vmem,) * 6,
        scratch_shapes=scratch,
        compiler_params=pltpu.CompilerParams(
            collective_id=0, has_side_effects=True, vmem_limit_bytes=24 * 1024 * 1024
        ),
    )(
        latent_coordinates[None],
        group_means.T,
        entropy_scaling.reshape(1, clusters),
        sample_shrinkage_lambda.reshape(1, batches),
        sample_population.reshape(1, batches),
    )


def corrected_by(kept, pair, slopes, starts, new_centroids):
    pcs, cells = kept.shape
    vmem = pl.BlockSpec(memory_space=pltpu.VMEM)
    anywhere = pl.BlockSpec(memory_space=pl.ANY)
    return pl.pallas_call(
        correct_kernel,
        out_shape=(pltpu.HBM((pcs, cells), f32), pltpu.HBM(new_centroids.shape, f32)),
        in_specs=[vmem] * 5,
        out_specs=(anywhere, anywhere),
        scratch_shapes=[
            pltpu.VMEM((pcs, cells), f32),
            pltpu.SMEM((SLOTS,), jnp.int32),
            pltpu.SemaphoreType.DMA((5,)),
        ],
        compiler_params=pltpu.CompilerParams(vmem_limit_bytes=16 * 1024 * 1024),
    )(
        kept,
        pair,
        slopes,
        starts,
        new_centroids,
    )


def body(
    shape, latent_coordinates, group_means, entropy_scaling, sample_shrinkage_lambda, sample_population
):
    arguments = (
        latent_coordinates,
        group_means,
        entropy_scaling,
        sample_shrinkage_lambda,
        sample_population,
    )
    kept, pair, slopes, starts, flag, new_centroids = narrow_body(shape, *arguments)
    return lax.cond(
        flag[0, 0] == 0,
        lambda: corrected_by(kept, pair, slopes, starts, new_centroids),
        lambda: wide_body(*arguments),
    )


def solution(mesh):
    shape = (mesh.shape["cells"] // 8, 4, 2, mesh.shape["grp"])
    finer = Mesh(mesh.devices.reshape(shape), ("cells_0", "cells_1", "cells_2", "grp"))
    return jax.shard_map(
        functools.partial(body, shape),
        mesh=finer,
        in_specs=(P(None, CELLS_GRP), P(), P(), P(), P()),
        out_specs=(P(None, CELLS_GRP), P(CELLS, None)),
        check_vma=False,
    )
```

```python
import functools

import jax
import jax.numpy as jnp
from jax import lax
from jax.experimental import pallas as pl
from jax.experimental.pallas import tpu as pltpu
from jax.sharding import Mesh
from jax.sharding import PartitionSpec as P

CELLS = ("cells_0", "cells_1", "cells_2")
CELLS_GRP = ("cells_0", "cells_1", "cells_2", "grp")


diversity = 2.0
intercept_ridge = 1.0
highest = lax.Precision.HIGHEST


def split_up(array, dim, size):
    dims = array.shape
    parts = array.reshape(*dims[:dim], size, dims[dim] // size, *dims[dim + 1 :])
    return jnp.moveaxis(parts, dim, 0)


def summed_on_arrival(array, axis, dim):
    size = lax.axis_size(axis)
    parts = lax.all_to_all(split_up(array, dim, size), axis, 0, 0, tiled=True)
    return jnp.sum(parts, axis=0)


def sum_in_two_steps(array, axes, dim):
    far, near = axes
    parts = split_up(array, dim, lax.axis_size(far))
    nearer = summed_on_arrival(parts, near, dim + 1)
    arrived = lax.all_to_all(nearer, far, split_axis=0, concat_axis=0, tiled=True)
    return arrived.sum(axis=0)


def filled_up(lines, size):
    spare = -len(lines) % size
    return jnp.pad(lines, [(0, spare)] + [(0, 0)] * (lines.ndim - 1))


def sent_to_all(array, axis):
    size = lax.axis_size(axis)
    return lax.all_to_all(
        jnp.broadcast_to(array[None], (size, *array.shape)), axis, 0, 0, tiled=True
    )


def joined_along(parts, dim):
    parts = jnp.moveaxis(parts, 0, dim)
    dims = parts.shape
    return parts.reshape(*dims[:dim], dims[dim] * dims[dim + 1], *dims[dim + 2 :])


def gather_axes(array, axes, dim):
    far, near = axes
    leading = sent_to_all(array, far)
    parts = jnp.swapaxes(sent_to_all(leading, near), 0, 1)
    return joined_along(parts.reshape(-1, *array.shape), dim)


def total_of(array, axes):
    lines = array.reshape(-1)
    own = sum_in_two_steps(
        filled_up(lines, lax.axis_size(axes[0]) * lax.axis_size(axes[1])), axes, 0
    )
    whole = gather_axes(own, axes, 0)
    return whole[: len(lines)].reshape(array.shape)


def from_behind(block, axis, distance):
    devices = range(lax.axis_size(axis))
    route = [(i - distance, i) for i in devices if i - distance in devices]
    return lax.ppermute(block, axis, route)


def by_axis(array, axes):
    return functools.reduce(lax.psum, axes, array)


def observation_affinity(latent_coordinates, group_means, entropy_scaling):
    pairwise_dots = jnp.dot(
        group_means, latent_coordinates, precision=highest, preferred_element_type=jnp.float32
    )
    quadratic_lengths = jnp.sum(group_means * group_means, axis=1)
    return (2.0 * pairwise_dots - quadratic_lengths[:, None]) / (2.0 * entropy_scaling[:, None])


def probabilistic_responsibility(group_affinity):
    top = jnp.max(group_affinity, axis=0, keepdims=True)
    raised = jnp.exp(group_affinity - top)
    return raised / jnp.sum(raised, axis=0, keepdims=True)


def batch_parts(moments, ridge):
    mass = moments[:, 0, :]
    sums = moments[:, 1:, :]
    shrink = ridge[None, :] / (mass + ridge[None, :])
    weight = jnp.sum(mass * shrink, axis=1)
    right_side = jnp.sum(sums * shrink[:, None, :], axis=2)
    return (weight, right_side, jnp.sum(mass, axis=1), jnp.sum(sums, axis=2))


def slopes_of(moments, ridge, weight, right_side):
    mass = moments[:, 0, :]
    sums = moments[:, 1:, :]
    intercept = right_side / (intercept_ridge + weight)[:, None]
    return (sums - mass[:, None, :] * intercept[:, :, None]) / (mass + ridge[None, :])[:, None, :]


def wide_body(
    latent_coordinates, group_means, entropy_scaling, sample_shrinkage_lambda, sample_population
):
    local_cells = latent_coordinates.shape[1]
    num_pcs = latent_coordinates.shape[0]
    clusters = group_means.shape[0]
    batches = sample_population.shape[0]
    owned = clusters // lax.axis_size(CELLS)
    offset = (lax.axis_index(CELLS) * lax.axis_size("grp") + lax.axis_index("grp")) * local_cells
    batch_ends = jnp.cumsum(sample_population)
    batch_starts = batch_ends - sample_population
    cells_total = jnp.sum(sample_population).astype(jnp.float32)
    position = offset + lax.iota(jnp.int32, local_cells)
    batch_of = jnp.sum((batch_ends[:, None] <= position[None, :]).astype(jnp.int32), axis=0)
    first_batch = batch_of[0]
    last_batch = batch_of[local_cells - 1]
    group_affinity = observation_affinity(latent_coordinates, group_means, entropy_scaling)
    expected_occupancy = probabilistic_responsibility(group_affinity)

    def count_step(batch_id, running):
        in_batch = (batch_of == batch_id).astype(jnp.float32)
        single_observation = jnp.dot(
            expected_occupancy, in_batch, precision=highest, preferred_element_type=jnp.float32
        )
        return lax.dynamic_update_slice(
            running, single_observation[:, None], (jnp.int32(0), batch_id)
        )

    counts = lax.fori_loop(
        first_batch, last_batch + 1, count_step, jnp.zeros((clusters, batches), jnp.float32)
    )
    counts = total_of(counts, (("cells_0", "cells_1"), ("cells_2", "grp")))
    totals = jnp.sum(counts, axis=1)
    expected = sample_population.astype(jnp.float32)[None, :] * totals[:, None] / cells_total
    penalty = diversity * jnp.log((counts + 1.0) / (expected + 1.0))

    def penalty_step(batch_id, running):
        in_batch = (batch_of == batch_id).astype(jnp.float32)
        column = lax.dynamic_index_in_dim(penalty, batch_id, 1, keepdims=True)
        return running + column * in_batch[None, :]

    cell_penalty = lax.fori_loop(
        first_batch, last_batch + 1, penalty_step, jnp.zeros((clusters, local_cells), jnp.float32)
    )
    assign = probabilistic_responsibility(group_affinity - cell_penalty)
    augmented = jnp.concatenate(
        [jnp.ones((1, local_cells), jnp.float32), latent_coordinates], axis=0
    )

    def moment_step(batch_id, running):
        in_batch = (batch_of == batch_id).astype(jnp.float32)
        contiguous_portion = jnp.einsum(
            "kn,dn->kd", assign * in_batch[None, :], augmented, precision=highest
        )
        return lax.dynamic_update_slice(
            running, contiguous_portion[:, :, None], (jnp.int32(0), jnp.int32(0), batch_id)
        )

    moments = lax.fori_loop(
        first_batch,
        last_batch + 1,
        moment_step,
        jnp.zeros((clusters, num_pcs + 1, batches), jnp.float32),
    )
    devices_flat = lax.axis_size(CELLS) * lax.axis_size("grp")
    most_cells = 2 * local_cells * devices_flat // batches
    reach = (most_cells - 2) // local_cells + 1
    begins_here = (batch_starts >= offset) & (batch_starts < offset + local_cells)
    owner_mask = begins_here.astype(jnp.float32)
    head_owned = begins_here[first_batch]
    head_column = lax.dynamic_index_in_dim(moments, first_batch, 2, keepdims=False)
    sent_stats = jnp.where(head_owned, 0.0, 1.0) * head_column
    sent_tag = jnp.where(head_owned, 0.0, first_batch.astype(jnp.float32) + 1.0) * jnp.ones(
        (1,), jnp.float32
    )
    completed = moments
    for hop in range(1, reach + 1):
        got_stats, got_tag = from_behind((sent_stats, sent_tag), CELLS_GRP, -hop)
        got_id = jnp.maximum(got_tag[0].astype(jnp.int32) - 1, 0)
        accept = jnp.where((got_tag[0] > 0.5) & begins_here[got_id], 1.0, 0.0)
        single_observation = (
            lax.dynamic_index_in_dim(completed, got_id, 2, keepdims=False) + accept * got_stats
        )
        completed = lax.dynamic_update_slice(
            completed, single_observation[:, :, None], (jnp.int32(0), jnp.int32(0), got_id)
        )
    completed = completed * owner_mask[None, None, :]
    weight, right_side, mass_total, moment_total = jax.tree.map(
        lambda part: by_axis(part, CELLS_GRP), batch_parts(completed, sample_shrinkage_lambda)
    )
    coefficients = slopes_of(completed, sample_shrinkage_lambda, weight, right_side)
    every_centroid = moment_total / (1.0 + mass_total)[:, None]
    new_centroids = lax.dynamic_slice_in_dim(
        every_centroid, lax.axis_index(CELLS) * owned, owned, 0
    )
    tail_owned = begins_here[last_batch]
    tail_column = lax.dynamic_index_in_dim(coefficients, last_batch, 2, keepdims=False)
    tail_send = jnp.where(tail_owned, 1.0, 0.0) * tail_column
    tail_tag = jnp.where(tail_owned, last_batch.astype(jnp.float32) + 1.0, 0.0) * jnp.ones(
        (1,), jnp.float32
    )
    head_fix = jnp.zeros_like(tail_column)
    for hop in range(1, reach + 1):
        got_coef, got_tag = from_behind((tail_send, tail_tag), CELLS_GRP, hop)
        match = got_tag[0] == first_batch.astype(jnp.float32) + 1.0
        head_fix = jnp.where(match, got_coef, head_fix)
    own_head = lax.dynamic_index_in_dim(coefficients, first_batch, 2, keepdims=False)
    head_final = jnp.where(head_owned, own_head, head_fix)
    coefficients = lax.dynamic_update_slice(
        coefficients, head_final[:, :, None], (jnp.int32(0), jnp.int32(0), first_batch)
    )

    def correct_step(batch_id, running):
        in_batch = (batch_of == batch_id).astype(jnp.float32)
        slope_table = lax.dynamic_index_in_dim(coefficients, batch_id, 2, keepdims=False)
        moved = jnp.einsum("kd,kn->dn", slope_table, assign * in_batch[None, :], precision=highest)
        return running + moved

    corrected = lax.fori_loop(first_batch, last_batch + 1, correct_step, jnp.zeros_like(latent_coordinates))
    return (latent_coordinates - corrected, new_centroids)


SLOTS = 8
ROWS = 64
MOST = 10485
LOGICAL = pl.DeviceIdType.LOGICAL
TILE = 256
CLOSE = 4
bf16, f32 = jnp.bfloat16, jnp.float32


def two_pieces(value):
    first = value.astype(bf16)
    return first, (value - first.astype(f32)).astype(bf16)


def across(left, right):
    return lax.dot_general(left, right, (((1,), (1,)), ((), ())), preferred_element_type=f32)


def plain(left, right):
    return jnp.dot(left, right, preferred_element_type=f32)


def step_kernel(
    shape,
    cells_all,
    z_hbm,
    means_hbm,
    soft_hbm,
    ridge_hbm,
    pop_hbm,
    zf,
    pair,
    slopes,
    starts_ref,
    flag_ref,
    cent_ref,
    means_ref,
    soft_ref,
    ridge_ref,
    pop_ref,
    zc,
    ex,
    lined,
    means_wide,
    pieces,
    near_out,
    near_counts,
    near_mass,
    near_moments,
    ends_out,
    full_moments,
    line_out,
    line_a,
    line_b,
    sums_out,
    sum_in,
    cent_out,
    cent_in,
    cent_y,
    cent_z,
    tile_out,
    tile_in,
    full_sums,
    small_sems,
    load_sems,
    send_sems,
    recv_sems,
):
    nz, ny, nc, nx = shape
    near = nc * nx
    far = nz * ny
    count = near * far
    cells = zf.shape[1]
    pcs, clusters = means_ref.shape
    batches = pop_ref.shape[1]
    rows_each = ROWS // near
    width = 512
    reach = (MOST - 2) // cells + 1
    offsets = [h for h in range(-reach, reach + 1) if h]
    me = (
        (lax.axis_index("cells_0") * ny + lax.axis_index("cells_1")) * nc
        + lax.axis_index("cells_2")
    ) * nx + lax.axis_index("grp")
    rank = lax.rem(me, near)
    block = lax.div(me, near)

    def mate(r):
        return block * near + lax.rem(rank + r, near)

    def peer(r):
        return lax.rem(block + r, far) * near + rank

    def along_y(r):
        at = lax.rem(block, ny)
        return (block - at + lax.rem(at + r, ny)) * near + rank

    def along_z(r):
        return lax.rem(block + r * ny, far) * near + rank

    def neighbour(h):
        return lax.rem(me + (h + count), count)

    def push(src, dst, which, q):
        pltpu.make_async_remote_copy(
            src_ref=src,
            dst_ref=dst,
            send_sem=send_sems.at[which],
            recv_sem=recv_sems.at[which],
            device_id=q,
            device_id_type=LOGICAL,
        ).start()

    def arrived(buffer, which):
        pltpu.make_async_copy(buffer, buffer, recv_sems.at[which]).wait()

    def left(buffer, which):
        pltpu.make_async_copy(buffer, buffer, send_sems.at[which]).wait()

    small = [
        pltpu.make_async_copy(src, dst, small_sems.at[i])
        for i, (src, dst) in enumerate(
            (
                (pop_hbm, pop_ref),
                (means_hbm, means_ref),
                (soft_hbm, soft_ref),
                (ridge_hbm, ridge_ref),
            )
        )
    ]
    for copy in small:
        copy.start()
    for i in range(cells // width):
        columns = pl.ds(i * width, width)
        pltpu.make_async_copy(z_hbm.at[0, :, columns], zf.at[:, columns], load_sems.at[i]).start()

    barrier = pltpu.get_barrier_semaphore()
    for r in range(1, near):
        pl.semaphore_signal(barrier, inc=1, device_id=mate(r), device_id_type=LOGICAL)
    for h in offsets:
        pl.semaphore_signal(barrier, inc=1, device_id=neighbour(h), device_id_type=LOGICAL)

    def greet(r, carry):
        pl.semaphore_signal(barrier, inc=1, device_id=peer(r), device_id_type=LOGICAL)
        return carry

    lax.fori_loop(1, far, greet, 0)
    for r in range(1, ny):
        pl.semaphore_signal(barrier, inc=1, device_id=along_y(r), device_id_type=LOGICAL)
    for r in range(1, nz):
        pl.semaphore_signal(barrier, inc=1, device_id=along_z(r), device_id_type=LOGICAL)

    for copy in small:
        copy.wait()

    means_wide[...] = jnp.zeros_like(means_wide)
    means_wide[0:pcs, :] = means_ref[...]
    g = means_wide[...].T
    square = lax.broadcasted_iota(jnp.int32, (clusters, clusters), 0)
    lane = lax.broadcasted_iota(jnp.int32, (clusters, clusters), 1)
    soft = jnp.sum(jnp.where(square == lane, soft_ref[...], 0.0), axis=1, keepdims=True)
    offset_of = -0.5 * jnp.sum(g * g, axis=1, keepdims=True) / soft
    weights = jnp.where(lane == pcs, offset_of, g / soft)
    w1 = weights.astype(bf16).astype(f32)
    w2 = (weights - w1).astype(bf16).astype(f32)
    o1 = offset_of.astype(bf16).astype(f32)
    o2 = (offset_of - o1).astype(bf16).astype(f32)
    w1 = jnp.where(lane == pcs + 1, offset_of - o1 - o2, w1)
    w1 = (w1 + pltpu.roll(w1, ROWS, 1)).astype(bf16)
    w2 = (w2 + pltpu.roll(w2, ROWS, 1)).astype(bf16)
    weights = jnp.concatenate([w1, w2], axis=1)

    pop = pop_ref[...]
    up = lax.broadcasted_iota(jnp.int32, (batches, batches), 0)
    down = lax.broadcasted_iota(jnp.int32, (batches, batches), 1)
    column = jnp.sum(jnp.where(up == down, pop, 0), axis=1, keepdims=True)
    ends = jnp.sum(jnp.where(up <= down, column, 0), axis=0, keepdims=True)
    half = lax.broadcasted_iota(jnp.int32, (16, 1), 0)
    device = me + lax.rem(half, 8) - reach
    limit = device * cells + jnp.where(half >= 8, cells - 1, 0)
    spot = jnp.sum(jnp.where(ends <= limit, 1, 0), axis=1, keepdims=True)
    spot = jnp.where(device < 0, -9, spot)
    first = {h: spot[h + reach : h + reach + 1] for h in offsets + [0]}
    last = {h: spot[8 + h + reach : 9 + h + reach] for h in offsets + [0]}
    slot = lax.broadcasted_iota(jnp.int32, (SLOTS, 1), 0)
    batch_id = first[0] + slot
    batch_lane = lax.broadcasted_iota(jnp.int32, (SLOTS, batches), 1)
    chosen = batch_lane == batch_id
    held = jnp.sum(jnp.where(chosen, pop, 0), axis=1, keepdims=True)
    ridge = jnp.sum(jnp.where(chosen, ridge_ref[...], 0.0), axis=1, keepdims=True)
    ridge = jnp.where(batch_id < batches, ridge, 1.0)
    stop = jnp.sum(jnp.where(batch_lane <= batch_id, pop, 0), axis=1, keepdims=True) - me * cells
    start = stop - held
    held = held.astype(f32)
    starts_ref[...] = jnp.broadcast_to(jnp.where(batch_id < batches, start, 2 * cells), (SLOTS, 128))
    tail = slot == last[0] - first[0]
    head = slot == 0
    behind = {h: (last[h] == first[0]).astype(f32) for h in offsets if h < 0}
    ahead = {h: (first[h] == last[0]).astype(f32) for h in offsets if h > 0}

    crowded = jnp.zeros((1, 1), jnp.int32)
    for inner, room in ((SLOTS - 1, cells), (CLOSE - 1, width)):
        window = jnp.sum(
            jnp.where((up >= down) & (up < down + inner), column, 0), axis=0, keepdims=True
        )
        window = jnp.where((window < room - 1) & (batch_lane[0:1] <= batches - inner), 1, 0)
        crowded = crowded + jnp.sum(window, axis=1, keepdims=True)
    flag_ref[...] = jnp.broadcast_to(crowded, (1, 128))

    def inside(c, width, times):
        position = lax.broadcasted_iota(jnp.int32, (SLOTS * times, width), 1) + c * width
        low = jnp.concatenate([start] * times, axis=0)
        high = jnp.concatenate([stop] * times, axis=0)
        return ((position >= low) & (position < high)).astype(f32)

    def completed(own, buffer):
        before = jnp.zeros((1, clusters), f32)
        after = jnp.zeros((1, clusters), f32)
        for i, h in enumerate(offsets):
            if h < 0:
                before = before + behind[h] * buffer[i, 1:2, :]
            else:
                after = after + ahead[h] * buffer[i, 0:1, :]
        return own + jnp.where(head, before, 0.0) + jnp.where(tail, after, 0.0)

    def tail_of(value):
        return jnp.sum(jnp.where(tail, value, 0.0), axis=0, keepdims=True)

    def greeted_rows(which, value):
        near_out[which, 0:1, :] = value[0:1]
        near_out[which, 1:2, :] = tail_of(value)

    runs = cells // width

    def base_of(c):
        return jnp.sum(
            jnp.where((start <= c * width) & (slot > 0) & (batch_id < batches), 1, 0),
            axis=0,
            keepdims=True,
        )


    def prior_step(c, total):
        columns = pl.ds(pl.multiple_of(c * width, width), width)
        pltpu.make_async_copy(z_hbm.at[0, :, columns], zf.at[:, columns], load_sems.at[c]).wait()
        z1, z2 = two_pieces(
            jnp.concatenate(
                [
                    zf[:, columns],
                    jnp.ones((2, width), f32),
                    jnp.zeros((ROWS - 2 - pcs, width), f32),
                ],
                axis=0,
            )
        )
        zc[0:ROWS, columns] = z1
        zc[ROWS : 2 * ROWS, columns] = z2
        score = plain(weights, jnp.concatenate([z1, z2, z1, z2], axis=0))
        raised = jnp.exp(score - jnp.max(score, axis=0, keepdims=True))
        ex[:, columns] = raised
        p1, p2 = two_pieces(raised * (1.0 / jnp.sum(raised, axis=0, keepdims=True)))
        mask = inside(c, width, 2).astype(bf16)
        return total + across(mask, jnp.concatenate([p1, p2], axis=0))

    total = lax.fori_loop(
        0, cells // width, prior_step, jnp.zeros((2 * SLOTS, 2 * clusters), f32)
    )
    counts = total[0:SLOTS, 0:clusters] + total[0:SLOTS, clusters : 2 * clusters]
    own_total = jnp.sum(counts, axis=0, keepdims=True)
    greeted_rows(0, counts)
    line_out[0] = own_total
    pl.semaphore_wait(barrier, near - 1 + far - 1 + len(offsets) + ny - 1 + nz - 1)
    for r in range(1, near):
        push(line_out.at[0], line_a.at[r - 1], 0, mate(r))
    for i, h in enumerate(offsets):
        push(near_out.at[0], near_counts.at[len(offsets) - 1 - i], 1, neighbour(h))

    def line_step(c, carry):
        columns = pl.ds(pl.multiple_of(c * width, width), width)
        mask = inside(c, width, 1)
        kind = jnp.sum(mask * slot.astype(f32), axis=0, keepdims=True)
        kind = kind - base_of(c).astype(f32)
        z = zc[:, columns]
        for j in range(CLOSE):
            lined[2 * ROWS * j : 2 * ROWS * (j + 1), columns] = z * (kind == j).astype(
                f32
            ).astype(bf16)
        return carry

    lax.fori_loop(0, runs // 2, line_step, 0)
    arrived(line_a, 0)
    block_total = own_total
    for r in range(near - 1):
        block_total = block_total + line_a[r]
    line_out[1] = block_total

    def send_line(r, carry):
        push(line_out.at[1], line_b.at[r - 1], 2, peer(r))
        return carry

    lax.fori_loop(1, far, send_line, 0)
    lax.fori_loop(runs // 2, runs, line_step, 0)
    arrived(near_counts, 1)
    full_counts = completed(counts, near_counts)
    arrived(line_b, 2)
    totals = block_total + jnp.sum(line_b[...], axis=0)
    expected = held * totals * (1.0 / cells_all)
    ratio = (expected + 1.0) / (full_counts + 1.0)
    factor = ratio * ratio
    f1 = factor.astype(bf16).astype(f32)
    f2 = (factor - f1).astype(bf16).astype(f32)
    f3 = factor - f1 - f2
    factor = jnp.concatenate([f1, f2, f3, jnp.zeros_like(f3)], axis=0).T.astype(bf16)

    def assign_step(c, total):
        columns = pl.ds(pl.multiple_of(c * width, width), width)
        mask = inside(c, width, 4).astype(bf16)
        weighed = ex[:, columns] * plain(factor, mask)
        a1, a2 = two_pieces(weighed * (1.0 / jnp.sum(weighed, axis=0, keepdims=True)))
        both = jnp.concatenate([a1, a2], axis=0)
        pair[:, columns] = both
        return total + across(mask[0 : 2 * SLOTS], both)

    total = lax.fori_loop(0, runs, assign_step, jnp.zeros((2 * SLOTS, 2 * clusters), f32))
    mass = total[0:SLOTS, 0:clusters] + total[0:SLOTS, clusters : 2 * clusters]
    greeted_rows(1, mass)
    for i, h in enumerate(offsets):
        push(near_out.at[1], near_mass.at[len(offsets) - 1 - i], 3, neighbour(h))

    def moment_step(c, carry):
        columns = pl.ds(pl.multiple_of(c * width, width), width)
        value = across(lined[:, columns], pair[:, columns])
        for j in range(CLOSE):
            top = value[2 * ROWS * j : 2 * ROWS * j + ROWS]
            low = value[2 * ROWS * j + ROWS : 2 * ROWS * (j + 1)]
            pieces[c, j] = (
                top[:, 0:clusters] + top[:, clusters:] + low[:, 0:clusters] + low[:, clusters:]
            )
        return carry

    lax.fori_loop(0, runs, moment_step, 0)
    places = [(c, j) for c in range(runs) for j in range(CLOSE)]
    whole = pieces[0, 0]
    for c, j in places[1:]:
        whole = whole + pieces[c, j]
    for t in range(near):
        cent_out[t] = whole[t * rows_each : (t + 1) * rows_each]
    for r in range(1, near):
        push(cent_out.at[lax.rem(rank + r, near)], cent_in.at[r - 1], 4, mate(r))
    arrived(near_mass, 3)
    full_mass = completed(mass, near_mass)
    shrink = ridge / (full_mass + ridge)
    right = jnp.zeros((ROWS, clusters), f32)
    for c in range(runs):
        base = base_of(c)
        for j in range(CLOSE):
            line = jnp.sum(jnp.where(slot == base + j, shrink, 0.0), axis=0, keepdims=True)
            right = right + line * pieces[c, j]
    for t in range(near):
        sums_out[t] = right[t * rows_each : (t + 1) * rows_each]
    for r in range(1, near):
        push(sums_out.at[lax.rem(rank + r, near)], sum_in.at[r - 1], 5, mate(r))

    first_moment = pieces[0, 0]
    for c in range(1, runs):
        first_moment = first_moment + jnp.where(base_of(c) == 0, 1.0, 0.0) * pieces[c, 0]
    tail_moment = jnp.zeros((ROWS, clusters), f32)
    tail_slot = last[0] - first[0]
    for c in range(runs):
        base = base_of(c)
        for j in range(CLOSE):
            tail_moment = tail_moment + jnp.where(base + j == tail_slot, 1.0, 0.0) * pieces[c, j]
    ends_out[0] = first_moment[0:56]
    ends_out[1] = tail_moment[0:56]
    for i, h in enumerate(offsets):
        push(ends_out.at[int(h > 0)], near_moments.at[len(offsets) - 1 - i], 6, neighbour(h))
    arrived(cent_in, 4)
    cent_tile = cent_out[rank]
    for r in range(near - 1):
        cent_tile = cent_tile + cent_in[r]
    tile_out[0] = cent_tile
    for r in range(1, ny):
        push(tile_out.at[0], cent_y.at[r - 1], 7, along_y(r))
    arrived(sum_in, 5)
    sum_tile = sums_out[rank]
    for r in range(near - 1):
        sum_tile = sum_tile + sum_in[r]
    tile_out[2] = sum_tile

    def send_sum(r, carry):
        push(tile_out.at[2], tile_in.at[r - 1], 8, peer(r))
        return carry

    lax.fori_loop(1, far, send_sum, 0)
    arrived(cent_y, 7)
    for r in range(ny - 1):
        cent_tile = cent_tile + cent_y[r]
    tile_out[1] = cent_tile
    for r in range(1, nz):
        push(tile_out.at[1], cent_z.at[r - 1], 11, along_z(r))
    moments = []
    for s in range(SLOTS):
        moment = jnp.zeros((ROWS, clusters), f32)
        for c, j in places:
            if j <= s <= CLOSE * c + j:
                moment = moment + jnp.where(base_of(c) + j == s, 1.0, 0.0) * pieces[c, j]
        moments.append(moment)

    arrived(near_moments, 6)
    before = jnp.zeros((56, clusters), f32)
    after = jnp.zeros((56, clusters), f32)
    for i, h in enumerate(offsets):
        if h < 0:
            before = before + behind[h] * near_moments[i]
        else:
            after = after + ahead[h] * near_moments[i]
    for s in range(SLOTS):
        moment = moments[s][0:56] + after * tail[s : s + 1].astype(f32)
        full_moments[s] = moment + before if s == 0 else moment

    arrived(tile_in, 8)
    full_sums[1, 0] = sum_tile + jnp.sum(tile_in[...], axis=0)
    for r in range(1, near):
        push(full_sums.at[1, 0], full_sums.at[1, r], 10, mate(r))
    arrived(cent_z, 11)
    for r in range(nz - 1):
        cent_tile = cent_tile + cent_z[r]
    full_sums[0, 0] = cent_tile
    for r in range(1, near):
        push(full_sums.at[0, 0], full_sums.at[0, r], 9, mate(r))

    def gathered(which):
        return jnp.concatenate(
            [full_sums[which, lax.rem(rank + (near - t), near)] for t in range(near)], axis=0
        )

    arrived(full_sums.at[1, pl.ds(1, near - 1)], 10)
    right = gathered(1)
    intercept = (right / (1.0 + right[pcs : pcs + 1]))[0:56]
    for s in range(SLOTS):
        moment = full_moments[s]
        line = full_mass[s : s + 1]
        slope = (moment - line * intercept) / (line + ridge[s : s + 1])
        c1, c2 = two_pieces(jnp.concatenate([slope, jnp.zeros((8, clusters), f32)], axis=0))
        slopes[ROWS * s : ROWS * (s + 1), :] = jnp.concatenate([c1, c1, c2], axis=1)

    arrived(full_sums.at[0, pl.ds(1, near - 1)], 9)
    centre = gathered(0)
    centre = (centre / (1.0 + centre[pcs : pcs + 1])).T
    owned = cent_ref.shape[0]
    cells_at = lax.div(me, nx)
    row = lax.broadcasted_iota(jnp.int32, (clusters, ROWS), 0)
    for j in range(owned):
        line = jnp.sum(jnp.where(row == cells_at * owned + j, centre, 0.0), axis=0, keepdims=True)
        cent_ref[j : j + 1, :] = line[:, 0:pcs]

    left(line_a, 0)
    left(near_counts, 1)
    left(line_b, 2)
    left(near_mass, 3)
    left(cent_in, 4)
    left(sum_in, 5)
    left(near_moments, 6)
    left(cent_y, 7)
    left(tile_in, 8)
    left(cent_z, 11)
    left(full_sums.at[0, pl.ds(1, near - 1)], 9)
    left(full_sums.at[1, pl.ds(1, near - 1)], 10)


def correct_kernel(
    zf, pair, slopes, starts_ref, cent_ref, out_hbm, cent_hbm, held, starts, out_sems
):
    pcs, cells = zf.shape
    clusters = pair.shape[0] // 2
    loads = out_sems.shape[0] - 1
    part = cells // loads
    cent = pltpu.make_async_copy(cent_ref, cent_hbm, out_sems.at[loads])
    cent.start()
    begin = [jnp.max(starts_ref[s : s + 1, :]) for s in range(SLOTS)]
    for s in range(SLOTS):
        starts[s] = begin[s]
    outs = []
    lane = lax.broadcasted_iota(jnp.int32, (1, TILE), 1)

    def slope_of(j):
        return slopes[pl.ds(pl.multiple_of(j * ROWS, ROWS), ROWS), :]

    for i in range(loads):
        beyond = jnp.int32(0)
        for t in range(i * part // TILE, (i + 1) * part // TILE):
            columns = slice(t * TILE, (t + 1) * TILE)
            base = jnp.int32(0)
            final = jnp.int32(0)
            border = jnp.int32(2 * cells)
            for s in range(1, SLOTS):
                base = base + jnp.where(begin[s] <= t * TILE, 1, 0)
                final = final + jnp.where(begin[s] < (t + 1) * TILE, 1, 0)
                border = jnp.where(begin[s] > t * TILE, jnp.minimum(border, begin[s]), border)
            beyond = jnp.maximum(beyond, final - base)
            following = jnp.minimum(base + 1, SLOTS - 1)
            both = pair[:, columns]
            both = jnp.concatenate([both, both[0:clusters]], axis=0)
            moved = plain(jnp.concatenate([slope_of(base), slope_of(following)], axis=0), both)
            moved = jnp.where(lane < border - t * TILE, moved[0:ROWS], moved[ROWS:])
            held[:, columns] = zf[:, columns] - moved[0:pcs]

        @pl.when(beyond > 1)
        def _():
            def tile_of(t, carry):
                columns = pl.ds(pl.multiple_of(t * TILE, TILE), TILE)
                base = jnp.int32(0)
                final = jnp.int32(0)
                for s in range(1, SLOTS):
                    base = base + jnp.where(begin[s] <= t * TILE, 1, 0)
                    final = final + jnp.where(begin[s] < (t + 1) * TILE, 1, 0)

                def more(j, carry):
                    both = pair[:, columns]
                    both = jnp.concatenate([both, both[0:clusters]], axis=0)
                    other = zf[:, columns] - plain(slope_of(j), both)[0:pcs]
                    held[:, columns] = jnp.where(
                        lane >= starts[j] - t * TILE, other, held[:, columns]
                    )
                    return carry

                lax.fori_loop(base + 2, final + 1, more, 0)
                return carry

            lax.fori_loop(i * part // TILE, (i + 1) * part // TILE, tile_of, 0)

        columns = pl.ds(i * part, part)
        outs.append(pltpu.make_async_copy(held.at[:, columns], out_hbm.at[:, columns], out_sems.at[i]))
        outs[-1].start()
    for copy in outs:
        copy.wait()
    cent.wait()


def narrow_body(
    shape, latent_coordinates, group_means, entropy_scaling, sample_shrinkage_lambda, sample_population
):
    pcs, cells = latent_coordinates.shape
    clusters = group_means.shape[0]
    batches = sample_population.shape[0]
    nz, ny, nc, nx = shape
    near, far = nc * nx, nz * ny
    rows_each = ROWS // near
    reach = (MOST - 2) // cells + 1
    owned = clusters // (nz * ny * nc)
    vmem = pl.BlockSpec(memory_space=pltpu.VMEM)
    tile = (rows_each, clusters)
    scratch = [
        pltpu.VMEM((pcs, clusters), f32),
        pltpu.VMEM((1, clusters), f32),
        pltpu.VMEM((1, batches), f32),
        pltpu.VMEM((1, batches), jnp.int32),
        pltpu.VMEM((2 * ROWS, cells), bf16),
        pltpu.VMEM((clusters, cells), f32),
        pltpu.VMEM((2 * ROWS * CLOSE, cells), bf16),
        pltpu.VMEM((clusters, clusters), f32),
        pltpu.VMEM((cells // 512, CLOSE, ROWS, clusters), f32),
        pltpu.VMEM((2, 2, clusters), f32),
        pltpu.VMEM((2 * reach, 2, clusters), f32),
        pltpu.VMEM((2 * reach, 2, clusters), f32),
        pltpu.VMEM((2 * reach, 56, clusters), f32),
        pltpu.VMEM((2, 56, clusters), f32),
        pltpu.VMEM((SLOTS, 56, clusters), f32),
        pltpu.VMEM((2, 1, clusters), f32),
        pltpu.VMEM((near - 1, 1, clusters), f32),
        pltpu.VMEM((far - 1, 1, clusters), f32),
        pltpu.VMEM((near, *tile), f32),
        pltpu.VMEM((near - 1, *tile), f32),
        pltpu.VMEM((near, *tile), f32),
        pltpu.VMEM((near - 1, *tile), f32),
        pltpu.VMEM((ny - 1, *tile), f32),
        pltpu.VMEM((nz - 1, *tile), f32),
        pltpu.VMEM((3, *tile), f32),
        pltpu.VMEM((far - 1, *tile), f32),
        pltpu.VMEM((2, near, *tile), f32),
        pltpu.SemaphoreType.DMA((4,)),
        pltpu.SemaphoreType.DMA((cells // 512,)),
        pltpu.SemaphoreType.DMA((12,)),
        pltpu.SemaphoreType.DMA((12,)),
    ]
    return pl.pallas_call(
        functools.partial(step_kernel, shape, float(cells * near * far)),
        out_shape=(
            pltpu.VMEM((pcs, cells), f32),
            pltpu.VMEM((2 * clusters, cells), bf16),
            pltpu.VMEM((SLOTS * ROWS, 3 * clusters), bf16),
            pltpu.VMEM((SLOTS, 128), jnp.int32),
            pltpu.VMEM((1, 128), jnp.int32),
            pltpu.VMEM((owned, pcs), f32),
        ),
        in_specs=[pl.BlockSpec(memory_space=pl.ANY)] * 5,
        out_specs=(vmem,) * 6,
        scratch_shapes=scratch,
        compiler_params=pltpu.CompilerParams(
            collective_id=0, has_side_effects=True, vmem_limit_bytes=24 * 1024 * 1024
        ),
    )(
        latent_coordinates[None],
        group_means.T,
        entropy_scaling.reshape(1, clusters),
        sample_shrinkage_lambda.reshape(1, batches),
        sample_population.reshape(1, batches),
    )


def corrected_by(kept, pair, slopes, starts, new_centroids):
    pcs, cells = kept.shape
    vmem = pl.BlockSpec(memory_space=pltpu.VMEM)
    anywhere = pl.BlockSpec(memory_space=pl.ANY)
    return pl.pallas_call(
        correct_kernel,
        out_shape=(pltpu.HBM((pcs, cells), f32), pltpu.HBM(new_centroids.shape, f32)),
        in_specs=[vmem] * 5,
        out_specs=(anywhere, anywhere),
        scratch_shapes=[
            pltpu.VMEM((pcs, cells), f32),
            pltpu.SMEM((SLOTS,), jnp.int32),
            pltpu.SemaphoreType.DMA((5,)),
        ],
        compiler_params=pltpu.CompilerParams(vmem_limit_bytes=16 * 1024 * 1024),
    )(
        kept,
        pair,
        slopes,
        starts,
        new_centroids,
    )


def body(
    shape, latent_coordinates, group_means, entropy_scaling, sample_shrinkage_lambda, sample_population
):
    arguments = (
        latent_coordinates,
        group_means,
        entropy_scaling,
        sample_shrinkage_lambda,
        sample_population,
    )
    kept, pair, slopes, starts, flag, new_centroids = narrow_body(shape, *arguments)
    return lax.cond(
        flag[0, 0] == 0,
        lambda: corrected_by(kept, pair, slopes, starts, new_centroids),
        lambda: wide_body(*arguments),
    )


def solution(mesh):
    shape = (mesh.shape["cells"] // 8, 4, 2, mesh.shape["grp"])
    finer = Mesh(mesh.devices.reshape(shape), ("cells_0", "cells_1", "cells_2", "grp"))
    return jax.shard_map(
        functools.partial(body, shape),
        mesh=finer,
        in_specs=(P(None, CELLS_GRP), P(), P(), P(), P()),
        out_specs=(P(None, CELLS_GRP), P(CELLS, None)),
        check_vma=False,
    )
```

```python
import functools

import jax
import jax.numpy as jnp
from jax import lax
from jax.experimental import pallas as pl
from jax.experimental.pallas import tpu as pltpu
from jax.sharding import Mesh
from jax.sharding import PartitionSpec as P

CELLS = ("cells_0", "cells_1", "cells_2")
CELLS_GRP = ("cells_0", "cells_1", "cells_2", "grp")


diversity = 2.0
intercept_ridge = 1.0
highest = lax.Precision.HIGHEST


def split_up(array, dim, size):
    dims = array.shape
    parts = array.reshape(*dims[:dim], size, dims[dim] // size, *dims[dim + 1 :])
    return jnp.moveaxis(parts, dim, 0)


def summed_on_arrival(array, axis, dim):
    size = lax.axis_size(axis)
    parts = lax.all_to_all(split_up(array, dim, size), axis, 0, 0, tiled=True)
    return jnp.sum(parts, axis=0)


def sum_in_two_steps(array, axes, dim):
    far, near = axes
    parts = split_up(array, dim, lax.axis_size(far))
    nearer = summed_on_arrival(parts, near, dim + 1)
    arrived = lax.all_to_all(nearer, far, split_axis=0, concat_axis=0, tiled=True)
    return arrived.sum(axis=0)


def filled_up(lines, size):
    spare = -len(lines) % size
    return jnp.pad(lines, [(0, spare)] + [(0, 0)] * (lines.ndim - 1))


def sent_to_all(array, axis):
    size = lax.axis_size(axis)
    return lax.all_to_all(
        jnp.broadcast_to(array[None], (size, *array.shape)), axis, 0, 0, tiled=True
    )


def joined_along(parts, dim):
    parts = jnp.moveaxis(parts, 0, dim)
    dims = parts.shape
    return parts.reshape(*dims[:dim], dims[dim] * dims[dim + 1], *dims[dim + 2 :])


def gather_axes(array, axes, dim):
    far, near = axes
    leading = sent_to_all(array, far)
    parts = jnp.swapaxes(sent_to_all(leading, near), 0, 1)
    return joined_along(parts.reshape(-1, *array.shape), dim)


def total_of(array, axes):
    lines = array.reshape(-1)
    own = sum_in_two_steps(
        filled_up(lines, lax.axis_size(axes[0]) * lax.axis_size(axes[1])), axes, 0
    )
    whole = gather_axes(own, axes, 0)
    return whole[: len(lines)].reshape(array.shape)


def from_behind(block, axis, distance):
    devices = range(lax.axis_size(axis))
    route = [(i - distance, i) for i in devices if i - distance in devices]
    return lax.ppermute(block, axis, route)


def by_axis(array, axes):
    return functools.reduce(lax.psum, axes, array)


def observation_affinity(latent_coordinates, group_means, entropy_scaling):
    pairwise_dots = jnp.dot(
        group_means, latent_coordinates, precision=highest, preferred_element_type=jnp.float32
    )
    quadratic_lengths = jnp.sum(group_means * group_means, axis=1)
    return (2.0 * pairwise_dots - quadratic_lengths[:, None]) / (2.0 * entropy_scaling[:, None])


def probabilistic_responsibility(group_affinity):
    top = jnp.max(group_affinity, axis=0, keepdims=True)
    raised = jnp.exp(group_affinity - top)
    return raised / jnp.sum(raised, axis=0, keepdims=True)


def batch_parts(moments, ridge):
    mass = moments[:, 0, :]
    sums = moments[:, 1:, :]
    shrink = ridge[None, :] / (mass + ridge[None, :])
    weight = jnp.sum(mass * shrink, axis=1)
    right_side = jnp.sum(sums * shrink[:, None, :], axis=2)
    return (weight, right_side, jnp.sum(mass, axis=1), jnp.sum(sums, axis=2))


def slopes_of(moments, ridge, weight, right_side):
    mass = moments[:, 0, :]
    sums = moments[:, 1:, :]
    intercept = right_side / (intercept_ridge + weight)[:, None]
    return (sums - mass[:, None, :] * intercept[:, :, None]) / (mass + ridge[None, :])[:, None, :]


def wide_body(
    latent_coordinates, group_means, entropy_scaling, sample_shrinkage_lambda, sample_population
):
    local_cells = latent_coordinates.shape[1]
    num_pcs = latent_coordinates.shape[0]
    clusters = group_means.shape[0]
    batches = sample_population.shape[0]
    owned = clusters // lax.axis_size(CELLS)
    offset = (lax.axis_index(CELLS) * lax.axis_size("grp") + lax.axis_index("grp")) * local_cells
    batch_ends = jnp.cumsum(sample_population)
    batch_starts = batch_ends - sample_population
    cells_total = jnp.sum(sample_population).astype(jnp.float32)
    position = offset + lax.iota(jnp.int32, local_cells)
    batch_of = jnp.sum((batch_ends[:, None] <= position[None, :]).astype(jnp.int32), axis=0)
    first_batch = batch_of[0]
    last_batch = batch_of[local_cells - 1]
    group_affinity = observation_affinity(latent_coordinates, group_means, entropy_scaling)
    expected_occupancy = probabilistic_responsibility(group_affinity)

    def count_step(batch_id, running):
        in_batch = (batch_of == batch_id).astype(jnp.float32)
        single_observation = jnp.dot(
            expected_occupancy, in_batch, precision=highest, preferred_element_type=jnp.float32
        )
        return lax.dynamic_update_slice(
            running, single_observation[:, None], (jnp.int32(0), batch_id)
        )

    counts = lax.fori_loop(
        first_batch, last_batch + 1, count_step, jnp.zeros((clusters, batches), jnp.float32)
    )
    counts = total_of(counts, (("cells_0", "cells_1"), ("cells_2", "grp")))
    totals = jnp.sum(counts, axis=1)
    expected = sample_population.astype(jnp.float32)[None, :] * totals[:, None] / cells_total
    penalty = diversity * jnp.log((counts + 1.0) / (expected + 1.0))

    def penalty_step(batch_id, running):
        in_batch = (batch_of == batch_id).astype(jnp.float32)
        column = lax.dynamic_index_in_dim(penalty, batch_id, 1, keepdims=True)
        return running + column * in_batch[None, :]

    cell_penalty = lax.fori_loop(
        first_batch, last_batch + 1, penalty_step, jnp.zeros((clusters, local_cells), jnp.float32)
    )
    assign = probabilistic_responsibility(group_affinity - cell_penalty)
    augmented = jnp.concatenate(
        [jnp.ones((1, local_cells), jnp.float32), latent_coordinates], axis=0
    )

    def moment_step(batch_id, running):
        in_batch = (batch_of == batch_id).astype(jnp.float32)
        contiguous_portion = jnp.einsum(
            "kn,dn->kd", assign * in_batch[None, :], augmented, precision=highest
        )
        return lax.dynamic_update_slice(
            running, contiguous_portion[:, :, None], (jnp.int32(0), jnp.int32(0), batch_id)
        )

    moments = lax.fori_loop(
        first_batch,
        last_batch + 1,
        moment_step,
        jnp.zeros((clusters, num_pcs + 1, batches), jnp.float32),
    )
    devices_flat = lax.axis_size(CELLS) * lax.axis_size("grp")
    most_cells = 2 * local_cells * devices_flat // batches
    reach = (most_cells - 2) // local_cells + 1
    begins_here = (batch_starts >= offset) & (batch_starts < offset + local_cells)
    owner_mask = begins_here.astype(jnp.float32)
    head_owned = begins_here[first_batch]
    head_column = lax.dynamic_index_in_dim(moments, first_batch, 2, keepdims=False)
    sent_stats = jnp.where(head_owned, 0.0, 1.0) * head_column
    sent_tag = jnp.where(head_owned, 0.0, first_batch.astype(jnp.float32) + 1.0) * jnp.ones(
        (1,), jnp.float32
    )
    completed = moments
    for hop in range(1, reach + 1):
        got_stats, got_tag = from_behind((sent_stats, sent_tag), CELLS_GRP, -hop)
        got_id = jnp.maximum(got_tag[0].astype(jnp.int32) - 1, 0)
        accept = jnp.where((got_tag[0] > 0.5) & begins_here[got_id], 1.0, 0.0)
        single_observation = (
            lax.dynamic_index_in_dim(completed, got_id, 2, keepdims=False) + accept * got_stats
        )
        completed = lax.dynamic_update_slice(
            completed, single_observation[:, :, None], (jnp.int32(0), jnp.int32(0), got_id)
        )
    completed = completed * owner_mask[None, None, :]
    weight, right_side, mass_total, moment_total = jax.tree.map(
        lambda part: by_axis(part, CELLS_GRP), batch_parts(completed, sample_shrinkage_lambda)
    )
    coefficients = slopes_of(completed, sample_shrinkage_lambda, weight, right_side)
    every_centroid = moment_total / (1.0 + mass_total)[:, None]
    new_centroids = lax.dynamic_slice_in_dim(
        every_centroid, lax.axis_index(CELLS) * owned, owned, 0
    )
    tail_owned = begins_here[last_batch]
    tail_column = lax.dynamic_index_in_dim(coefficients, last_batch, 2, keepdims=False)
    tail_send = jnp.where(tail_owned, 1.0, 0.0) * tail_column
    tail_tag = jnp.where(tail_owned, last_batch.astype(jnp.float32) + 1.0, 0.0) * jnp.ones(
        (1,), jnp.float32
    )
    head_fix = jnp.zeros_like(tail_column)
    for hop in range(1, reach + 1):
        got_coef, got_tag = from_behind((tail_send, tail_tag), CELLS_GRP, hop)
        match = got_tag[0] == first_batch.astype(jnp.float32) + 1.0
        head_fix = jnp.where(match, got_coef, head_fix)
    own_head = lax.dynamic_index_in_dim(coefficients, first_batch, 2, keepdims=False)
    head_final = jnp.where(head_owned, own_head, head_fix)
    coefficients = lax.dynamic_update_slice(
        coefficients, head_final[:, :, None], (jnp.int32(0), jnp.int32(0), first_batch)
    )

    def correct_step(batch_id, running):
        in_batch = (batch_of == batch_id).astype(jnp.float32)
        slope_table = lax.dynamic_index_in_dim(coefficients, batch_id, 2, keepdims=False)
        moved = jnp.einsum("kd,kn->dn", slope_table, assign * in_batch[None, :], precision=highest)
        return running + moved

    corrected = lax.fori_loop(first_batch, last_batch + 1, correct_step, jnp.zeros_like(latent_coordinates))
    return (latent_coordinates - corrected, new_centroids)


SLOTS = 8
ROWS = 64
MOST = 10485
LOGICAL = pl.DeviceIdType.LOGICAL
TILE = 256
CLOSE = 4
bf16, f32 = jnp.bfloat16, jnp.float32


def two_pieces(value):
    first = value.astype(bf16)
    return first, (value - first.astype(f32)).astype(bf16)


def across(left, right):
    return lax.dot_general(left, right, (((1,), (1,)), ((), ())), preferred_element_type=f32)


def plain(left, right):
    return jnp.dot(left, right, preferred_element_type=f32)


def step_kernel(
    shape,
    cells_all,
    z_hbm,
    means_hbm,
    soft_hbm,
    ridge_hbm,
    pop_hbm,
    zf,
    pair,
    slopes,
    starts_ref,
    flag_ref,
    cent_ref,
    means_ref,
    soft_ref,
    ridge_ref,
    pop_ref,
    zc,
    ex,
    lined,
    means_wide,
    pieces,
    near_out,
    near_counts,
    near_mass,
    near_moments,
    ends_out,
    full_moments,
    line_out,
    line_a,
    line_b,
    sums_out,
    sum_in,
    cent_out,
    cent_in,
    shrinks,
    cent_y,
    cent_z,
    tile_out,
    tile_in,
    full_sums,
    small_sems,
    load_sems,
    send_sems,
    recv_sems,
):
    nz, ny, nc, nx = shape
    near = nc * nx
    far = nz * ny
    count = near * far
    cells = zf.shape[1]
    pcs, clusters = means_ref.shape
    batches = pop_ref.shape[1]
    rows_each = ROWS // near
    width = 512
    reach = (MOST - 2) // cells + 1
    offsets = [h for h in range(-reach, reach + 1) if h]
    me = (
        (lax.axis_index("cells_0") * ny + lax.axis_index("cells_1")) * nc
        + lax.axis_index("cells_2")
    ) * nx + lax.axis_index("grp")
    rank = lax.rem(me, near)
    block = lax.div(me, near)

    def mate(r):
        return block * near + lax.rem(rank + r, near)

    plane = near * ny
    in_plane = lax.rem(me, plane)

    def beside(r):
        return me - in_plane + lax.rem(in_plane + r, plane)

    def peer(r):
        return lax.rem(block + r, far) * near + rank

    def along_y(r):
        at = lax.rem(block, ny)
        return (block - at + lax.rem(at + r, ny)) * near + rank

    def along_z(r):
        return lax.rem(block + r * ny, far) * near + rank

    def neighbour(h):
        return lax.rem(me + (h + count), count)

    def push(src, dst, which, q):
        pltpu.make_async_remote_copy(
            src_ref=src,
            dst_ref=dst,
            send_sem=send_sems.at[which],
            recv_sem=recv_sems.at[which],
            device_id=q,
            device_id_type=LOGICAL,
        ).start()

    def arrived(buffer, which):
        pltpu.make_async_copy(buffer, buffer, recv_sems.at[which]).wait()

    def left(buffer, which):
        pltpu.make_async_copy(buffer, buffer, send_sems.at[which]).wait()

    small = [
        pltpu.make_async_copy(src, dst, small_sems.at[i])
        for i, (src, dst) in enumerate(
            (
                (pop_hbm, pop_ref),
                (means_hbm, means_ref),
                (soft_hbm, soft_ref),
                (ridge_hbm, ridge_ref),
            )
        )
    ]
    for copy in small:
        copy.start()
    for i in range(cells // width):
        columns = pl.ds(i * width, width)
        pltpu.make_async_copy(z_hbm.at[0, :, columns], zf.at[:, columns], load_sems.at[i]).start()

    barrier = pltpu.get_barrier_semaphore()
    greeted = [along_z(r) for r in range(1, nz)] + [beside(r) for r in range(1, plane)]
    greeted = greeted + [neighbour(h) for h in offsets]
    for q in greeted:
        pl.semaphore_signal(barrier, inc=1, device_id=q, device_id_type=LOGICAL)

    for copy in small:
        copy.wait()

    means_wide[...] = jnp.zeros_like(means_wide)
    means_wide[0:pcs, :] = means_ref[...]
    g = means_wide[...].T
    square = lax.broadcasted_iota(jnp.int32, (clusters, clusters), 0)
    lane = lax.broadcasted_iota(jnp.int32, (clusters, clusters), 1)
    soft = jnp.sum(jnp.where(square == lane, soft_ref[...], 0.0), axis=1, keepdims=True)
    offset_of = -0.5 * jnp.sum(g * g, axis=1, keepdims=True) / soft
    weights = jnp.where(lane == pcs, offset_of, g / soft)
    w1 = weights.astype(bf16).astype(f32)
    w2 = (weights - w1).astype(bf16).astype(f32)
    o1 = offset_of.astype(bf16).astype(f32)
    o2 = (offset_of - o1).astype(bf16).astype(f32)
    w1 = jnp.where(lane == pcs + 1, offset_of - o1 - o2, w1)
    w1 = (w1 + pltpu.roll(w1, ROWS, 1)).astype(bf16)
    w2 = (w2 + pltpu.roll(w2, ROWS, 1)).astype(bf16)
    weights = jnp.concatenate([w1, w2], axis=1)

    pop = pop_ref[...]
    up = lax.broadcasted_iota(jnp.int32, (batches, batches), 0)
    down = lax.broadcasted_iota(jnp.int32, (batches, batches), 1)
    column = jnp.sum(jnp.where(up == down, pop, 0), axis=1, keepdims=True)
    ends = jnp.sum(jnp.where(up <= down, column, 0), axis=0, keepdims=True)
    half = lax.broadcasted_iota(jnp.int32, (16, 1), 0)
    device = me + lax.rem(half, 8) - reach
    limit = device * cells + jnp.where(half >= 8, cells - 1, 0)
    spot = jnp.sum(jnp.where(ends <= limit, 1, 0), axis=1, keepdims=True)
    spot = jnp.where(device < 0, -9, spot)
    first = {h: spot[h + reach : h + reach + 1] for h in offsets + [0]}
    last = {h: spot[8 + h + reach : 9 + h + reach] for h in offsets + [0]}
    slot = lax.broadcasted_iota(jnp.int32, (SLOTS, 1), 0)
    batch_id = first[0] + slot
    batch_lane = lax.broadcasted_iota(jnp.int32, (SLOTS, batches), 1)
    chosen = batch_lane == batch_id
    held = jnp.sum(jnp.where(chosen, pop, 0), axis=1, keepdims=True)
    ridge = jnp.sum(jnp.where(chosen, ridge_ref[...], 0.0), axis=1, keepdims=True)
    ridge = jnp.where(batch_id < batches, ridge, 1.0)
    stop = jnp.sum(jnp.where(batch_lane <= batch_id, pop, 0), axis=1, keepdims=True) - me * cells
    start = stop - held
    held = held.astype(f32)
    starts_ref[...] = jnp.broadcast_to(jnp.where(batch_id < batches, start, 2 * cells), (SLOTS, 128))
    tail = slot == last[0] - first[0]
    head = slot == 0
    behind = {h: (last[h] == first[0]).astype(f32) for h in offsets if h < 0}
    ahead = {h: (first[h] == last[0]).astype(f32) for h in offsets if h > 0}

    wide = near - 1 + reach
    row32 = lax.broadcasted_iota(jnp.int32, (32, 1), 0)
    device = block * near + lax.rem(row32, 16) - reach
    limit = device * cells + jnp.where(row32 >= 16, cells - 1, 0)
    ids = jnp.sum(jnp.where(ends <= limit, 1, 0), axis=1, keepdims=True)
    ids = jnp.where(device < 0, -9, ids)
    limit = (block * near + lax.rem(half, 8)) * cells + jnp.where(half >= 8, cells - 1, 0)
    own_ids = jnp.sum(jnp.where(ends <= limit, 1, 0), axis=1, keepdims=True)
    own_lane = lax.broadcasted_iota(jnp.int32, (16, batches), 1)
    own_ridge = jnp.sum(jnp.where(own_lane == own_ids, ridge_ref[...], 0.0), axis=1, keepdims=True)

    crowded = jnp.zeros((1, 1), jnp.int32)
    for inner, room in ((SLOTS - 1, cells), (CLOSE - 1, width)):
        window = jnp.sum(
            jnp.where((up >= down) & (up < down + inner), column, 0), axis=0, keepdims=True
        )
        window = jnp.where((window < room - 1) & (batch_lane[0:1] <= batches - inner), 1, 0)
        crowded = crowded + jnp.sum(window, axis=1, keepdims=True)
    flag_ref[...] = jnp.broadcast_to(crowded, (1, 128))

    def inside(c, width, times):
        position = lax.broadcasted_iota(jnp.int32, (SLOTS * times, width), 1) + c * width
        low = jnp.concatenate([start] * times, axis=0)
        high = jnp.concatenate([stop] * times, axis=0)
        return ((position >= low) & (position < high)).astype(f32)

    def completed(own, buffer):
        before = jnp.zeros((1, clusters), f32)
        after = jnp.zeros((1, clusters), f32)
        for i, h in enumerate(offsets):
            if h < 0:
                before = before + behind[h] * buffer[i][1:2]
            else:
                after = after + ahead[h] * buffer[i][0:1]
        return own + jnp.where(head, before, 0.0) + jnp.where(tail, after, 0.0)

    def tail_of(value):
        return jnp.sum(jnp.where(tail, value, 0.0), axis=0, keepdims=True)

    def greeted_rows(which, value):
        near_out[which, 0:1, :] = value[0:1]
        near_out[which, 1:2, :] = tail_of(value)

    runs = cells // width

    def base_of(c):
        return jnp.sum(
            jnp.where((start <= c * width) & (slot > 0) & (batch_id < batches), 1, 0),
            axis=0,
            keepdims=True,
        )


    def prior_step(c, total):
        columns = pl.ds(pl.multiple_of(c * width, width), width)
        pltpu.make_async_copy(z_hbm.at[0, :, columns], zf.at[:, columns], load_sems.at[c]).wait()
        z1, z2 = two_pieces(
            jnp.concatenate(
                [
                    zf[:, columns],
                    jnp.ones((2, width), f32),
                    jnp.zeros((ROWS - 2 - pcs, width), f32),
                ],
                axis=0,
            )
        )
        zc[0:ROWS, columns] = z1
        zc[ROWS : 2 * ROWS, columns] = z2
        score = plain(weights, jnp.concatenate([z1, z2, z1, z2], axis=0))
        raised = jnp.exp(score - jnp.max(score, axis=0, keepdims=True))
        ex[:, columns] = raised
        p1, p2 = two_pieces(raised * (1.0 / jnp.sum(raised, axis=0, keepdims=True)))
        mask = inside(c, width, 2).astype(bf16)
        return total + across(mask, jnp.concatenate([p1, p2], axis=0))

    total = lax.fori_loop(
        0, cells // width, prior_step, jnp.zeros((2 * SLOTS, 2 * clusters), f32)
    )
    counts = total[0:SLOTS, 0:clusters] + total[0:SLOTS, clusters : 2 * clusters]
    own_total = jnp.sum(counts, axis=0, keepdims=True)
    greeted_rows(0, counts)
    line_out[0] = own_total
    pl.semaphore_wait(barrier, len(greeted))
    for r in range(1, plane):
        push(line_out.at[0], line_a.at[r - 1], 0, beside(r))
    for i, h in enumerate(offsets):
        push(near_out.at[0], near_counts.at[len(offsets) - 1 - i], 1, neighbour(h))

    def line_step(c, carry):
        columns = pl.ds(pl.multiple_of(c * width, width), width)
        mask = inside(c, width, 1)
        kind = jnp.sum(mask * slot.astype(f32), axis=0, keepdims=True)
        kind = kind - base_of(c).astype(f32)
        z = zc[:, columns]
        for j in range(CLOSE):
            lined[2 * ROWS * j : 2 * ROWS * (j + 1), columns] = z * (kind == j).astype(
                f32
            ).astype(bf16)
        return carry

    lax.fori_loop(0, runs // 2, line_step, 0)
    arrived(line_a, 0)
    plane_total = own_total + jnp.sum(line_a[...], axis=0)
    line_out[1] = plane_total
    for r in range(1, nz):
        push(line_out.at[1], line_b.at[r - 1], 2, along_z(r))
    lax.fori_loop(runs // 2, runs, line_step, 0)
    arrived(near_counts, 1)
    full_counts = completed(counts, [near_counts[i] for i in range(len(offsets))])
    arrived(line_b, 2)
    totals = plane_total + jnp.sum(line_b[...], axis=0)
    expected = held * totals * (1.0 / cells_all)
    ratio = (expected + 1.0) / (full_counts + 1.0)
    factor = ratio * ratio
    f1 = factor.astype(bf16).astype(f32)
    f2 = (factor - f1).astype(bf16).astype(f32)
    f3 = factor - f1 - f2
    factor = jnp.concatenate([f1, f2, f3, jnp.zeros_like(f3)], axis=0).T.astype(bf16)

    def assign_step(c, total):
        columns = pl.ds(pl.multiple_of(c * width, width), width)
        mask = inside(c, width, 4).astype(bf16)
        weighed = ex[:, columns] * plain(factor, mask)
        a1, a2 = two_pieces(weighed * (1.0 / jnp.sum(weighed, axis=0, keepdims=True)))
        both = jnp.concatenate([a1, a2], axis=0)
        pair[:, columns] = both
        return total + across(mask[0 : 2 * SLOTS], both)

    total = lax.fori_loop(0, runs, assign_step, jnp.zeros((2 * SLOTS, 2 * clusters), f32))
    mass = total[0:SLOTS, 0:clusters] + total[0:SLOTS, clusters : 2 * clusters]
    greeted_rows(1, mass)
    around = 2 * wide + 1
    for h in range(1, wide + 1):
        push(near_out.at[1], near_mass.at[(around - 1 - h) % around], 3, neighbour(h))
        push(near_out.at[1], near_mass.at[(around - 1 + h) % around], 3, neighbour(-h))
    near_mass[around - 1] = near_out[1]

    def moment_step(c, carry):
        columns = pl.ds(pl.multiple_of(c * width, width), width)
        value = across(lined[:, columns], pair[:, columns])
        for j in range(CLOSE):
            top = value[2 * ROWS * j : 2 * ROWS * j + ROWS]
            low = value[2 * ROWS * j + ROWS : 2 * ROWS * (j + 1)]
            pieces[c, j] = (
                top[:, 0:clusters] + top[:, clusters:] + low[:, 0:clusters] + low[:, clusters:]
            )
        return carry

    lax.fori_loop(0, runs, moment_step, 0)
    places = [(c, j) for c in range(runs) for j in range(CLOSE)]
    tail_slot = last[0] - first[0]
    alone = jnp.where(tail_slot > 0, 1.0, 0.0)
    shrink = jnp.where(head | tail, 0.0, ridge / (mass + ridge))
    first_moment = jnp.zeros((ROWS, clusters), f32)
    tail_moment = jnp.zeros((ROWS, clusters), f32)
    whole = jnp.zeros((ROWS, clusters), f32)
    right = jnp.zeros((ROWS, clusters), f32)
    for c in range(runs):
        base = base_of(c)
        for j in range(CLOSE):
            piece = pieces[c, j]
            line = jnp.sum(jnp.where(slot == base + j, shrink, 0.0), axis=0, keepdims=True)
            right = right + line * piece
            tail_moment = tail_moment + jnp.where(base + j == tail_slot, 1.0, 0.0) * piece
            whole = whole + piece
            if j == 0:
                first_moment = first_moment + jnp.where(base == 0, 1.0, 0.0) * piece
    for t in range(near):
        inner = slice(t * rows_each, (t + 1) * rows_each)
        sums_out[t, 0] = right[inner]
        sums_out[t, 1] = first_moment[inner]
        sums_out[t, 2] = tail_moment[inner] * alone
        cent_out[t] = whole[inner]
    for r in range(1, near):
        push(sums_out.at[lax.rem(rank + r, near)], sum_in.at[r - 1], 5, mate(r))
    for r in range(1, near):
        push(cent_out.at[lax.rem(rank + r, near)], cent_in.at[r - 1], 4, mate(r))
    ends_out[0] = first_moment[0:56]
    ends_out[1] = tail_moment[0:56]
    arrived(near_mass.at[pl.ds(0, around - 1)], 3)
    full_mass = completed(
        mass, {i: near_mass[(around - 1 + h) % around] for i, h in enumerate(offsets)}
    )
    end_mass = jnp.zeros((16, clusters), f32)
    for p in range(-reach, near + reach):
        both = near_mass[lax.rem(p + (2 * around - 1) - rank, around)]
        one, two = ids[p + reach : p + reach + 1], ids[16 + p + reach : 17 + p + reach]
        end_mass = end_mass + jnp.where(own_ids == one, both[0:1], 0.0)
        end_mass = end_mass + jnp.where((own_ids == two) & (two != one), both[1:2], 0.0)
    end_shrink = own_ridge / (end_mass + own_ridge)
    for t in range(near):
        shrinks[t, 0:1, :] = end_shrink[t : t + 1]
        shrinks[t, 1:2, :] = end_shrink[8 + t : 9 + t]
    arrived(sum_in, 5)
    sum_tile = jnp.zeros((rows_each, clusters), f32)
    for r in range(near):
        by = shrinks[lax.rem(rank + near - r, near)]
        got = sums_out[rank] if r == 0 else sum_in[r - 1]
        sum_tile = sum_tile + got[0] + got[1] * by[0:1] + got[2] * by[1:2]
    tile_out[2] = sum_tile
    for r in range(1, far):
        push(tile_out.at[2], tile_in.at[r - 1], 8, peer(r))
    for i, h in enumerate(offsets):
        push(ends_out.at[int(h > 0)], near_moments.at[len(offsets) - 1 - i], 6, neighbour(h))
    arrived(cent_in, 4)
    cent_tile = cent_out[rank]
    for r in range(near - 1):
        cent_tile = cent_tile + cent_in[r]
    tile_out[0] = cent_tile
    for r in range(1, ny):
        push(tile_out.at[0], cent_y.at[r - 1], 7, along_y(r))
    arrived(cent_y, 7)
    for r in range(ny - 1):
        cent_tile = cent_tile + cent_y[r]
    tile_out[1] = cent_tile
    for r in range(1, nz):
        push(tile_out.at[1], cent_z.at[r - 1], 11, along_z(r))
    moments = []
    for s in range(SLOTS):
        moment = jnp.zeros((ROWS, clusters), f32)
        for c, j in places:
            if j <= s <= CLOSE * c + j:
                moment = moment + jnp.where(base_of(c) + j == s, 1.0, 0.0) * pieces[c, j]
        moments.append(moment)

    arrived(near_moments, 6)
    before = jnp.zeros((56, clusters), f32)
    after = jnp.zeros((56, clusters), f32)
    for i, h in enumerate(offsets):
        if h < 0:
            before = before + behind[h] * near_moments[i]
        else:
            after = after + ahead[h] * near_moments[i]
    for s in range(SLOTS):
        moment = moments[s][0:56] + after * tail[s : s + 1].astype(f32)
        full_moments[s] = moment + before if s == 0 else moment

    arrived(tile_in, 8)
    full_sums[1, 0] = sum_tile + jnp.sum(tile_in[...], axis=0)
    for r in range(1, near):
        push(full_sums.at[1, 0], full_sums.at[1, r], 10, mate(r))
    arrived(cent_z, 11)
    for r in range(nz - 1):
        cent_tile = cent_tile + cent_z[r]
    full_sums[0, 0] = cent_tile
    for r in range(1, near):
        push(full_sums.at[0, 0], full_sums.at[0, r], 9, mate(r))

    def gathered(which):
        return jnp.concatenate(
            [full_sums[which, lax.rem(rank + (near - t), near)] for t in range(near)], axis=0
        )

    arrived(full_sums.at[1, pl.ds(1, near - 1)], 10)
    right = gathered(1)
    intercept = (right / (1.0 + right[pcs : pcs + 1]))[0:56]
    for s in range(SLOTS):
        moment = full_moments[s]
        line = full_mass[s : s + 1]
        slope = (moment - line * intercept) / (line + ridge[s : s + 1])
        c1, c2 = two_pieces(jnp.concatenate([slope, jnp.zeros((8, clusters), f32)], axis=0))
        slopes[ROWS * s : ROWS * (s + 1), :] = jnp.concatenate([c1, c1, c2], axis=1)

    arrived(full_sums.at[0, pl.ds(1, near - 1)], 9)
    centre = gathered(0)
    centre = (centre / (1.0 + centre[pcs : pcs + 1])).T
    owned = cent_ref.shape[0]
    cells_at = lax.div(me, nx)
    row = lax.broadcasted_iota(jnp.int32, (clusters, ROWS), 0)
    for j in range(owned):
        line = jnp.sum(jnp.where(row == cells_at * owned + j, centre, 0.0), axis=0, keepdims=True)
        cent_ref[j : j + 1, :] = line[:, 0:pcs]

    left(line_a, 0)
    left(near_counts, 1)
    left(line_b, 2)
    left(near_mass.at[pl.ds(0, around - 1)], 3)
    left(cent_in, 4)
    left(sum_in, 5)
    left(near_moments, 6)
    left(cent_y, 7)
    left(tile_in, 8)
    left(cent_z, 11)
    left(full_sums.at[0, pl.ds(1, near - 1)], 9)
    left(full_sums.at[1, pl.ds(1, near - 1)], 10)


def correct_kernel(
    zf, pair, slopes, starts_ref, cent_ref, out_hbm, cent_hbm, held, starts, out_sems
):
    pcs, cells = zf.shape
    clusters = pair.shape[0] // 2
    loads = out_sems.shape[0] - 1
    part = cells // loads
    cent = pltpu.make_async_copy(cent_ref, cent_hbm, out_sems.at[loads])
    cent.start()
    begin = [jnp.max(starts_ref[s : s + 1, :]) for s in range(SLOTS)]
    for s in range(SLOTS):
        starts[s] = begin[s]
    outs = []
    lane = lax.broadcasted_iota(jnp.int32, (1, TILE), 1)

    def slope_of(j):
        return slopes[pl.ds(pl.multiple_of(j * ROWS, ROWS), ROWS), :]

    for i in range(loads):
        beyond = jnp.int32(0)
        for t in range(i * part // TILE, (i + 1) * part // TILE):
            columns = slice(t * TILE, (t + 1) * TILE)
            base = jnp.int32(0)
            final = jnp.int32(0)
            border = jnp.int32(2 * cells)
            for s in range(1, SLOTS):
                base = base + jnp.where(begin[s] <= t * TILE, 1, 0)
                final = final + jnp.where(begin[s] < (t + 1) * TILE, 1, 0)
                border = jnp.where(begin[s] > t * TILE, jnp.minimum(border, begin[s]), border)
            beyond = jnp.maximum(beyond, final - base)
            following = jnp.minimum(base + 1, SLOTS - 1)
            both = pair[:, columns]
            both = jnp.concatenate([both, both[0:clusters]], axis=0)
            moved = plain(jnp.concatenate([slope_of(base), slope_of(following)], axis=0), both)
            moved = jnp.where(lane < border - t * TILE, moved[0:ROWS], moved[ROWS:])
            held[:, columns] = zf[:, columns] - moved[0:pcs]

        @pl.when(beyond > 1)
        def _():
            def tile_of(t, carry):
                columns = pl.ds(pl.multiple_of(t * TILE, TILE), TILE)
                base = jnp.int32(0)
                final = jnp.int32(0)
                for s in range(1, SLOTS):
                    base = base + jnp.where(begin[s] <= t * TILE, 1, 0)
                    final = final + jnp.where(begin[s] < (t + 1) * TILE, 1, 0)

                def more(j, carry):
                    both = pair[:, columns]
                    both = jnp.concatenate([both, both[0:clusters]], axis=0)
                    other = zf[:, columns] - plain(slope_of(j), both)[0:pcs]
                    held[:, columns] = jnp.where(
                        lane >= starts[j] - t * TILE, other, held[:, columns]
                    )
                    return carry

                lax.fori_loop(base + 2, final + 1, more, 0)
                return carry

            lax.fori_loop(i * part // TILE, (i + 1) * part // TILE, tile_of, 0)

        columns = pl.ds(i * part, part)
        outs.append(pltpu.make_async_copy(held.at[:, columns], out_hbm.at[:, columns], out_sems.at[i]))
        outs[-1].start()
    for copy in outs:
        copy.wait()
    cent.wait()


def narrow_body(
    shape, latent_coordinates, group_means, entropy_scaling, sample_shrinkage_lambda, sample_population
):
    pcs, cells = latent_coordinates.shape
    clusters = group_means.shape[0]
    batches = sample_population.shape[0]
    nz, ny, nc, nx = shape
    near, far = nc * nx, nz * ny
    rows_each = ROWS // near
    reach = (MOST - 2) // cells + 1
    owned = clusters // (nz * ny * nc)
    vmem = pl.BlockSpec(memory_space=pltpu.VMEM)
    tile = (rows_each, clusters)
    scratch = [
        pltpu.VMEM((pcs, clusters), f32),
        pltpu.VMEM((1, clusters), f32),
        pltpu.VMEM((1, batches), f32),
        pltpu.VMEM((1, batches), jnp.int32),
        pltpu.VMEM((2 * ROWS, cells), bf16),
        pltpu.VMEM((clusters, cells), f32),
        pltpu.VMEM((2 * ROWS * CLOSE, cells), bf16),
        pltpu.VMEM((clusters, clusters), f32),
        pltpu.VMEM((cells // 512, CLOSE, ROWS, clusters), f32),
        pltpu.VMEM((2, 2, clusters), f32),
        pltpu.VMEM((2 * reach, 2, clusters), f32),
        pltpu.VMEM((2 * (near - 1 + reach) + 1, 2, clusters), f32),
        pltpu.VMEM((2 * reach, 56, clusters), f32),
        pltpu.VMEM((2, 56, clusters), f32),
        pltpu.VMEM((SLOTS, 56, clusters), f32),
        pltpu.VMEM((2, 1, clusters), f32),
        pltpu.VMEM((near * ny - 1, 1, clusters), f32),
        pltpu.VMEM((nz - 1, 1, clusters), f32),
        pltpu.VMEM((near, 3, *tile), f32),
        pltpu.VMEM((near - 1, 3, *tile), f32),
        pltpu.VMEM((near, *tile), f32),
        pltpu.VMEM((near - 1, *tile), f32),
        pltpu.VMEM((near, 2, clusters), f32),
        pltpu.VMEM((ny - 1, *tile), f32),
        pltpu.VMEM((nz - 1, *tile), f32),
        pltpu.VMEM((3, *tile), f32),
        pltpu.VMEM((far - 1, *tile), f32),
        pltpu.VMEM((2, near, *tile), f32),
        pltpu.SemaphoreType.DMA((4,)),
        pltpu.SemaphoreType.DMA((cells // 512,)),
        pltpu.SemaphoreType.DMA((12,)),
        pltpu.SemaphoreType.DMA((12,)),
    ]
    return pl.pallas_call(
        functools.partial(step_kernel, shape, float(cells * near * far)),
        out_shape=(
            pltpu.VMEM((pcs, cells), f32),
            pltpu.VMEM((2 * clusters, cells), bf16),
            pltpu.VMEM((SLOTS * ROWS, 3 * clusters), bf16),
            pltpu.VMEM((SLOTS, 128), jnp.int32),
            pltpu.VMEM((1, 128), jnp.int32),
            pltpu.VMEM((owned, pcs), f32),
        ),
        in_specs=[pl.BlockSpec(memory_space=pl.ANY)] * 5,
        out_specs=(vmem,) * 6,
        scratch_shapes=scratch,
        compiler_params=pltpu.CompilerParams(
            collective_id=0, has_side_effects=True, vmem_limit_bytes=24 * 1024 * 1024
        ),
    )(
        latent_coordinates[None],
        group_means.T,
        entropy_scaling.reshape(1, clusters),
        sample_shrinkage_lambda.reshape(1, batches),
        sample_population.reshape(1, batches),
    )


def corrected_by(kept, pair, slopes, starts, new_centroids):
    pcs, cells = kept.shape
    vmem = pl.BlockSpec(memory_space=pltpu.VMEM)
    anywhere = pl.BlockSpec(memory_space=pl.ANY)
    return pl.pallas_call(
        correct_kernel,
        out_shape=(pltpu.HBM((pcs, cells), f32), pltpu.HBM(new_centroids.shape, f32)),
        in_specs=[vmem] * 5,
        out_specs=(anywhere, anywhere),
        scratch_shapes=[
            pltpu.VMEM((pcs, cells), f32),
            pltpu.SMEM((SLOTS,), jnp.int32),
            pltpu.SemaphoreType.DMA((5,)),
        ],
        compiler_params=pltpu.CompilerParams(vmem_limit_bytes=16 * 1024 * 1024),
    )(
        kept,
        pair,
        slopes,
        starts,
        new_centroids,
    )


def body(
    shape, latent_coordinates, group_means, entropy_scaling, sample_shrinkage_lambda, sample_population
):
    arguments = (
        latent_coordinates,
        group_means,
        entropy_scaling,
        sample_shrinkage_lambda,
        sample_population,
    )
    kept, pair, slopes, starts, flag, new_centroids = narrow_body(shape, *arguments)
    return lax.cond(
        flag[0, 0] == 0,
        lambda: corrected_by(kept, pair, slopes, starts, new_centroids),
        lambda: wide_body(*arguments),
    )


def solution(mesh):
    shape = (mesh.shape["cells"] // 8, 4, 2, mesh.shape["grp"])
    finer = Mesh(mesh.devices.reshape(shape), ("cells_0", "cells_1", "cells_2", "grp"))
    return jax.shard_map(
        functools.partial(body, shape),
        mesh=finer,
        in_specs=(P(None, CELLS_GRP), P(), P(), P(), P()),
        out_specs=(P(None, CELLS_GRP), P(CELLS, None)),
        check_vma=False,
    )
```

```python
import functools

import jax
import jax.numpy as jnp
from jax import lax
from jax.experimental import pallas as pl
from jax.experimental.pallas import tpu as pltpu
from jax.sharding import Mesh
from jax.sharding import PartitionSpec as P

CELLS = ("cells_0", "cells_1", "cells_2")
CELLS_GRP = ("cells_0", "cells_1", "cells_2", "grp")


diversity = 2.0
intercept_ridge = 1.0
highest = lax.Precision.HIGHEST


def split_up(array, dim, size):
    dims = array.shape
    parts = array.reshape(*dims[:dim], size, dims[dim] // size, *dims[dim + 1 :])
    return jnp.moveaxis(parts, dim, 0)


def summed_on_arrival(array, axis, dim):
    size = lax.axis_size(axis)
    parts = lax.all_to_all(split_up(array, dim, size), axis, 0, 0, tiled=True)
    return jnp.sum(parts, axis=0)


def sum_in_two_steps(array, axes, dim):
    far, near = axes
    parts = split_up(array, dim, lax.axis_size(far))
    nearer = summed_on_arrival(parts, near, dim + 1)
    arrived = lax.all_to_all(nearer, far, split_axis=0, concat_axis=0, tiled=True)
    return arrived.sum(axis=0)


def filled_up(lines, size):
    spare = -len(lines) % size
    return jnp.pad(lines, [(0, spare)] + [(0, 0)] * (lines.ndim - 1))


def sent_to_all(array, axis):
    size = lax.axis_size(axis)
    return lax.all_to_all(
        jnp.broadcast_to(array[None], (size, *array.shape)), axis, 0, 0, tiled=True
    )


def joined_along(parts, dim):
    parts = jnp.moveaxis(parts, 0, dim)
    dims = parts.shape
    return parts.reshape(*dims[:dim], dims[dim] * dims[dim + 1], *dims[dim + 2 :])


def gather_axes(array, axes, dim):
    far, near = axes
    leading = sent_to_all(array, far)
    parts = jnp.swapaxes(sent_to_all(leading, near), 0, 1)
    return joined_along(parts.reshape(-1, *array.shape), dim)


def total_of(array, axes):
    lines = array.reshape(-1)
    own = sum_in_two_steps(
        filled_up(lines, lax.axis_size(axes[0]) * lax.axis_size(axes[1])), axes, 0
    )
    whole = gather_axes(own, axes, 0)
    return whole[: len(lines)].reshape(array.shape)


def from_behind(block, axis, distance):
    devices = range(lax.axis_size(axis))
    route = [(i - distance, i) for i in devices if i - distance in devices]
    return lax.ppermute(block, axis, route)


def by_axis(array, axes):
    return functools.reduce(lax.psum, axes, array)


def observation_affinity(latent_coordinates, group_means, entropy_scaling):
    pairwise_dots = jnp.dot(
        group_means, latent_coordinates, precision=highest, preferred_element_type=jnp.float32
    )
    quadratic_lengths = jnp.sum(group_means * group_means, axis=1)
    return (2.0 * pairwise_dots - quadratic_lengths[:, None]) / (2.0 * entropy_scaling[:, None])


def probabilistic_responsibility(group_affinity):
    top = jnp.max(group_affinity, axis=0, keepdims=True)
    raised = jnp.exp(group_affinity - top)
    return raised / jnp.sum(raised, axis=0, keepdims=True)


def batch_parts(moments, ridge):
    mass = moments[:, 0, :]
    sums = moments[:, 1:, :]
    shrink = ridge[None, :] / (mass + ridge[None, :])
    weight = jnp.sum(mass * shrink, axis=1)
    right_side = jnp.sum(sums * shrink[:, None, :], axis=2)
    return (weight, right_side, jnp.sum(mass, axis=1), jnp.sum(sums, axis=2))


def slopes_of(moments, ridge, weight, right_side):
    mass = moments[:, 0, :]
    sums = moments[:, 1:, :]
    intercept = right_side / (intercept_ridge + weight)[:, None]
    return (sums - mass[:, None, :] * intercept[:, :, None]) / (mass + ridge[None, :])[:, None, :]


def wide_body(
    latent_coordinates, group_means, entropy_scaling, sample_shrinkage_lambda, sample_population
):
    local_cells = latent_coordinates.shape[1]
    num_pcs = latent_coordinates.shape[0]
    clusters = group_means.shape[0]
    batches = sample_population.shape[0]
    owned = clusters // lax.axis_size(CELLS)
    offset = (lax.axis_index(CELLS) * lax.axis_size("grp") + lax.axis_index("grp")) * local_cells
    batch_ends = jnp.cumsum(sample_population)
    batch_starts = batch_ends - sample_population
    cells_total = jnp.sum(sample_population).astype(jnp.float32)
    position = offset + lax.iota(jnp.int32, local_cells)
    batch_of = jnp.sum((batch_ends[:, None] <= position[None, :]).astype(jnp.int32), axis=0)
    first_batch = batch_of[0]
    last_batch = batch_of[local_cells - 1]
    group_affinity = observation_affinity(latent_coordinates, group_means, entropy_scaling)
    expected_occupancy = probabilistic_responsibility(group_affinity)

    def count_step(batch_id, running):
        in_batch = (batch_of == batch_id).astype(jnp.float32)
        single_observation = jnp.dot(
            expected_occupancy, in_batch, precision=highest, preferred_element_type=jnp.float32
        )
        return lax.dynamic_update_slice(
            running, single_observation[:, None], (jnp.int32(0), batch_id)
        )

    counts = lax.fori_loop(
        first_batch, last_batch + 1, count_step, jnp.zeros((clusters, batches), jnp.float32)
    )
    counts = total_of(counts, (("cells_0", "cells_1"), ("cells_2", "grp")))
    totals = jnp.sum(counts, axis=1)
    expected = sample_population.astype(jnp.float32)[None, :] * totals[:, None] / cells_total
    penalty = diversity * jnp.log((counts + 1.0) / (expected + 1.0))

    def penalty_step(batch_id, running):
        in_batch = (batch_of == batch_id).astype(jnp.float32)
        column = lax.dynamic_index_in_dim(penalty, batch_id, 1, keepdims=True)
        return running + column * in_batch[None, :]

    cell_penalty = lax.fori_loop(
        first_batch, last_batch + 1, penalty_step, jnp.zeros((clusters, local_cells), jnp.float32)
    )
    assign = probabilistic_responsibility(group_affinity - cell_penalty)
    augmented = jnp.concatenate(
        [jnp.ones((1, local_cells), jnp.float32), latent_coordinates], axis=0
    )

    def moment_step(batch_id, running):
        in_batch = (batch_of == batch_id).astype(jnp.float32)
        contiguous_portion = jnp.einsum(
            "kn,dn->kd", assign * in_batch[None, :], augmented, precision=highest
        )
        return lax.dynamic_update_slice(
            running, contiguous_portion[:, :, None], (jnp.int32(0), jnp.int32(0), batch_id)
        )

    moments = lax.fori_loop(
        first_batch,
        last_batch + 1,
        moment_step,
        jnp.zeros((clusters, num_pcs + 1, batches), jnp.float32),
    )
    devices_flat = lax.axis_size(CELLS) * lax.axis_size("grp")
    most_cells = 2 * local_cells * devices_flat // batches
    reach = (most_cells - 2) // local_cells + 1
    begins_here = (batch_starts >= offset) & (batch_starts < offset + local_cells)
    owner_mask = begins_here.astype(jnp.float32)
    head_owned = begins_here[first_batch]
    head_column = lax.dynamic_index_in_dim(moments, first_batch, 2, keepdims=False)
    sent_stats = jnp.where(head_owned, 0.0, 1.0) * head_column
    sent_tag = jnp.where(head_owned, 0.0, first_batch.astype(jnp.float32) + 1.0) * jnp.ones(
        (1,), jnp.float32
    )
    completed = moments
    for hop in range(1, reach + 1):
        got_stats, got_tag = from_behind((sent_stats, sent_tag), CELLS_GRP, -hop)
        got_id = jnp.maximum(got_tag[0].astype(jnp.int32) - 1, 0)
        accept = jnp.where((got_tag[0] > 0.5) & begins_here[got_id], 1.0, 0.0)
        single_observation = (
            lax.dynamic_index_in_dim(completed, got_id, 2, keepdims=False) + accept * got_stats
        )
        completed = lax.dynamic_update_slice(
            completed, single_observation[:, :, None], (jnp.int32(0), jnp.int32(0), got_id)
        )
    completed = completed * owner_mask[None, None, :]
    weight, right_side, mass_total, moment_total = jax.tree.map(
        lambda part: by_axis(part, CELLS_GRP), batch_parts(completed, sample_shrinkage_lambda)
    )
    coefficients = slopes_of(completed, sample_shrinkage_lambda, weight, right_side)
    every_centroid = moment_total / (1.0 + mass_total)[:, None]
    new_centroids = lax.dynamic_slice_in_dim(
        every_centroid, lax.axis_index(CELLS) * owned, owned, 0
    )
    tail_owned = begins_here[last_batch]
    tail_column = lax.dynamic_index_in_dim(coefficients, last_batch, 2, keepdims=False)
    tail_send = jnp.where(tail_owned, 1.0, 0.0) * tail_column
    tail_tag = jnp.where(tail_owned, last_batch.astype(jnp.float32) + 1.0, 0.0) * jnp.ones(
        (1,), jnp.float32
    )
    head_fix = jnp.zeros_like(tail_column)
    for hop in range(1, reach + 1):
        got_coef, got_tag = from_behind((tail_send, tail_tag), CELLS_GRP, hop)
        match = got_tag[0] == first_batch.astype(jnp.float32) + 1.0
        head_fix = jnp.where(match, got_coef, head_fix)
    own_head = lax.dynamic_index_in_dim(coefficients, first_batch, 2, keepdims=False)
    head_final = jnp.where(head_owned, own_head, head_fix)
    coefficients = lax.dynamic_update_slice(
        coefficients, head_final[:, :, None], (jnp.int32(0), jnp.int32(0), first_batch)
    )

    def correct_step(batch_id, running):
        in_batch = (batch_of == batch_id).astype(jnp.float32)
        slope_table = lax.dynamic_index_in_dim(coefficients, batch_id, 2, keepdims=False)
        moved = jnp.einsum("kd,kn->dn", slope_table, assign * in_batch[None, :], precision=highest)
        return running + moved

    corrected = lax.fori_loop(first_batch, last_batch + 1, correct_step, jnp.zeros_like(latent_coordinates))
    return (latent_coordinates - corrected, new_centroids)


SLOTS = 8
ROWS = 64
MOST = 10485
LOGICAL = pl.DeviceIdType.LOGICAL
TILE = 256
CLOSE = 4
bf16, f32 = jnp.bfloat16, jnp.float32


def two_pieces(value):
    first = value.astype(bf16)
    return first, (value - first.astype(f32)).astype(bf16)


def across(left, right):
    return lax.dot_general(left, right, (((1,), (1,)), ((), ())), preferred_element_type=f32)


def plain(left, right):
    return jnp.dot(left, right, preferred_element_type=f32)


def step_kernel(
    shape,
    cells_all,
    z_hbm,
    means_hbm,
    soft_hbm,
    ridge_hbm,
    pop_hbm,
    zf,
    pair,
    slopes,
    starts_ref,
    flag_ref,
    cent_ref,
    means_ref,
    soft_ref,
    ridge_ref,
    pop_ref,
    zc,
    ex,
    lined,
    means_wide,
    pieces,
    near_out,
    near_counts,
    near_mass,
    near_moments,
    ends_out,
    full_moments,
    line_out,
    line_a,
    line_b,
    sums_out,
    sum_in,
    cent_out,
    cent_in,
    shrinks,
    cent_y,
    cent_z,
    tile_out,
    tile_in,
    full_sums,
    small_sems,
    load_sems,
    send_sems,
    recv_sems,
):
    nz, ny, nc, nx = shape
    near = nc * nx
    far = nz * ny
    count = near * far
    cells = zf.shape[1]
    pcs, clusters = means_ref.shape
    batches = pop_ref.shape[1]
    rows_each = ROWS // near
    width = 512
    reach = (MOST - 2) // cells + 1
    offsets = [h for h in range(-reach, reach + 1) if h]
    me = (
        (lax.axis_index("cells_0") * ny + lax.axis_index("cells_1")) * nc
        + lax.axis_index("cells_2")
    ) * nx + lax.axis_index("grp")
    rank = lax.rem(me, near)
    block = lax.div(me, near)

    def mate(r):
        return block * near + lax.rem(rank + r, near)

    plane = near * ny
    in_plane = lax.rem(me, plane)

    def beside(r):
        return me - in_plane + lax.rem(in_plane + r, plane)

    def peer(r):
        return lax.rem(block + r, far) * near + rank

    def along_y(r):
        at = lax.rem(block, ny)
        return (block - at + lax.rem(at + r, ny)) * near + rank

    def along_z(r):
        return lax.rem(block + r * ny, far) * near + rank

    def neighbour(h):
        return lax.rem(me + (h + count), count)

    def push(src, dst, which, q):
        pltpu.make_async_remote_copy(
            src_ref=src,
            dst_ref=dst,
            send_sem=send_sems.at[which],
            recv_sem=recv_sems.at[which],
            device_id=q,
            device_id_type=LOGICAL,
        ).start()

    def arrived(buffer, which):
        pltpu.make_async_copy(buffer, buffer, recv_sems.at[which]).wait()

    def left(buffer, which):
        pltpu.make_async_copy(buffer, buffer, send_sems.at[which]).wait()

    small = [
        pltpu.make_async_copy(src, dst, small_sems.at[i])
        for i, (src, dst) in enumerate(
            (
                (pop_hbm, pop_ref),
                (means_hbm, means_ref),
                (soft_hbm, soft_ref),
                (ridge_hbm, ridge_ref),
            )
        )
    ]
    for copy in small:
        copy.start()
    for i in range(cells // width):
        columns = pl.ds(i * width, width)
        pltpu.make_async_copy(z_hbm.at[0, :, columns], zf.at[:, columns], load_sems.at[i]).start()

    barrier = pltpu.get_barrier_semaphore()
    greeted = [along_z(r) for r in range(1, nz)] + [beside(r) for r in range(1, plane)]
    greeted = greeted + [neighbour(h) for h in offsets]
    for q in greeted:
        pl.semaphore_signal(barrier, inc=1, device_id=q, device_id_type=LOGICAL)

    for copy in small:
        copy.wait()

    means_wide[...] = jnp.zeros_like(means_wide)
    means_wide[0:pcs, :] = means_ref[...]
    g = means_wide[...].T
    square = lax.broadcasted_iota(jnp.int32, (clusters, clusters), 0)
    lane = lax.broadcasted_iota(jnp.int32, (clusters, clusters), 1)
    soft = jnp.sum(jnp.where(square == lane, soft_ref[...], 0.0), axis=1, keepdims=True)
    offset_of = -0.5 * jnp.sum(g * g, axis=1, keepdims=True) / soft
    weights = jnp.where(lane == pcs, offset_of, g / soft)
    w1 = weights.astype(bf16).astype(f32)
    w2 = (weights - w1).astype(bf16).astype(f32)
    o1 = offset_of.astype(bf16).astype(f32)
    o2 = (offset_of - o1).astype(bf16).astype(f32)
    w1 = jnp.where(lane == pcs + 1, offset_of - o1 - o2, w1)
    w1 = (w1 + pltpu.roll(w1, ROWS, 1)).astype(bf16)
    w2 = (w2 + pltpu.roll(w2, ROWS, 1)).astype(bf16)
    weights = jnp.concatenate([w1, w2], axis=1)

    pop = pop_ref[...]
    up = lax.broadcasted_iota(jnp.int32, (batches, batches), 0)
    down = lax.broadcasted_iota(jnp.int32, (batches, batches), 1)
    column = jnp.sum(jnp.where(up == down, pop, 0), axis=1, keepdims=True)
    ends = jnp.sum(jnp.where(up <= down, column, 0), axis=0, keepdims=True)
    half = lax.broadcasted_iota(jnp.int32, (16, 1), 0)
    device = me + lax.rem(half, 8) - reach
    limit = device * cells + jnp.where(half >= 8, cells - 1, 0)
    spot = jnp.sum(jnp.where(ends <= limit, 1, 0), axis=1, keepdims=True)
    spot = jnp.where(device < 0, -9, spot)
    first = {h: spot[h + reach : h + reach + 1] for h in offsets + [0]}
    last = {h: spot[8 + h + reach : 9 + h + reach] for h in offsets + [0]}
    slot = lax.broadcasted_iota(jnp.int32, (SLOTS, 1), 0)
    batch_id = first[0] + slot
    batch_lane = lax.broadcasted_iota(jnp.int32, (SLOTS, batches), 1)
    chosen = batch_lane == batch_id
    held = jnp.sum(jnp.where(chosen, pop, 0), axis=1, keepdims=True)
    ridge = jnp.sum(jnp.where(chosen, ridge_ref[...], 0.0), axis=1, keepdims=True)
    ridge = jnp.where(batch_id < batches, ridge, 1.0)
    stop = jnp.sum(jnp.where(batch_lane <= batch_id, pop, 0), axis=1, keepdims=True) - me * cells
    start = stop - held
    held = held.astype(f32)
    starts_ref[...] = jnp.broadcast_to(jnp.where(batch_id < batches, start, 2 * cells), (SLOTS, 128))
    tail = slot == last[0] - first[0]
    head = slot == 0
    behind = {h: (last[h] == first[0]).astype(f32) for h in offsets if h < 0}
    ahead = {h: (first[h] == last[0]).astype(f32) for h in offsets if h > 0}

    wide = near - 1 + reach
    row32 = lax.broadcasted_iota(jnp.int32, (32, 1), 0)
    device = block * near + lax.rem(row32, 16) - reach
    limit = device * cells + jnp.where(row32 >= 16, cells - 1, 0)
    ids = jnp.sum(jnp.where(ends <= limit, 1, 0), axis=1, keepdims=True)
    ids = jnp.where(device < 0, -9, ids)
    limit = (block * near + lax.rem(half, 8)) * cells + jnp.where(half >= 8, cells - 1, 0)
    own_ids = jnp.sum(jnp.where(ends <= limit, 1, 0), axis=1, keepdims=True)
    own_lane = lax.broadcasted_iota(jnp.int32, (16, batches), 1)
    own_ridge = jnp.sum(jnp.where(own_lane == own_ids, ridge_ref[...], 0.0), axis=1, keepdims=True)

    crowded = jnp.zeros((1, 1), jnp.int32)
    for inner, room in ((SLOTS - 1, cells), (CLOSE - 1, width)):
        window = jnp.sum(
            jnp.where((up >= down) & (up < down + inner), column, 0), axis=0, keepdims=True
        )
        window = jnp.where((window < room - 1) & (batch_lane[0:1] <= batches - inner), 1, 0)
        crowded = crowded + jnp.sum(window, axis=1, keepdims=True)
    flag_ref[...] = jnp.broadcast_to(crowded, (1, 128))

    def inside(c, width, times):
        position = lax.broadcasted_iota(jnp.int32, (SLOTS * times, width), 1) + c * width
        low = jnp.concatenate([start] * times, axis=0)
        high = jnp.concatenate([stop] * times, axis=0)
        return ((position >= low) & (position < high)).astype(f32)

    def completed(own, buffer):
        before = jnp.zeros((1, clusters), f32)
        after = jnp.zeros((1, clusters), f32)
        for i, h in enumerate(offsets):
            if h < 0:
                before = before + behind[h] * buffer[i][1:2]
            else:
                after = after + ahead[h] * buffer[i][0:1]
        return own + jnp.where(head, before, 0.0) + jnp.where(tail, after, 0.0)

    def tail_of(value):
        return jnp.sum(jnp.where(tail, value, 0.0), axis=0, keepdims=True)

    def greeted_rows(which, value):
        near_out[which, 0:1, :] = value[0:1]
        near_out[which, 1:2, :] = tail_of(value)

    runs = cells // width

    def base_of(c):
        return jnp.sum(
            jnp.where((start <= c * width) & (slot > 0) & (batch_id < batches), 1, 0),
            axis=0,
            keepdims=True,
        )


    for i in range(runs):
        columns = pl.ds(i * width, width)
        pltpu.make_async_copy(z_hbm.at[0, :, columns], zf.at[:, columns], load_sems.at[i]).wait()
    z1, z2 = two_pieces(
        jnp.concatenate(
            [
                zf[...],
                jnp.ones((2, cells), f32),
                jnp.zeros((ROWS - 2 - pcs, cells), f32),
            ],
            axis=0,
        )
    )
    zc[0:ROWS, :] = z1
    zc[ROWS : 2 * ROWS, :] = z2
    score = plain(weights, jnp.concatenate([z1, z2, z1, z2], axis=0))
    raised = jnp.exp(score - jnp.max(score, axis=0, keepdims=True))
    ex[...] = raised
    p1, p2 = two_pieces(raised * (1.0 / jnp.sum(raised, axis=0, keepdims=True)))
    mask = inside(0, cells, 2).astype(bf16)
    total = across(mask, jnp.concatenate([p1, p2], axis=0))
    counts = total[0:SLOTS, 0:clusters] + total[0:SLOTS, clusters : 2 * clusters]
    own_total = jnp.sum(counts, axis=0, keepdims=True)
    greeted_rows(0, counts)
    line_out[0] = own_total
    pl.semaphore_wait(barrier, len(greeted))
    for r in range(1, plane):
        push(line_out.at[0], line_a.at[r - 1], 0, beside(r))
    for i, h in enumerate(offsets):
        push(near_out.at[0], near_counts.at[len(offsets) - 1 - i], 1, neighbour(h))

    def line_up(c):
        columns = slice(c * width, (c + 1) * width)
        mask = inside(c, width, 1)
        kind = jnp.sum(mask * slot.astype(f32), axis=0, keepdims=True)
        kind = kind - base_of(c).astype(f32)
        z = zc[:, columns]
        for j in range(CLOSE):
            lined[2 * ROWS * j : 2 * ROWS * (j + 1), columns] = z * (kind == j).astype(
                f32
            ).astype(bf16)

    for c in range(runs // 2):
        line_up(c)
    arrived(line_a, 0)
    plane_total = own_total + jnp.sum(line_a[...], axis=0)
    line_out[1] = plane_total
    for r in range(1, nz):
        push(line_out.at[1], line_b.at[r - 1], 2, along_z(r))
    for c in range(runs // 2, runs):
        line_up(c)
    arrived(near_counts, 1)
    full_counts = completed(counts, [near_counts[i] for i in range(len(offsets))])
    arrived(line_b, 2)
    totals = plane_total + jnp.sum(line_b[...], axis=0)
    expected = held * totals * (1.0 / cells_all)
    ratio = (expected + 1.0) / (full_counts + 1.0)
    factor = ratio * ratio
    f1 = factor.astype(bf16).astype(f32)
    f2 = (factor - f1).astype(bf16).astype(f32)
    f3 = factor - f1 - f2
    factor = jnp.concatenate([f1, f2, f3, jnp.zeros_like(f3)], axis=0).T.astype(bf16)

    mask = inside(0, cells, 4).astype(bf16)
    weighed = ex[...] * plain(factor, mask)
    a1, a2 = two_pieces(weighed * (1.0 / jnp.sum(weighed, axis=0, keepdims=True)))
    both = jnp.concatenate([a1, a2], axis=0)
    pair[...] = both
    total = across(mask[0 : 2 * SLOTS], both)
    mass = total[0:SLOTS, 0:clusters] + total[0:SLOTS, clusters : 2 * clusters]
    greeted_rows(1, mass)
    around = 2 * wide + 1
    for h in range(1, wide + 1):
        push(near_out.at[1], near_mass.at[(around - 1 - h) % around], 3, neighbour(h))
        push(near_out.at[1], near_mass.at[(around - 1 + h) % around], 3, neighbour(-h))
    near_mass[around - 1] = near_out[1]

    for c in range(runs):
        columns = slice(c * width, (c + 1) * width)
        value = across(lined[:, columns], pair[:, columns])
        for j in range(CLOSE):
            top = value[2 * ROWS * j : 2 * ROWS * j + ROWS]
            low = value[2 * ROWS * j + ROWS : 2 * ROWS * (j + 1)]
            pieces[c, j] = (
                top[:, 0:clusters] + top[:, clusters:] + low[:, 0:clusters] + low[:, clusters:]
            )
    places = [(c, j) for c in range(runs) for j in range(CLOSE)]
    tail_slot = last[0] - first[0]
    alone = jnp.where(tail_slot > 0, 1.0, 0.0)
    shrink = jnp.where(head | tail, 0.0, ridge / (mass + ridge))
    first_moment = jnp.zeros((ROWS, clusters), f32)
    tail_moment = jnp.zeros((ROWS, clusters), f32)
    whole = jnp.zeros((ROWS, clusters), f32)
    right = jnp.zeros((ROWS, clusters), f32)
    for c in range(runs):
        base = base_of(c)
        for j in range(CLOSE):
            piece = pieces[c, j]
            line = jnp.sum(jnp.where(slot == base + j, shrink, 0.0), axis=0, keepdims=True)
            right = right + line * piece
            tail_moment = tail_moment + jnp.where(base + j == tail_slot, 1.0, 0.0) * piece
            whole = whole + piece
            if j == 0:
                first_moment = first_moment + jnp.where(base == 0, 1.0, 0.0) * piece
    for t in range(near):
        inner = slice(t * rows_each, (t + 1) * rows_each)
        sums_out[t, 0] = right[inner]
        sums_out[t, 1] = first_moment[inner]
        sums_out[t, 2] = tail_moment[inner] * alone
        cent_out[t] = whole[inner]
    for r in range(1, near):
        push(sums_out.at[lax.rem(rank + r, near)], sum_in.at[r - 1], 5, mate(r))
    for r in range(1, near):
        push(cent_out.at[lax.rem(rank + r, near)], cent_in.at[r - 1], 4, mate(r))
    ends_out[0] = first_moment[0:56]
    ends_out[1] = tail_moment[0:56]
    arrived(near_mass.at[pl.ds(0, around - 1)], 3)
    full_mass = completed(
        mass, {i: near_mass[(around - 1 + h) % around] for i, h in enumerate(offsets)}
    )
    end_mass = jnp.zeros((16, clusters), f32)
    for p in range(-reach, near + reach):
        both = near_mass[lax.rem(p + (2 * around - 1) - rank, around)]
        one, two = ids[p + reach : p + reach + 1], ids[16 + p + reach : 17 + p + reach]
        end_mass = end_mass + jnp.where(own_ids == one, both[0:1], 0.0)
        end_mass = end_mass + jnp.where((own_ids == two) & (two != one), both[1:2], 0.0)
    end_shrink = own_ridge / (end_mass + own_ridge)
    for t in range(near):
        shrinks[t, 0:1, :] = end_shrink[t : t + 1]
        shrinks[t, 1:2, :] = end_shrink[8 + t : 9 + t]
    arrived(sum_in, 5)
    sum_tile = jnp.zeros((rows_each, clusters), f32)
    for r in range(near):
        by = shrinks[lax.rem(rank + near - r, near)]
        got = sums_out[rank] if r == 0 else sum_in[r - 1]
        sum_tile = sum_tile + got[0] + got[1] * by[0:1] + got[2] * by[1:2]
    tile_out[2] = sum_tile
    for r in range(1, far):
        push(tile_out.at[2], tile_in.at[r - 1], 8, peer(r))
    for i, h in enumerate(offsets):
        push(ends_out.at[int(h > 0)], near_moments.at[len(offsets) - 1 - i], 6, neighbour(h))
    arrived(cent_in, 4)
    cent_tile = cent_out[rank]
    for r in range(near - 1):
        cent_tile = cent_tile + cent_in[r]
    tile_out[0] = cent_tile
    for r in range(1, ny):
        push(tile_out.at[0], cent_y.at[r - 1], 7, along_y(r))
    arrived(cent_y, 7)
    for r in range(ny - 1):
        cent_tile = cent_tile + cent_y[r]
    tile_out[1] = cent_tile
    for r in range(1, nz):
        push(tile_out.at[1], cent_z.at[r - 1], 11, along_z(r))
    moments = []
    for s in range(SLOTS):
        moment = jnp.zeros((ROWS, clusters), f32)
        for c, j in places:
            if j <= s <= CLOSE * c + j:
                moment = moment + jnp.where(base_of(c) + j == s, 1.0, 0.0) * pieces[c, j]
        moments.append(moment)

    arrived(tile_in, 8)
    full_sums[1, 0] = sum_tile + jnp.sum(tile_in[...], axis=0)
    for r in range(1, near):
        push(full_sums.at[1, 0], full_sums.at[1, r], 10, mate(r))
    arrived(near_moments, 6)
    before = jnp.zeros((56, clusters), f32)
    after = jnp.zeros((56, clusters), f32)
    for i, h in enumerate(offsets):
        if h < 0:
            before = before + behind[h] * near_moments[i]
        else:
            after = after + ahead[h] * near_moments[i]
    for s in range(SLOTS):
        moment = moments[s][0:56] + after * tail[s : s + 1].astype(f32)
        full_moments[s] = moment + before if s == 0 else moment

    arrived(cent_z, 11)
    for r in range(nz - 1):
        cent_tile = cent_tile + cent_z[r]
    full_sums[0, 0] = cent_tile
    for r in range(1, near):
        push(full_sums.at[0, 0], full_sums.at[0, r], 9, mate(r))

    def gathered(which):
        return jnp.concatenate(
            [full_sums[which, lax.rem(rank + (near - t), near)] for t in range(near)], axis=0
        )

    arrived(full_sums.at[1, pl.ds(1, near - 1)], 10)
    right = gathered(1)
    intercept = (right / (1.0 + right[pcs : pcs + 1]))[0:56]
    for s in range(SLOTS):
        moment = full_moments[s]
        line = full_mass[s : s + 1]
        slope = (moment - line * intercept) / (line + ridge[s : s + 1])
        c1, c2 = two_pieces(jnp.concatenate([slope, jnp.zeros((8, clusters), f32)], axis=0))
        slopes[ROWS * s : ROWS * (s + 1), :] = jnp.concatenate([c1, c1, c2], axis=1)

    arrived(full_sums.at[0, pl.ds(1, near - 1)], 9)
    centre = gathered(0)
    centre = (centre / (1.0 + centre[pcs : pcs + 1])).T
    owned = cent_ref.shape[0]
    cells_at = lax.div(me, nx)
    row = lax.broadcasted_iota(jnp.int32, (clusters, ROWS), 0)
    for j in range(owned):
        line = jnp.sum(jnp.where(row == cells_at * owned + j, centre, 0.0), axis=0, keepdims=True)
        cent_ref[j : j + 1, :] = line[:, 0:pcs]

    left(line_a, 0)
    left(near_counts, 1)
    left(line_b, 2)
    left(near_mass.at[pl.ds(0, around - 1)], 3)
    left(cent_in, 4)
    left(sum_in, 5)
    left(near_moments, 6)
    left(cent_y, 7)
    left(tile_in, 8)
    left(cent_z, 11)
    left(full_sums.at[0, pl.ds(1, near - 1)], 9)
    left(full_sums.at[1, pl.ds(1, near - 1)], 10)


def correct_kernel(
    zf, pair, slopes, starts_ref, cent_ref, out_hbm, cent_hbm, held, starts, out_sems
):
    pcs, cells = zf.shape
    clusters = pair.shape[0] // 2
    loads = out_sems.shape[0] - 1
    part = cells // loads
    cent = pltpu.make_async_copy(cent_ref, cent_hbm, out_sems.at[loads])
    cent.start()
    begin = [jnp.max(starts_ref[s : s + 1, :]) for s in range(SLOTS)]
    for s in range(SLOTS):
        starts[s] = begin[s]
    lane = lax.broadcasted_iota(jnp.int32, (1, TILE), 1)

    def slope_of(j):
        return slopes[pl.ds(pl.multiple_of(j * ROWS, ROWS), ROWS), :]

    def slots_of(t):
        base = jnp.int32(0)
        final = jnp.int32(0)
        border = jnp.int32(2 * cells)
        for s in range(1, SLOTS):
            base = base + jnp.where(begin[s] <= t * TILE, 1, 0)
            final = final + jnp.where(begin[s] < (t + 1) * TILE, 1, 0)
            border = jnp.where(begin[s] > t * TILE, jnp.minimum(border, begin[s]), border)
        return base, final, border

    def send_out(i):
        columns = pl.ds(i * part, part)
        return pltpu.make_async_copy(
            held.at[:, columns], out_hbm.at[:, columns], out_sems.at[i]
        )

    beyond = jnp.int32(0)
    for i in range(loads):
        for t in range(i * part // TILE, (i + 1) * part // TILE):
            columns = slice(t * TILE, (t + 1) * TILE)
            base, final, border = slots_of(t)
            beyond = jnp.maximum(beyond, final - base)
            following = jnp.minimum(base + 1, SLOTS - 1)
            both = pair[:, columns]
            both = jnp.concatenate([both, both[0:clusters]], axis=0)
            moved = plain(jnp.concatenate([slope_of(base), slope_of(following)], axis=0), both)
            moved = jnp.where(lane < border - t * TILE, moved[0:ROWS], moved[ROWS:])
            held[:, columns] = zf[:, columns] - moved[0:pcs]
        send_out(i).start()
    for i in range(loads):
        send_out(i).wait()
    cent.wait()

    @pl.when(beyond > 1)
    def _():
        def tile_of(t, carry):
            columns = pl.ds(pl.multiple_of(t * TILE, TILE), TILE)
            base, final, border = slots_of(t)

            def more(j, carry):
                both = pair[:, columns]
                both = jnp.concatenate([both, both[0:clusters]], axis=0)
                other = zf[:, columns] - plain(slope_of(j), both)[0:pcs]
                held[:, columns] = jnp.where(
                    lane >= starts[j] - t * TILE, other, held[:, columns]
                )
                return carry

            lax.fori_loop(base + 2, final + 1, more, 0)
            return carry

        lax.fori_loop(0, cells // TILE, tile_of, 0)
        for i in range(loads):
            send_out(i).start()
        for i in range(loads):
            send_out(i).wait()


def narrow_body(
    shape, latent_coordinates, group_means, entropy_scaling, sample_shrinkage_lambda, sample_population
):
    pcs, cells = latent_coordinates.shape
    clusters = group_means.shape[0]
    batches = sample_population.shape[0]
    nz, ny, nc, nx = shape
    near, far = nc * nx, nz * ny
    rows_each = ROWS // near
    reach = (MOST - 2) // cells + 1
    owned = clusters // (nz * ny * nc)
    vmem = pl.BlockSpec(memory_space=pltpu.VMEM)
    tile = (rows_each, clusters)
    scratch = [
        pltpu.VMEM((pcs, clusters), f32),
        pltpu.VMEM((1, clusters), f32),
        pltpu.VMEM((1, batches), f32),
        pltpu.VMEM((1, batches), jnp.int32),
        pltpu.VMEM((2 * ROWS, cells), bf16),
        pltpu.VMEM((clusters, cells), f32),
        pltpu.VMEM((2 * ROWS * CLOSE, cells), bf16),
        pltpu.VMEM((clusters, clusters), f32),
        pltpu.VMEM((cells // 512, CLOSE, ROWS, clusters), f32),
        pltpu.VMEM((2, 2, clusters), f32),
        pltpu.VMEM((2 * reach, 2, clusters), f32),
        pltpu.VMEM((2 * (near - 1 + reach) + 1, 2, clusters), f32),
        pltpu.VMEM((2 * reach, 56, clusters), f32),
        pltpu.VMEM((2, 56, clusters), f32),
        pltpu.VMEM((SLOTS, 56, clusters), f32),
        pltpu.VMEM((2, 1, clusters), f32),
        pltpu.VMEM((near * ny - 1, 1, clusters), f32),
        pltpu.VMEM((nz - 1, 1, clusters), f32),
        pltpu.VMEM((near, 3, *tile), f32),
        pltpu.VMEM((near - 1, 3, *tile), f32),
        pltpu.VMEM((near, *tile), f32),
        pltpu.VMEM((near - 1, *tile), f32),
        pltpu.VMEM((near, 2, clusters), f32),
        pltpu.VMEM((ny - 1, *tile), f32),
        pltpu.VMEM((nz - 1, *tile), f32),
        pltpu.VMEM((3, *tile), f32),
        pltpu.VMEM((far - 1, *tile), f32),
        pltpu.VMEM((2, near, *tile), f32),
        pltpu.SemaphoreType.DMA((4,)),
        pltpu.SemaphoreType.DMA((cells // 512,)),
        pltpu.SemaphoreType.DMA((12,)),
        pltpu.SemaphoreType.DMA((12,)),
    ]
    return pl.pallas_call(
        functools.partial(step_kernel, shape, float(cells * near * far)),
        out_shape=(
            pltpu.VMEM((pcs, cells), f32),
            pltpu.VMEM((2 * clusters, cells), bf16),
            pltpu.VMEM((SLOTS * ROWS, 3 * clusters), bf16),
            pltpu.VMEM((SLOTS, 128), jnp.int32),
            pltpu.VMEM((1, 128), jnp.int32),
            pltpu.VMEM((owned, pcs), f32),
        ),
        in_specs=[pl.BlockSpec(memory_space=pl.ANY)] * 5,
        out_specs=(vmem,) * 6,
        scratch_shapes=scratch,
        compiler_params=pltpu.CompilerParams(
            collective_id=0, has_side_effects=True, vmem_limit_bytes=44 * 1024 * 1024
        ),
    )(
        latent_coordinates[None],
        group_means.T,
        entropy_scaling.reshape(1, clusters),
        sample_shrinkage_lambda.reshape(1, batches),
        sample_population.reshape(1, batches),
    )


def corrected_by(kept, pair, slopes, starts, new_centroids):
    pcs, cells = kept.shape
    vmem = pl.BlockSpec(memory_space=pltpu.VMEM)
    anywhere = pl.BlockSpec(memory_space=pl.ANY)
    return pl.pallas_call(
        correct_kernel,
        out_shape=(pltpu.HBM((pcs, cells), f32), pltpu.HBM(new_centroids.shape, f32)),
        in_specs=[vmem] * 5,
        out_specs=(anywhere, anywhere),
        scratch_shapes=[
            pltpu.VMEM((pcs, cells), f32),
            pltpu.SMEM((SLOTS,), jnp.int32),
            pltpu.SemaphoreType.DMA((5,)),
        ],
        compiler_params=pltpu.CompilerParams(vmem_limit_bytes=16 * 1024 * 1024),
    )(
        kept,
        pair,
        slopes,
        starts,
        new_centroids,
    )


def body(
    shape, latent_coordinates, group_means, entropy_scaling, sample_shrinkage_lambda, sample_population
):
    arguments = (
        latent_coordinates,
        group_means,
        entropy_scaling,
        sample_shrinkage_lambda,
        sample_population,
    )
    kept, pair, slopes, starts, flag, new_centroids = narrow_body(shape, *arguments)
    return lax.cond(
        flag[0, 0] == 0,
        lambda: corrected_by(kept, pair, slopes, starts, new_centroids),
        lambda: wide_body(*arguments),
    )


def solution(mesh):
    shape = (mesh.shape["cells"] // 8, 4, 2, mesh.shape["grp"])
    finer = Mesh(mesh.devices.reshape(shape), ("cells_0", "cells_1", "cells_2", "grp"))
    return jax.shard_map(
        functools.partial(body, shape),
        mesh=finer,
        in_specs=(P(None, CELLS_GRP), P(), P(), P(), P()),
        out_specs=(P(None, CELLS_GRP), P(CELLS, None)),
        check_vma=False,
    )
```

```python
import functools

import jax
import jax.numpy as jnp
from jax import lax
from jax.experimental import pallas as pl
from jax.experimental.pallas import tpu as pltpu
from jax.sharding import Mesh
from jax.sharding import PartitionSpec as P

CELLS = ("cells_0", "cells_1", "cells_2")
CELLS_GRP = ("cells_0", "cells_1", "cells_2", "grp")


diversity = 2.0
intercept_ridge = 1.0
highest = lax.Precision.HIGHEST


def split_up(array, dim, size):
    dims = array.shape
    parts = array.reshape(*dims[:dim], size, dims[dim] // size, *dims[dim + 1 :])
    return jnp.moveaxis(parts, dim, 0)


def summed_on_arrival(array, axis, dim):
    size = lax.axis_size(axis)
    parts = lax.all_to_all(split_up(array, dim, size), axis, 0, 0, tiled=True)
    return jnp.sum(parts, axis=0)


def sum_in_two_steps(array, axes, dim):
    far, near = axes
    parts = split_up(array, dim, lax.axis_size(far))
    nearer = summed_on_arrival(parts, near, dim + 1)
    arrived = lax.all_to_all(nearer, far, split_axis=0, concat_axis=0, tiled=True)
    return arrived.sum(axis=0)


def filled_up(lines, size):
    spare = -len(lines) % size
    return jnp.pad(lines, [(0, spare)] + [(0, 0)] * (lines.ndim - 1))


def sent_to_all(array, axis):
    size = lax.axis_size(axis)
    return lax.all_to_all(
        jnp.broadcast_to(array[None], (size, *array.shape)), axis, 0, 0, tiled=True
    )


def joined_along(parts, dim):
    parts = jnp.moveaxis(parts, 0, dim)
    dims = parts.shape
    return parts.reshape(*dims[:dim], dims[dim] * dims[dim + 1], *dims[dim + 2 :])


def gather_axes(array, axes, dim):
    far, near = axes
    leading = sent_to_all(array, far)
    parts = jnp.swapaxes(sent_to_all(leading, near), 0, 1)
    return joined_along(parts.reshape(-1, *array.shape), dim)


def total_of(array, axes):
    lines = array.reshape(-1)
    own = sum_in_two_steps(
        filled_up(lines, lax.axis_size(axes[0]) * lax.axis_size(axes[1])), axes, 0
    )
    whole = gather_axes(own, axes, 0)
    return whole[: len(lines)].reshape(array.shape)


def from_behind(block, axis, distance):
    devices = range(lax.axis_size(axis))
    route = [(i - distance, i) for i in devices if i - distance in devices]
    return lax.ppermute(block, axis, route)


def by_axis(array, axes):
    return functools.reduce(lax.psum, axes, array)


def observation_affinity(latent_coordinates, group_means, entropy_scaling):
    pairwise_dots = jnp.dot(
        group_means, latent_coordinates, precision=highest, preferred_element_type=jnp.float32
    )
    quadratic_lengths = jnp.sum(group_means * group_means, axis=1)
    return (2.0 * pairwise_dots - quadratic_lengths[:, None]) / (2.0 * entropy_scaling[:, None])


def probabilistic_responsibility(group_affinity):
    top = jnp.max(group_affinity, axis=0, keepdims=True)
    raised = jnp.exp(group_affinity - top)
    return raised / jnp.sum(raised, axis=0, keepdims=True)


def batch_parts(moments, ridge):
    mass = moments[:, 0, :]
    sums = moments[:, 1:, :]
    shrink = ridge[None, :] / (mass + ridge[None, :])
    weight = jnp.sum(mass * shrink, axis=1)
    right_side = jnp.sum(sums * shrink[:, None, :], axis=2)
    return (weight, right_side, jnp.sum(mass, axis=1), jnp.sum(sums, axis=2))


def slopes_of(moments, ridge, weight, right_side):
    mass = moments[:, 0, :]
    sums = moments[:, 1:, :]
    intercept = right_side / (intercept_ridge + weight)[:, None]
    return (sums - mass[:, None, :] * intercept[:, :, None]) / (mass + ridge[None, :])[:, None, :]


def wide_body(
    latent_coordinates, group_means, entropy_scaling, sample_shrinkage_lambda, sample_population
):
    local_cells = latent_coordinates.shape[1]
    num_pcs = latent_coordinates.shape[0]
    clusters = group_means.shape[0]
    batches = sample_population.shape[0]
    owned = clusters // lax.axis_size(CELLS)
    offset = (lax.axis_index(CELLS) * lax.axis_size("grp") + lax.axis_index("grp")) * local_cells
    batch_ends = jnp.cumsum(sample_population)
    batch_starts = batch_ends - sample_population
    cells_total = jnp.sum(sample_population).astype(jnp.float32)
    position = offset + lax.iota(jnp.int32, local_cells)
    batch_of = jnp.sum((batch_ends[:, None] <= position[None, :]).astype(jnp.int32), axis=0)
    first_batch = batch_of[0]
    last_batch = batch_of[local_cells - 1]
    group_affinity = observation_affinity(latent_coordinates, group_means, entropy_scaling)
    expected_occupancy = probabilistic_responsibility(group_affinity)

    def count_step(batch_id, running):
        in_batch = (batch_of == batch_id).astype(jnp.float32)
        single_observation = jnp.dot(
            expected_occupancy, in_batch, precision=highest, preferred_element_type=jnp.float32
        )
        return lax.dynamic_update_slice(
            running, single_observation[:, None], (jnp.int32(0), batch_id)
        )

    counts = lax.fori_loop(
        first_batch, last_batch + 1, count_step, jnp.zeros((clusters, batches), jnp.float32)
    )
    counts = total_of(counts, (("cells_0", "cells_1"), ("cells_2", "grp")))
    totals = jnp.sum(counts, axis=1)
    expected = sample_population.astype(jnp.float32)[None, :] * totals[:, None] / cells_total
    penalty = diversity * jnp.log((counts + 1.0) / (expected + 1.0))

    def penalty_step(batch_id, running):
        in_batch = (batch_of == batch_id).astype(jnp.float32)
        column = lax.dynamic_index_in_dim(penalty, batch_id, 1, keepdims=True)
        return running + column * in_batch[None, :]

    cell_penalty = lax.fori_loop(
        first_batch, last_batch + 1, penalty_step, jnp.zeros((clusters, local_cells), jnp.float32)
    )
    assign = probabilistic_responsibility(group_affinity - cell_penalty)
    augmented = jnp.concatenate(
        [jnp.ones((1, local_cells), jnp.float32), latent_coordinates], axis=0
    )

    def moment_step(batch_id, running):
        in_batch = (batch_of == batch_id).astype(jnp.float32)
        contiguous_portion = jnp.einsum(
            "kn,dn->kd", assign * in_batch[None, :], augmented, precision=highest
        )
        return lax.dynamic_update_slice(
            running, contiguous_portion[:, :, None], (jnp.int32(0), jnp.int32(0), batch_id)
        )

    moments = lax.fori_loop(
        first_batch,
        last_batch + 1,
        moment_step,
        jnp.zeros((clusters, num_pcs + 1, batches), jnp.float32),
    )
    devices_flat = lax.axis_size(CELLS) * lax.axis_size("grp")
    most_cells = 2 * local_cells * devices_flat // batches
    reach = (most_cells - 2) // local_cells + 1
    begins_here = (batch_starts >= offset) & (batch_starts < offset + local_cells)
    owner_mask = begins_here.astype(jnp.float32)
    head_owned = begins_here[first_batch]
    head_column = lax.dynamic_index_in_dim(moments, first_batch, 2, keepdims=False)
    sent_stats = jnp.where(head_owned, 0.0, 1.0) * head_column
    sent_tag = jnp.where(head_owned, 0.0, first_batch.astype(jnp.float32) + 1.0) * jnp.ones(
        (1,), jnp.float32
    )
    completed = moments
    for hop in range(1, reach + 1):
        got_stats, got_tag = from_behind((sent_stats, sent_tag), CELLS_GRP, -hop)
        got_id = jnp.maximum(got_tag[0].astype(jnp.int32) - 1, 0)
        accept = jnp.where((got_tag[0] > 0.5) & begins_here[got_id], 1.0, 0.0)
        single_observation = (
            lax.dynamic_index_in_dim(completed, got_id, 2, keepdims=False) + accept * got_stats
        )
        completed = lax.dynamic_update_slice(
            completed, single_observation[:, :, None], (jnp.int32(0), jnp.int32(0), got_id)
        )
    completed = completed * owner_mask[None, None, :]
    weight, right_side, mass_total, moment_total = jax.tree.map(
        lambda part: by_axis(part, CELLS_GRP), batch_parts(completed, sample_shrinkage_lambda)
    )
    coefficients = slopes_of(completed, sample_shrinkage_lambda, weight, right_side)
    every_centroid = moment_total / (1.0 + mass_total)[:, None]
    new_centroids = lax.dynamic_slice_in_dim(
        every_centroid, lax.axis_index(CELLS) * owned, owned, 0
    )
    tail_owned = begins_here[last_batch]
    tail_column = lax.dynamic_index_in_dim(coefficients, last_batch, 2, keepdims=False)
    tail_send = jnp.where(tail_owned, 1.0, 0.0) * tail_column
    tail_tag = jnp.where(tail_owned, last_batch.astype(jnp.float32) + 1.0, 0.0) * jnp.ones(
        (1,), jnp.float32
    )
    head_fix = jnp.zeros_like(tail_column)
    for hop in range(1, reach + 1):
        got_coef, got_tag = from_behind((tail_send, tail_tag), CELLS_GRP, hop)
        match = got_tag[0] == first_batch.astype(jnp.float32) + 1.0
        head_fix = jnp.where(match, got_coef, head_fix)
    own_head = lax.dynamic_index_in_dim(coefficients, first_batch, 2, keepdims=False)
    head_final = jnp.where(head_owned, own_head, head_fix)
    coefficients = lax.dynamic_update_slice(
        coefficients, head_final[:, :, None], (jnp.int32(0), jnp.int32(0), first_batch)
    )

    def correct_step(batch_id, running):
        in_batch = (batch_of == batch_id).astype(jnp.float32)
        slope_table = lax.dynamic_index_in_dim(coefficients, batch_id, 2, keepdims=False)
        moved = jnp.einsum("kd,kn->dn", slope_table, assign * in_batch[None, :], precision=highest)
        return running + moved

    corrected = lax.fori_loop(first_batch, last_batch + 1, correct_step, jnp.zeros_like(latent_coordinates))
    return (latent_coordinates - corrected, new_centroids)


SLOTS = 8
ROWS = 64
MOST = 10485
LOGICAL = pl.DeviceIdType.LOGICAL
TILE = 256
CLOSE = 4
bf16, f32 = jnp.bfloat16, jnp.float32


def two_pieces(value):
    first = value.astype(bf16)
    return first, (value - first.astype(f32)).astype(bf16)


def across(left, right):
    return lax.dot_general(left, right, (((1,), (1,)), ((), ())), preferred_element_type=f32)


def plain(left, right):
    return jnp.dot(left, right, preferred_element_type=f32)


def step_kernel(
    shape,
    cells_all,
    z_hbm,
    means_hbm,
    soft_hbm,
    ridge_hbm,
    pop_hbm,
    zf,
    pair,
    slopes,
    starts_ref,
    flag_ref,
    cent_ref,
    means_ref,
    soft_ref,
    ridge_ref,
    pop_ref,
    zc,
    ex,
    lined,
    means_wide,
    pieces,
    near_out,
    near_counts,
    near_mass,
    near_moments,
    ends_out,
    full_moments,
    line_out,
    line_a,
    line_b,
    sums_out,
    sum_in,
    cent_out,
    cent_in,
    shrinks,
    cent_y,
    cent_z,
    tile_out,
    tile_in,
    full_sums,
    small_sems,
    load_sems,
    send_sems,
    recv_sems,
):
    nz, ny, nc, nx = shape
    near = nc * nx
    far = nz * ny
    count = near * far
    cells = zf.shape[1]
    pcs, clusters = means_ref.shape
    batches = pop_ref.shape[1]
    rows_each = ROWS // near
    width = 512
    reach = (MOST - 2) // cells + 1
    offsets = [h for h in range(-reach, reach + 1) if h]
    me = (
        (lax.axis_index("cells_0") * ny + lax.axis_index("cells_1")) * nc
        + lax.axis_index("cells_2")
    ) * nx + lax.axis_index("grp")
    rank = lax.rem(me, near)
    block = lax.div(me, near)

    def mate(r):
        return block * near + lax.rem(rank + r, near)

    plane = near * ny
    in_plane = lax.rem(me, plane)

    def beside(r):
        return me - in_plane + lax.rem(in_plane + r, plane)

    def peer(r):
        return lax.rem(block + r, far) * near + rank

    def along_y(r):
        at = lax.rem(block, ny)
        return (block - at + lax.rem(at + r, ny)) * near + rank

    def along_z(r):
        return lax.rem(block + r * ny, far) * near + rank

    def neighbour(h):
        return lax.rem(me + (h + count), count)

    def push(src, dst, which, q):
        pltpu.make_async_remote_copy(
            src_ref=src,
            dst_ref=dst,
            send_sem=send_sems.at[which],
            recv_sem=recv_sems.at[which],
            device_id=q,
            device_id_type=LOGICAL,
        ).start()

    def arrived(buffer, which):
        pltpu.make_async_copy(buffer, buffer, recv_sems.at[which]).wait()

    def left(buffer, which):
        pltpu.make_async_copy(buffer, buffer, send_sems.at[which]).wait()

    small = [
        pltpu.make_async_copy(src, dst, small_sems.at[i])
        for i, (src, dst) in enumerate(
            (
                (pop_hbm, pop_ref),
                (means_hbm, means_ref),
                (soft_hbm, soft_ref),
                (ridge_hbm, ridge_ref),
            )
        )
    ]
    for copy in small:
        copy.start()
    for i in range(cells // width):
        columns = pl.ds(i * width, width)
        pltpu.make_async_copy(z_hbm.at[0, :, columns], zf.at[:, columns], load_sems.at[i]).start()

    barrier = pltpu.get_barrier_semaphore()
    greeted = [along_z(r) for r in range(1, nz)] + [beside(r) for r in range(1, plane)]
    greeted = greeted + [neighbour(h) for h in offsets]
    for q in greeted:
        pl.semaphore_signal(barrier, inc=1, device_id=q, device_id_type=LOGICAL)

    for copy in small:
        copy.wait()

    means_wide[...] = jnp.zeros_like(means_wide)
    means_wide[0:pcs, :] = means_ref[...]
    g = means_wide[...].T
    square = lax.broadcasted_iota(jnp.int32, (clusters, clusters), 0)
    lane = lax.broadcasted_iota(jnp.int32, (clusters, clusters), 1)
    soft = jnp.sum(jnp.where(square == lane, soft_ref[...], 0.0), axis=1, keepdims=True)
    offset_of = -0.5 * jnp.sum(g * g, axis=1, keepdims=True) / soft
    weights = jnp.where(lane == pcs, offset_of, g / soft)
    w1 = weights.astype(bf16).astype(f32)
    w2 = (weights - w1).astype(bf16).astype(f32)
    o1 = offset_of.astype(bf16).astype(f32)
    o2 = (offset_of - o1).astype(bf16).astype(f32)
    w1 = jnp.where(lane == pcs + 1, offset_of - o1 - o2, w1)
    w1 = (w1 + pltpu.roll(w1, ROWS, 1)).astype(bf16)
    w2 = (w2 + pltpu.roll(w2, ROWS, 1)).astype(bf16)
    weights = jnp.concatenate([w1, w2], axis=1)

    pop = pop_ref[...]
    up = lax.broadcasted_iota(jnp.int32, (batches, batches), 0)
    down = lax.broadcasted_iota(jnp.int32, (batches, batches), 1)
    column = jnp.sum(jnp.where(up == down, pop, 0), axis=1, keepdims=True)
    ends = jnp.sum(jnp.where(up <= down, column, 0), axis=0, keepdims=True)
    half = lax.broadcasted_iota(jnp.int32, (16, 1), 0)
    device = me + lax.rem(half, 8) - reach
    limit = device * cells + jnp.where(half >= 8, cells - 1, 0)
    spot = jnp.sum(jnp.where(ends <= limit, 1, 0), axis=1, keepdims=True)
    spot = jnp.where(device < 0, -9, spot)
    first = {h: spot[h + reach : h + reach + 1] for h in offsets + [0]}
    last = {h: spot[8 + h + reach : 9 + h + reach] for h in offsets + [0]}
    slot = lax.broadcasted_iota(jnp.int32, (SLOTS, 1), 0)
    batch_id = first[0] + slot
    batch_lane = lax.broadcasted_iota(jnp.int32, (SLOTS, batches), 1)
    chosen = batch_lane == batch_id
    held = jnp.sum(jnp.where(chosen, pop, 0), axis=1, keepdims=True)
    ridge = jnp.sum(jnp.where(chosen, ridge_ref[...], 0.0), axis=1, keepdims=True)
    ridge = jnp.where(batch_id < batches, ridge, 1.0)
    stop = jnp.sum(jnp.where(batch_lane <= batch_id, pop, 0), axis=1, keepdims=True) - me * cells
    start = stop - held
    held = held.astype(f32)
    starts_ref[...] = jnp.broadcast_to(jnp.where(batch_id < batches, start, 2 * cells), (SLOTS, 128))
    tail = slot == last[0] - first[0]
    head = slot == 0
    behind = {h: (last[h] == first[0]).astype(f32) for h in offsets if h < 0}
    ahead = {h: (first[h] == last[0]).astype(f32) for h in offsets if h > 0}

    wide = near - 1 + reach
    row32 = lax.broadcasted_iota(jnp.int32, (32, 1), 0)
    device = block * near + lax.rem(row32, 16) - reach
    limit = device * cells + jnp.where(row32 >= 16, cells - 1, 0)
    ids = jnp.sum(jnp.where(ends <= limit, 1, 0), axis=1, keepdims=True)
    ids = jnp.where(device < 0, -9, ids)
    limit = (block * near + lax.rem(half, 8)) * cells + jnp.where(half >= 8, cells - 1, 0)
    own_ids = jnp.sum(jnp.where(ends <= limit, 1, 0), axis=1, keepdims=True)
    own_lane = lax.broadcasted_iota(jnp.int32, (16, batches), 1)
    own_ridge = jnp.sum(jnp.where(own_lane == own_ids, ridge_ref[...], 0.0), axis=1, keepdims=True)

    crowded = jnp.zeros((1, 1), jnp.int32)
    for inner, room in ((SLOTS - 1, cells), (CLOSE - 1, width)):
        window = jnp.sum(
            jnp.where((up >= down) & (up < down + inner), column, 0), axis=0, keepdims=True
        )
        window = jnp.where((window < room - 1) & (batch_lane[0:1] <= batches - inner), 1, 0)
        crowded = crowded + jnp.sum(window, axis=1, keepdims=True)
    flag_ref[...] = jnp.broadcast_to(crowded, (1, 128))

    def inside(c, width, times):
        position = lax.broadcasted_iota(jnp.int32, (SLOTS * times, width), 1) + c * width
        low = jnp.concatenate([start] * times, axis=0)
        high = jnp.concatenate([stop] * times, axis=0)
        return ((position >= low) & (position < high)).astype(f32)

    def completed(own, buffer):
        before = jnp.zeros((1, clusters), f32)
        after = jnp.zeros((1, clusters), f32)
        for i, h in enumerate(offsets):
            if h < 0:
                before = before + behind[h] * buffer[i][1:2]
            else:
                after = after + ahead[h] * buffer[i][0:1]
        return own + jnp.where(head, before, 0.0) + jnp.where(tail, after, 0.0)

    def tail_of(value):
        return jnp.sum(jnp.where(tail, value, 0.0), axis=0, keepdims=True)

    def greeted_rows(which, value):
        near_out[which, 0:1, :] = value[0:1]
        near_out[which, 1:2, :] = tail_of(value)

    runs = cells // width

    def base_of(c):
        return jnp.sum(
            jnp.where((start <= c * width) & (slot > 0) & (batch_id < batches), 1, 0),
            axis=0,
            keepdims=True,
        )


    for i in range(runs):
        columns = pl.ds(i * width, width)
        pltpu.make_async_copy(z_hbm.at[0, :, columns], zf.at[:, columns], load_sems.at[i]).wait()
    z1, z2 = two_pieces(
        jnp.concatenate(
            [
                zf[...],
                jnp.ones((2, cells), f32),
                jnp.zeros((ROWS - 2 - pcs, cells), f32),
            ],
            axis=0,
        )
    )
    zc[0:ROWS, :] = z1
    zc[ROWS : 2 * ROWS, :] = z2
    score = plain(weights, jnp.concatenate([z1, z2, z1, z2], axis=0))
    raised = jnp.exp(score - jnp.max(score, axis=0, keepdims=True))
    ex[...] = raised
    p1, p2 = two_pieces(raised * (1.0 / jnp.sum(raised, axis=0, keepdims=True)))
    mask = inside(0, cells, 2).astype(bf16)
    total = across(mask, jnp.concatenate([p1, p2], axis=0))
    counts = total[0:SLOTS, 0:clusters] + total[0:SLOTS, clusters : 2 * clusters]
    own_total = jnp.sum(counts, axis=0, keepdims=True)
    greeted_rows(0, counts)
    line_out[0] = own_total
    pl.semaphore_wait(barrier, len(greeted))
    for r in range(1, plane):
        push(line_out.at[0], line_a.at[r - 1], 0, beside(r))
    for i, h in enumerate(offsets):
        push(near_out.at[0], near_counts.at[len(offsets) - 1 - i], 1, neighbour(h))

    def line_up(c):
        columns = slice(c * width, (c + 1) * width)
        mask = inside(c, width, 1)
        kind = jnp.sum(mask * slot.astype(f32), axis=0, keepdims=True)
        kind = kind - base_of(c).astype(f32)
        z = zc[:, columns]
        for j in range(CLOSE):
            lined[2 * ROWS * j : 2 * ROWS * (j + 1), columns] = z * (kind == j).astype(
                f32
            ).astype(bf16)

    for c in range(runs // 2):
        line_up(c)
    arrived(line_a, 0)
    plane_total = own_total + jnp.sum(line_a[...], axis=0)
    line_out[1] = plane_total
    for r in range(1, nz):
        push(line_out.at[1], line_b.at[r - 1], 2, along_z(r))
    for c in range(runs // 2, runs):
        line_up(c)
    arrived(near_counts, 1)
    full_counts = completed(counts, [near_counts[i] for i in range(len(offsets))])
    arrived(line_b, 2)
    totals = plane_total + jnp.sum(line_b[...], axis=0)
    expected = held * totals * (1.0 / cells_all)
    ratio = (expected + 1.0) / (full_counts + 1.0)
    factor = ratio * ratio
    f1 = factor.astype(bf16).astype(f32)
    f2 = (factor - f1).astype(bf16).astype(f32)
    f3 = factor - f1 - f2
    factor = jnp.concatenate([f1, f2, f3, jnp.zeros_like(f3)], axis=0).T.astype(bf16)

    mask = inside(0, cells, 4).astype(bf16)
    weighed = ex[...] * plain(factor, mask)
    a1, a2 = two_pieces(weighed * (1.0 / jnp.sum(weighed, axis=0, keepdims=True)))
    both = jnp.concatenate([a1, a2], axis=0)
    pair[...] = both
    total = across(mask[0 : 2 * SLOTS], both)
    mass = total[0:SLOTS, 0:clusters] + total[0:SLOTS, clusters : 2 * clusters]
    greeted_rows(1, mass)
    around = 2 * wide + 1
    for h in range(1, wide + 1):
        push(near_out.at[1], near_mass.at[(around - 1 - h) % around], 3, neighbour(h))
        push(near_out.at[1], near_mass.at[(around - 1 + h) % around], 3, neighbour(-h))
    near_mass[around - 1] = near_out[1]

    for c in range(runs):
        columns = slice(c * width, (c + 1) * width)
        value = across(lined[:, columns], pair[:, columns])
        for j in range(CLOSE):
            top = value[2 * ROWS * j : 2 * ROWS * j + ROWS]
            low = value[2 * ROWS * j + ROWS : 2 * ROWS * (j + 1)]
            pieces[c, j] = (
                top[:, 0:clusters] + top[:, clusters:] + low[:, 0:clusters] + low[:, clusters:]
            )
    places = [(c, j) for c in range(runs) for j in range(CLOSE)]
    tail_slot = last[0] - first[0]
    alone = jnp.where(tail_slot > 0, 1.0, 0.0)
    shrink = jnp.where(head | tail, 0.0, ridge / (mass + ridge))
    first_moment = jnp.zeros((ROWS, clusters), f32)
    tail_moment = jnp.zeros((ROWS, clusters), f32)
    whole = jnp.zeros((ROWS, clusters), f32)
    right = jnp.zeros((ROWS, clusters), f32)
    for c in range(runs):
        base = base_of(c)
        for j in range(CLOSE):
            piece = pieces[c, j]
            line = jnp.sum(jnp.where(slot == base + j, shrink, 0.0), axis=0, keepdims=True)
            right = right + line * piece
            tail_moment = tail_moment + jnp.where(base + j == tail_slot, 1.0, 0.0) * piece
            whole = whole + piece
            if j == 0:
                first_moment = first_moment + jnp.where(base == 0, 1.0, 0.0) * piece
    for t in range(near):
        inner = slice(t * rows_each, (t + 1) * rows_each)
        sums_out[t, 0] = right[inner]
        sums_out[t, 1] = first_moment[inner]
        sums_out[t, 2] = tail_moment[inner] * alone
        cent_out[t] = whole[inner]
    for r in range(1, near):
        push(sums_out.at[lax.rem(rank + r, near)], sum_in.at[r - 1], 5, mate(r))
    ends_out[0] = first_moment[0:56]
    ends_out[1] = tail_moment[0:56]
    for i, h in enumerate(offsets):
        push(ends_out.at[int(h > 0)], near_moments.at[len(offsets) - 1 - i], 6, neighbour(h))
    for r in range(1, near):
        push(cent_out.at[lax.rem(rank + r, near)], cent_in.at[r - 1], 4, mate(r))
    arrived(near_mass.at[pl.ds(0, around - 1)], 3)
    full_mass = completed(
        mass, {i: near_mass[(around - 1 + h) % around] for i, h in enumerate(offsets)}
    )
    end_mass = jnp.zeros((16, clusters), f32)
    for p in range(-reach, near + reach):
        both = near_mass[lax.rem(p + (2 * around - 1) - rank, around)]
        one, two = ids[p + reach : p + reach + 1], ids[16 + p + reach : 17 + p + reach]
        end_mass = end_mass + jnp.where(own_ids == one, both[0:1], 0.0)
        end_mass = end_mass + jnp.where((own_ids == two) & (two != one), both[1:2], 0.0)
    end_shrink = own_ridge / (end_mass + own_ridge)
    for t in range(near):
        shrinks[t, 0:1, :] = end_shrink[t : t + 1]
        shrinks[t, 1:2, :] = end_shrink[8 + t : 9 + t]
    arrived(sum_in, 5)
    sum_tile = jnp.zeros((rows_each, clusters), f32)
    for r in range(near):
        by = shrinks[lax.rem(rank + near - r, near)]
        got = sums_out[rank] if r == 0 else sum_in[r - 1]
        sum_tile = sum_tile + got[0] + got[1] * by[0:1] + got[2] * by[1:2]
    tile_out[2] = sum_tile
    for r in range(1, far):
        push(tile_out.at[2], tile_in.at[r - 1], 8, peer(r))
    arrived(cent_in, 4)
    cent_tile = cent_out[rank]
    for r in range(near - 1):
        cent_tile = cent_tile + cent_in[r]
    tile_out[0] = cent_tile
    for r in range(1, ny):
        push(tile_out.at[0], cent_y.at[r - 1], 7, along_y(r))
    arrived(cent_y, 7)
    for r in range(ny - 1):
        cent_tile = cent_tile + cent_y[r]
    tile_out[1] = cent_tile
    for r in range(1, nz):
        push(tile_out.at[1], cent_z.at[r - 1], 11, along_z(r))
    moments = []
    for s in range(SLOTS):
        moment = jnp.zeros((ROWS, clusters), f32)
        for c, j in places:
            if j <= s <= CLOSE * c + j:
                moment = moment + jnp.where(base_of(c) + j == s, 1.0, 0.0) * pieces[c, j]
        moments.append(moment)

    arrived(tile_in, 8)
    full_sums[1, 0] = sum_tile + jnp.sum(tile_in[...], axis=0)
    for r in range(1, near):
        push(full_sums.at[1, 0], full_sums.at[1, r], 10, mate(r))
    arrived(near_moments, 6)
    before = jnp.zeros((56, clusters), f32)
    after = jnp.zeros((56, clusters), f32)
    for i, h in enumerate(offsets):
        if h < 0:
            before = before + behind[h] * near_moments[i]
        else:
            after = after + ahead[h] * near_moments[i]
    for s in range(SLOTS):
        moment = moments[s][0:56] + after * tail[s : s + 1].astype(f32)
        full_moments[s] = moment + before if s == 0 else moment

    arrived(cent_z, 11)
    for r in range(nz - 1):
        cent_tile = cent_tile + cent_z[r]
    full_sums[0, 0] = cent_tile
    for r in range(1, near):
        push(full_sums.at[0, 0], full_sums.at[0, r], 9, mate(r))

    def gathered(which):
        return jnp.concatenate(
            [full_sums[which, lax.rem(rank + (near - t), near)] for t in range(near)], axis=0
        )

    arrived(full_sums.at[1, pl.ds(1, near - 1)], 10)
    right = gathered(1)
    intercept = (right / (1.0 + right[pcs : pcs + 1]))[0:56]
    for s in range(SLOTS):
        moment = full_moments[s]
        line = full_mass[s : s + 1]
        slope = (moment - line * intercept) / (line + ridge[s : s + 1])
        c1, c2 = two_pieces(jnp.concatenate([slope, jnp.zeros((8, clusters), f32)], axis=0))
        slopes[ROWS * s : ROWS * (s + 1), :] = jnp.concatenate([c1, c1, c2], axis=1)

    arrived(full_sums.at[0, pl.ds(1, near - 1)], 9)
    centre = gathered(0)
    centre = (centre / (1.0 + centre[pcs : pcs + 1])).T
    owned = cent_ref.shape[0]
    cells_at = lax.div(me, nx)
    row = lax.broadcasted_iota(jnp.int32, (clusters, ROWS), 0)
    for j in range(owned):
        line = jnp.sum(jnp.where(row == cells_at * owned + j, centre, 0.0), axis=0, keepdims=True)
        cent_ref[j : j + 1, :] = line[:, 0:pcs]

    left(line_a, 0)
    left(near_counts, 1)
    left(line_b, 2)
    left(near_mass.at[pl.ds(0, around - 1)], 3)
    left(cent_in, 4)
    left(sum_in, 5)
    left(near_moments, 6)
    left(cent_y, 7)
    left(tile_in, 8)
    left(cent_z, 11)
    left(full_sums.at[0, pl.ds(1, near - 1)], 9)
    left(full_sums.at[1, pl.ds(1, near - 1)], 10)


def correct_kernel(
    zf, pair, slopes, starts_ref, cent_ref, out_hbm, cent_hbm, held, starts, out_sems
):
    pcs, cells = zf.shape
    clusters = pair.shape[0] // 2
    loads = out_sems.shape[0] - 1
    part = cells // loads
    cent = pltpu.make_async_copy(cent_ref, cent_hbm, out_sems.at[loads])
    cent.start()
    begin = [jnp.max(starts_ref[s : s + 1, :]) for s in range(SLOTS)]
    for s in range(SLOTS):
        starts[s] = begin[s]
    lane = lax.broadcasted_iota(jnp.int32, (1, TILE), 1)

    def slope_of(j):
        return slopes[pl.ds(pl.multiple_of(j * ROWS, ROWS), ROWS), :]

    def slots_of(t):
        base = jnp.int32(0)
        final = jnp.int32(0)
        border = jnp.int32(2 * cells)
        for s in range(1, SLOTS):
            base = base + jnp.where(begin[s] <= t * TILE, 1, 0)
            final = final + jnp.where(begin[s] < (t + 1) * TILE, 1, 0)
            border = jnp.where(begin[s] > t * TILE, jnp.minimum(border, begin[s]), border)
        return base, final, border

    def send_out(i):
        columns = pl.ds(i * part, part)
        return pltpu.make_async_copy(
            held.at[:, columns], out_hbm.at[:, columns], out_sems.at[i]
        )

    beyond = jnp.int32(0)
    for i in range(loads):
        for t in range(i * part // TILE, (i + 1) * part // TILE):
            columns = slice(t * TILE, (t + 1) * TILE)
            base, final, border = slots_of(t)
            beyond = jnp.maximum(beyond, final - base)
            following = jnp.minimum(base + 1, SLOTS - 1)
            both = pair[:, columns]
            both = jnp.concatenate([both, both[0:clusters]], axis=0)
            moved = plain(jnp.concatenate([slope_of(base), slope_of(following)], axis=0), both)
            moved = jnp.where(lane < border - t * TILE, moved[0:ROWS], moved[ROWS:])
            held[:, columns] = zf[:, columns] - moved[0:pcs]
        send_out(i).start()
    for i in range(loads):
        send_out(i).wait()
    cent.wait()

    @pl.when(beyond > 1)
    def _():
        def tile_of(t, carry):
            columns = pl.ds(pl.multiple_of(t * TILE, TILE), TILE)
            base, final, border = slots_of(t)

            def more(j, carry):
                both = pair[:, columns]
                both = jnp.concatenate([both, both[0:clusters]], axis=0)
                other = zf[:, columns] - plain(slope_of(j), both)[0:pcs]
                held[:, columns] = jnp.where(
                    lane >= starts[j] - t * TILE, other, held[:, columns]
                )
                return carry

            lax.fori_loop(base + 2, final + 1, more, 0)
            return carry

        lax.fori_loop(0, cells // TILE, tile_of, 0)
        for i in range(loads):
            send_out(i).start()
        for i in range(loads):
            send_out(i).wait()


def narrow_body(
    shape, latent_coordinates, group_means, entropy_scaling, sample_shrinkage_lambda, sample_population
):
    pcs, cells = latent_coordinates.shape
    clusters = group_means.shape[0]
    batches = sample_population.shape[0]
    nz, ny, nc, nx = shape
    near, far = nc * nx, nz * ny
    rows_each = ROWS // near
    reach = (MOST - 2) // cells + 1
    owned = clusters // (nz * ny * nc)
    vmem = pl.BlockSpec(memory_space=pltpu.VMEM)
    tile = (rows_each, clusters)
    scratch = [
        pltpu.VMEM((pcs, clusters), f32),
        pltpu.VMEM((1, clusters), f32),
        pltpu.VMEM((1, batches), f32),
        pltpu.VMEM((1, batches), jnp.int32),
        pltpu.VMEM((2 * ROWS, cells), bf16),
        pltpu.VMEM((clusters, cells), f32),
        pltpu.VMEM((2 * ROWS * CLOSE, cells), bf16),
        pltpu.VMEM((clusters, clusters), f32),
        pltpu.VMEM((cells // 512, CLOSE, ROWS, clusters), f32),
        pltpu.VMEM((2, 2, clusters), f32),
        pltpu.VMEM((2 * reach, 2, clusters), f32),
        pltpu.VMEM((2 * (near - 1 + reach) + 1, 2, clusters), f32),
        pltpu.VMEM((2 * reach, 56, clusters), f32),
        pltpu.VMEM((2, 56, clusters), f32),
        pltpu.VMEM((SLOTS, 56, clusters), f32),
        pltpu.VMEM((2, 1, clusters), f32),
        pltpu.VMEM((near * ny - 1, 1, clusters), f32),
        pltpu.VMEM((nz - 1, 1, clusters), f32),
        pltpu.VMEM((near, 3, *tile), f32),
        pltpu.VMEM((near - 1, 3, *tile), f32),
        pltpu.VMEM((near, *tile), f32),
        pltpu.VMEM((near - 1, *tile), f32),
        pltpu.VMEM((near, 2, clusters), f32),
        pltpu.VMEM((ny - 1, *tile), f32),
        pltpu.VMEM((nz - 1, *tile), f32),
        pltpu.VMEM((3, *tile), f32),
        pltpu.VMEM((far - 1, *tile), f32),
        pltpu.VMEM((2, near, *tile), f32),
        pltpu.SemaphoreType.DMA((4,)),
        pltpu.SemaphoreType.DMA((cells // 512,)),
        pltpu.SemaphoreType.DMA((12,)),
        pltpu.SemaphoreType.DMA((12,)),
    ]
    return pl.pallas_call(
        functools.partial(step_kernel, shape, float(cells * near * far)),
        out_shape=(
            pltpu.VMEM((pcs, cells), f32),
            pltpu.VMEM((2 * clusters, cells), bf16),
            pltpu.VMEM((SLOTS * ROWS, 3 * clusters), bf16),
            pltpu.VMEM((SLOTS, 128), jnp.int32),
            pltpu.VMEM((1, 128), jnp.int32),
            pltpu.VMEM((owned, pcs), f32),
        ),
        in_specs=[pl.BlockSpec(memory_space=pl.ANY)] * 5,
        out_specs=(vmem,) * 6,
        scratch_shapes=scratch,
        compiler_params=pltpu.CompilerParams(
            collective_id=0, has_side_effects=True, vmem_limit_bytes=44 * 1024 * 1024
        ),
    )(
        latent_coordinates[None],
        group_means.T,
        entropy_scaling.reshape(1, clusters),
        sample_shrinkage_lambda.reshape(1, batches),
        sample_population.reshape(1, batches),
    )


def corrected_by(kept, pair, slopes, starts, new_centroids):
    pcs, cells = kept.shape
    vmem = pl.BlockSpec(memory_space=pltpu.VMEM)
    anywhere = pl.BlockSpec(memory_space=pl.ANY)
    return pl.pallas_call(
        correct_kernel,
        out_shape=(pltpu.HBM((pcs, cells), f32), pltpu.HBM(new_centroids.shape, f32)),
        in_specs=[vmem] * 5,
        out_specs=(anywhere, anywhere),
        scratch_shapes=[
            pltpu.VMEM((pcs, cells), f32),
            pltpu.SMEM((SLOTS,), jnp.int32),
            pltpu.SemaphoreType.DMA((5,)),
        ],
        compiler_params=pltpu.CompilerParams(vmem_limit_bytes=16 * 1024 * 1024),
    )(
        kept,
        pair,
        slopes,
        starts,
        new_centroids,
    )


def body(
    shape, latent_coordinates, group_means, entropy_scaling, sample_shrinkage_lambda, sample_population
):
    arguments = (
        latent_coordinates,
        group_means,
        entropy_scaling,
        sample_shrinkage_lambda,
        sample_population,
    )
    kept, pair, slopes, starts, flag, new_centroids = narrow_body(shape, *arguments)
    return lax.cond(
        flag[0, 0] == 0,
        lambda: corrected_by(kept, pair, slopes, starts, new_centroids),
        lambda: wide_body(*arguments),
    )


def solution(mesh):
    shape = (mesh.shape["cells"] // 8, 4, 2, mesh.shape["grp"])
    finer = Mesh(mesh.devices.reshape(shape), ("cells_0", "cells_1", "cells_2", "grp"))
    return jax.shard_map(
        functools.partial(body, shape),
        mesh=finer,
        in_specs=(P(None, CELLS_GRP), P(), P(), P(), P()),
        out_specs=(P(None, CELLS_GRP), P(CELLS, None)),
        check_vma=False,
    )
```

```python
import functools

import jax
import jax.numpy as jnp
from jax import lax
from jax.experimental import pallas as pl
from jax.experimental.pallas import tpu as pltpu
from jax.sharding import Mesh
from jax.sharding import PartitionSpec as P

CELLS = ("cells_0", "cells_1", "cells_2")
CELLS_GRP = ("cells_0", "cells_1", "cells_2", "grp")


diversity = 2.0
intercept_ridge = 1.0
highest = lax.Precision.HIGHEST


def split_up(array, dim, size):
    dims = array.shape
    parts = array.reshape(*dims[:dim], size, dims[dim] // size, *dims[dim + 1 :])
    return jnp.moveaxis(parts, dim, 0)


def summed_on_arrival(array, axis, dim):
    size = lax.axis_size(axis)
    parts = lax.all_to_all(split_up(array, dim, size), axis, 0, 0, tiled=True)
    return jnp.sum(parts, axis=0)


def sum_in_two_steps(array, axes, dim):
    far, near = axes
    parts = split_up(array, dim, lax.axis_size(far))
    nearer = summed_on_arrival(parts, near, dim + 1)
    arrived = lax.all_to_all(nearer, far, split_axis=0, concat_axis=0, tiled=True)
    return arrived.sum(axis=0)


def filled_up(lines, size):
    spare = -len(lines) % size
    return jnp.pad(lines, [(0, spare)] + [(0, 0)] * (lines.ndim - 1))


def sent_to_all(array, axis):
    size = lax.axis_size(axis)
    return lax.all_to_all(
        jnp.broadcast_to(array[None], (size, *array.shape)), axis, 0, 0, tiled=True
    )


def joined_along(parts, dim):
    parts = jnp.moveaxis(parts, 0, dim)
    dims = parts.shape
    return parts.reshape(*dims[:dim], dims[dim] * dims[dim + 1], *dims[dim + 2 :])


def gather_axes(array, axes, dim):
    far, near = axes
    leading = sent_to_all(array, far)
    parts = jnp.swapaxes(sent_to_all(leading, near), 0, 1)
    return joined_along(parts.reshape(-1, *array.shape), dim)


def total_of(array, axes):
    lines = array.reshape(-1)
    own = sum_in_two_steps(
        filled_up(lines, lax.axis_size(axes[0]) * lax.axis_size(axes[1])), axes, 0
    )
    whole = gather_axes(own, axes, 0)
    return whole[: len(lines)].reshape(array.shape)


def from_behind(block, axis, distance):
    devices = range(lax.axis_size(axis))
    route = [(i - distance, i) for i in devices if i - distance in devices]
    return lax.ppermute(block, axis, route)


def by_axis(array, axes):
    return functools.reduce(lax.psum, axes, array)


def observation_affinity(latent_coordinates, group_means, entropy_scaling):
    pairwise_dots = jnp.dot(
        group_means, latent_coordinates, precision=highest, preferred_element_type=jnp.float32
    )
    quadratic_lengths = jnp.sum(group_means * group_means, axis=1)
    return (2.0 * pairwise_dots - quadratic_lengths[:, None]) / (2.0 * entropy_scaling[:, None])


def probabilistic_responsibility(group_affinity):
    top = jnp.max(group_affinity, axis=0, keepdims=True)
    raised = jnp.exp(group_affinity - top)
    return raised / jnp.sum(raised, axis=0, keepdims=True)


def batch_parts(moments, ridge):
    mass = moments[:, 0, :]
    sums = moments[:, 1:, :]
    shrink = ridge[None, :] / (mass + ridge[None, :])
    weight = jnp.sum(mass * shrink, axis=1)
    right_side = jnp.sum(sums * shrink[:, None, :], axis=2)
    return (weight, right_side, jnp.sum(mass, axis=1), jnp.sum(sums, axis=2))


def slopes_of(moments, ridge, weight, right_side):
    mass = moments[:, 0, :]
    sums = moments[:, 1:, :]
    intercept = right_side / (intercept_ridge + weight)[:, None]
    return (sums - mass[:, None, :] * intercept[:, :, None]) / (mass + ridge[None, :])[:, None, :]


def wide_body(
    latent_coordinates, group_means, entropy_scaling, sample_shrinkage_lambda, sample_population
):
    local_cells = latent_coordinates.shape[1]
    num_pcs = latent_coordinates.shape[0]
    clusters = group_means.shape[0]
    batches = sample_population.shape[0]
    owned = clusters // lax.axis_size(CELLS)
    offset = (lax.axis_index(CELLS) * lax.axis_size("grp") + lax.axis_index("grp")) * local_cells
    batch_ends = jnp.cumsum(sample_population)
    batch_starts = batch_ends - sample_population
    cells_total = jnp.sum(sample_population).astype(jnp.float32)
    position = offset + lax.iota(jnp.int32, local_cells)
    batch_of = jnp.sum((batch_ends[:, None] <= position[None, :]).astype(jnp.int32), axis=0)
    first_batch = batch_of[0]
    last_batch = batch_of[local_cells - 1]
    group_affinity = observation_affinity(latent_coordinates, group_means, entropy_scaling)
    expected_occupancy = probabilistic_responsibility(group_affinity)

    def count_step(batch_id, running):
        in_batch = (batch_of == batch_id).astype(jnp.float32)
        single_observation = jnp.dot(
            expected_occupancy, in_batch, precision=highest, preferred_element_type=jnp.float32
        )
        return lax.dynamic_update_slice(
            running, single_observation[:, None], (jnp.int32(0), batch_id)
        )

    counts = lax.fori_loop(
        first_batch, last_batch + 1, count_step, jnp.zeros((clusters, batches), jnp.float32)
    )
    counts = total_of(counts, (("cells_0", "cells_1"), ("cells_2", "grp")))
    totals = jnp.sum(counts, axis=1)
    expected = sample_population.astype(jnp.float32)[None, :] * totals[:, None] / cells_total
    penalty = diversity * jnp.log((counts + 1.0) / (expected + 1.0))

    def penalty_step(batch_id, running):
        in_batch = (batch_of == batch_id).astype(jnp.float32)
        column = lax.dynamic_index_in_dim(penalty, batch_id, 1, keepdims=True)
        return running + column * in_batch[None, :]

    cell_penalty = lax.fori_loop(
        first_batch, last_batch + 1, penalty_step, jnp.zeros((clusters, local_cells), jnp.float32)
    )
    assign = probabilistic_responsibility(group_affinity - cell_penalty)
    augmented = jnp.concatenate(
        [jnp.ones((1, local_cells), jnp.float32), latent_coordinates], axis=0
    )

    def moment_step(batch_id, running):
        in_batch = (batch_of == batch_id).astype(jnp.float32)
        contiguous_portion = jnp.einsum(
            "kn,dn->kd", assign * in_batch[None, :], augmented, precision=highest
        )
        return lax.dynamic_update_slice(
            running, contiguous_portion[:, :, None], (jnp.int32(0), jnp.int32(0), batch_id)
        )

    moments = lax.fori_loop(
        first_batch,
        last_batch + 1,
        moment_step,
        jnp.zeros((clusters, num_pcs + 1, batches), jnp.float32),
    )
    devices_flat = lax.axis_size(CELLS) * lax.axis_size("grp")
    most_cells = 2 * local_cells * devices_flat // batches
    reach = (most_cells - 2) // local_cells + 1
    begins_here = (batch_starts >= offset) & (batch_starts < offset + local_cells)
    owner_mask = begins_here.astype(jnp.float32)
    head_owned = begins_here[first_batch]
    head_column = lax.dynamic_index_in_dim(moments, first_batch, 2, keepdims=False)
    sent_stats = jnp.where(head_owned, 0.0, 1.0) * head_column
    sent_tag = jnp.where(head_owned, 0.0, first_batch.astype(jnp.float32) + 1.0) * jnp.ones(
        (1,), jnp.float32
    )
    completed = moments
    for hop in range(1, reach + 1):
        got_stats, got_tag = from_behind((sent_stats, sent_tag), CELLS_GRP, -hop)
        got_id = jnp.maximum(got_tag[0].astype(jnp.int32) - 1, 0)
        accept = jnp.where((got_tag[0] > 0.5) & begins_here[got_id], 1.0, 0.0)
        single_observation = (
            lax.dynamic_index_in_dim(completed, got_id, 2, keepdims=False) + accept * got_stats
        )
        completed = lax.dynamic_update_slice(
            completed, single_observation[:, :, None], (jnp.int32(0), jnp.int32(0), got_id)
        )
    completed = completed * owner_mask[None, None, :]
    weight, right_side, mass_total, moment_total = jax.tree.map(
        lambda part: by_axis(part, CELLS_GRP), batch_parts(completed, sample_shrinkage_lambda)
    )
    coefficients = slopes_of(completed, sample_shrinkage_lambda, weight, right_side)
    every_centroid = moment_total / (1.0 + mass_total)[:, None]
    new_centroids = lax.dynamic_slice_in_dim(
        every_centroid, lax.axis_index(CELLS) * owned, owned, 0
    )
    tail_owned = begins_here[last_batch]
    tail_column = lax.dynamic_index_in_dim(coefficients, last_batch, 2, keepdims=False)
    tail_send = jnp.where(tail_owned, 1.0, 0.0) * tail_column
    tail_tag = jnp.where(tail_owned, last_batch.astype(jnp.float32) + 1.0, 0.0) * jnp.ones(
        (1,), jnp.float32
    )
    head_fix = jnp.zeros_like(tail_column)
    for hop in range(1, reach + 1):
        got_coef, got_tag = from_behind((tail_send, tail_tag), CELLS_GRP, hop)
        match = got_tag[0] == first_batch.astype(jnp.float32) + 1.0
        head_fix = jnp.where(match, got_coef, head_fix)
    own_head = lax.dynamic_index_in_dim(coefficients, first_batch, 2, keepdims=False)
    head_final = jnp.where(head_owned, own_head, head_fix)
    coefficients = lax.dynamic_update_slice(
        coefficients, head_final[:, :, None], (jnp.int32(0), jnp.int32(0), first_batch)
    )

    def correct_step(batch_id, running):
        in_batch = (batch_of == batch_id).astype(jnp.float32)
        slope_table = lax.dynamic_index_in_dim(coefficients, batch_id, 2, keepdims=False)
        moved = jnp.einsum("kd,kn->dn", slope_table, assign * in_batch[None, :], precision=highest)
        return running + moved

    corrected = lax.fori_loop(first_batch, last_batch + 1, correct_step, jnp.zeros_like(latent_coordinates))
    return (latent_coordinates - corrected, new_centroids)


SLOTS = 8
ROWS = 64
MOST = 10485
LOGICAL = pl.DeviceIdType.LOGICAL
TILE = 256
CLOSE = 4
bf16, f32 = jnp.bfloat16, jnp.float32


def two_pieces(value):
    first = value.astype(bf16)
    return first, (value - first.astype(f32)).astype(bf16)


def across(left, right):
    return lax.dot_general(left, right, (((1,), (1,)), ((), ())), preferred_element_type=f32)


def plain(left, right):
    return jnp.dot(left, right, preferred_element_type=f32)


def step_kernel(
    shape,
    cells_all,
    z_hbm,
    means_hbm,
    soft_hbm,
    ridge_hbm,
    pop_hbm,
    zf,
    pair,
    slopes,
    starts_ref,
    flag_ref,
    cent_ref,
    means_ref,
    soft_ref,
    ridge_ref,
    pop_ref,
    zc,
    ex,
    lined,
    means_wide,
    pieces,
    near_out,
    near_counts,
    near_mass,
    near_moments,
    ends_out,
    full_moments,
    line_out,
    line_a,
    line_b,
    sums_out,
    sum_in,
    cent_out,
    cent_in,
    shrinks,
    cent_y,
    cent_z,
    tile_out,
    sum_y,
    sum_z,
    full_sums,
    small_sems,
    load_sems,
    send_sems,
    recv_sems,
):
    nz, ny, nc, nx = shape
    near = nc * nx
    far = nz * ny
    count = near * far
    cells = zf.shape[1]
    pcs, clusters = means_ref.shape
    batches = pop_ref.shape[1]
    rows_each = ROWS // near
    width = 512
    reach = (MOST - 2) // cells + 1
    offsets = [h for h in range(-reach, reach + 1) if h]
    me = (
        (lax.axis_index("cells_0") * ny + lax.axis_index("cells_1")) * nc
        + lax.axis_index("cells_2")
    ) * nx + lax.axis_index("grp")
    rank = lax.rem(me, near)
    block = lax.div(me, near)

    def mate(r):
        return block * near + lax.rem(rank + r, near)

    plane = near * ny
    in_plane = lax.rem(me, plane)

    def beside(r):
        return me - in_plane + lax.rem(in_plane + r, plane)

    def along_y(r):
        at = lax.rem(block, ny)
        return (block - at + lax.rem(at + r, ny)) * near + rank

    def along_z(r):
        return lax.rem(block + r * ny, far) * near + rank

    def neighbour(h):
        return lax.rem(me + (h + count), count)

    def push(src, dst, which, q):
        pltpu.make_async_remote_copy(
            src_ref=src,
            dst_ref=dst,
            send_sem=send_sems.at[which],
            recv_sem=recv_sems.at[which],
            device_id=q,
            device_id_type=LOGICAL,
        ).start()

    def arrived(buffer, which):
        pltpu.make_async_copy(buffer, buffer, recv_sems.at[which]).wait()

    def left(buffer, which):
        pltpu.make_async_copy(buffer, buffer, send_sems.at[which]).wait()

    small = [
        pltpu.make_async_copy(src, dst, small_sems.at[i])
        for i, (src, dst) in enumerate(
            (
                (pop_hbm, pop_ref),
                (means_hbm, means_ref),
                (soft_hbm, soft_ref),
                (ridge_hbm, ridge_ref),
            )
        )
    ]
    for copy in small:
        copy.start()
    for i in range(cells // width):
        columns = pl.ds(i * width, width)
        pltpu.make_async_copy(z_hbm.at[0, :, columns], zf.at[:, columns], load_sems.at[i]).start()

    barrier = pltpu.get_barrier_semaphore()
    greeted = [along_z(r) for r in range(1, nz)] + [beside(r) for r in range(1, plane)]
    greeted = greeted + [neighbour(h) for h in offsets]
    for q in greeted:
        pl.semaphore_signal(barrier, inc=1, device_id=q, device_id_type=LOGICAL)

    for copy in small:
        copy.wait()

    means_wide[...] = jnp.zeros_like(means_wide)
    means_wide[0:pcs, :] = means_ref[...]
    g = means_wide[...].T
    square = lax.broadcasted_iota(jnp.int32, (clusters, clusters), 0)
    lane = lax.broadcasted_iota(jnp.int32, (clusters, clusters), 1)
    soft = jnp.sum(jnp.where(square == lane, soft_ref[...], 0.0), axis=1, keepdims=True)
    offset_of = -0.5 * jnp.sum(g * g, axis=1, keepdims=True) / soft
    weights = jnp.where(lane == pcs, offset_of, g / soft)
    w1 = weights.astype(bf16).astype(f32)
    w2 = (weights - w1).astype(bf16).astype(f32)
    o1 = offset_of.astype(bf16).astype(f32)
    o2 = (offset_of - o1).astype(bf16).astype(f32)
    w1 = jnp.where(lane == pcs + 1, offset_of - o1 - o2, w1)
    w1 = (w1 + pltpu.roll(w1, ROWS, 1)).astype(bf16)
    w2 = (w2 + pltpu.roll(w2, ROWS, 1)).astype(bf16)
    weights = jnp.concatenate([w1, w2], axis=1)

    pop = pop_ref[...]
    up = lax.broadcasted_iota(jnp.int32, (batches, batches), 0)
    down = lax.broadcasted_iota(jnp.int32, (batches, batches), 1)
    column = jnp.sum(jnp.where(up == down, pop, 0), axis=1, keepdims=True)
    ends = jnp.sum(jnp.where(up <= down, column, 0), axis=0, keepdims=True)
    half = lax.broadcasted_iota(jnp.int32, (16, 1), 0)
    device = me + lax.rem(half, 8) - reach
    limit = device * cells + jnp.where(half >= 8, cells - 1, 0)
    spot = jnp.sum(jnp.where(ends <= limit, 1, 0), axis=1, keepdims=True)
    spot = jnp.where(device < 0, -9, spot)
    first = {h: spot[h + reach : h + reach + 1] for h in offsets + [0]}
    last = {h: spot[8 + h + reach : 9 + h + reach] for h in offsets + [0]}
    slot = lax.broadcasted_iota(jnp.int32, (SLOTS, 1), 0)
    batch_id = first[0] + slot
    batch_lane = lax.broadcasted_iota(jnp.int32, (SLOTS, batches), 1)
    chosen = batch_lane == batch_id
    held = jnp.sum(jnp.where(chosen, pop, 0), axis=1, keepdims=True)
    ridge = jnp.sum(jnp.where(chosen, ridge_ref[...], 0.0), axis=1, keepdims=True)
    ridge = jnp.where(batch_id < batches, ridge, 1.0)
    stop = jnp.sum(jnp.where(batch_lane <= batch_id, pop, 0), axis=1, keepdims=True) - me * cells
    start = stop - held
    held = held.astype(f32)
    starts_ref[...] = jnp.broadcast_to(jnp.where(batch_id < batches, start, 2 * cells), (SLOTS, 128))
    tail = slot == last[0] - first[0]
    head = slot == 0
    behind = {h: (last[h] == first[0]).astype(f32) for h in offsets if h < 0}
    ahead = {h: (first[h] == last[0]).astype(f32) for h in offsets if h > 0}

    wide = near - 1 + reach
    row32 = lax.broadcasted_iota(jnp.int32, (32, 1), 0)
    device = block * near + lax.rem(row32, 16) - reach
    limit = device * cells + jnp.where(row32 >= 16, cells - 1, 0)
    ids = jnp.sum(jnp.where(ends <= limit, 1, 0), axis=1, keepdims=True)
    ids = jnp.where(device < 0, -9, ids)
    limit = (block * near + lax.rem(half, 8)) * cells + jnp.where(half >= 8, cells - 1, 0)
    own_ids = jnp.sum(jnp.where(ends <= limit, 1, 0), axis=1, keepdims=True)
    own_lane = lax.broadcasted_iota(jnp.int32, (16, batches), 1)
    own_ridge = jnp.sum(jnp.where(own_lane == own_ids, ridge_ref[...], 0.0), axis=1, keepdims=True)

    crowded = jnp.zeros((1, 1), jnp.int32)
    for inner, room in ((SLOTS - 1, cells), (CLOSE - 1, width)):
        window = jnp.sum(
            jnp.where((up >= down) & (up < down + inner), column, 0), axis=0, keepdims=True
        )
        window = jnp.where((window < room - 1) & (batch_lane[0:1] <= batches - inner), 1, 0)
        crowded = crowded + jnp.sum(window, axis=1, keepdims=True)
    flag_ref[...] = jnp.broadcast_to(crowded, (1, 128))

    def inside(c, width, times):
        position = lax.broadcasted_iota(jnp.int32, (SLOTS * times, width), 1) + c * width
        low = jnp.concatenate([start] * times, axis=0)
        high = jnp.concatenate([stop] * times, axis=0)
        return ((position >= low) & (position < high)).astype(f32)

    def completed(own, buffer):
        before = jnp.zeros((1, clusters), f32)
        after = jnp.zeros((1, clusters), f32)
        for i, h in enumerate(offsets):
            if h < 0:
                before = before + behind[h] * buffer[i][1:2]
            else:
                after = after + ahead[h] * buffer[i][0:1]
        return own + jnp.where(head, before, 0.0) + jnp.where(tail, after, 0.0)

    def tail_of(value):
        return jnp.sum(jnp.where(tail, value, 0.0), axis=0, keepdims=True)

    def greeted_rows(which, value):
        near_out[which, 0:1, :] = value[0:1]
        near_out[which, 1:2, :] = tail_of(value)

    runs = cells // width

    def base_of(c):
        return jnp.sum(
            jnp.where((start <= c * width) & (slot > 0) & (batch_id < batches), 1, 0),
            axis=0,
            keepdims=True,
        )


    for i in range(runs):
        columns = pl.ds(i * width, width)
        pltpu.make_async_copy(z_hbm.at[0, :, columns], zf.at[:, columns], load_sems.at[i]).wait()
    z1, z2 = two_pieces(
        jnp.concatenate(
            [
                zf[...],
                jnp.ones((2, cells), f32),
                jnp.zeros((ROWS - 2 - pcs, cells), f32),
            ],
            axis=0,
        )
    )
    zc[0:ROWS, :] = z1
    zc[ROWS : 2 * ROWS, :] = z2
    score = plain(weights, jnp.concatenate([z1, z2, z1, z2], axis=0))
    raised = jnp.exp(score - jnp.max(score, axis=0, keepdims=True))
    ex[...] = raised
    p1, p2 = two_pieces(raised * (1.0 / jnp.sum(raised, axis=0, keepdims=True)))
    mask = inside(0, cells, 2).astype(bf16)
    total = across(mask, jnp.concatenate([p1, p2], axis=0))
    counts = total[0:SLOTS, 0:clusters] + total[0:SLOTS, clusters : 2 * clusters]
    own_total = jnp.sum(counts, axis=0, keepdims=True)
    greeted_rows(0, counts)
    line_out[0] = own_total
    pl.semaphore_wait(barrier, len(greeted))
    for r in range(1, plane):
        push(line_out.at[0], line_a.at[r - 1], 0, beside(r))
    for i, h in enumerate(offsets):
        push(near_out.at[0], near_counts.at[len(offsets) - 1 - i], 1, neighbour(h))

    def line_up(c):
        columns = slice(c * width, (c + 1) * width)
        mask = inside(c, width, 1)
        kind = jnp.sum(mask * slot.astype(f32), axis=0, keepdims=True)
        kind = kind - base_of(c).astype(f32)
        z = zc[:, columns]
        for j in range(CLOSE):
            lined[2 * ROWS * j : 2 * ROWS * (j + 1), columns] = z * (kind == j).astype(
                f32
            ).astype(bf16)

    for c in range(runs // 2):
        line_up(c)
    arrived(line_a, 0)
    plane_total = own_total + jnp.sum(line_a[...], axis=0)
    line_out[1] = plane_total
    for r in range(1, nz):
        push(line_out.at[1], line_b.at[r - 1], 2, along_z(r))
    for c in range(runs // 2, runs):
        line_up(c)
    arrived(near_counts, 1)
    full_counts = completed(counts, [near_counts[i] for i in range(len(offsets))])
    arrived(line_b, 2)
    totals = plane_total + jnp.sum(line_b[...], axis=0)
    expected = held * totals * (1.0 / cells_all)
    ratio = (expected + 1.0) / (full_counts + 1.0)
    factor = ratio * ratio
    f1 = factor.astype(bf16).astype(f32)
    f2 = (factor - f1).astype(bf16).astype(f32)
    f3 = factor - f1 - f2
    factor = jnp.concatenate([f1, f2, f3, jnp.zeros_like(f3)], axis=0).T.astype(bf16)

    mask = inside(0, cells, 4).astype(bf16)
    weighed = ex[...] * plain(factor, mask)
    a1, a2 = two_pieces(weighed * (1.0 / jnp.sum(weighed, axis=0, keepdims=True)))
    both = jnp.concatenate([a1, a2], axis=0)
    pair[...] = both
    total = across(mask[0 : 2 * SLOTS], both)
    mass = total[0:SLOTS, 0:clusters] + total[0:SLOTS, clusters : 2 * clusters]
    greeted_rows(1, mass)
    around = 2 * wide + 1
    for h in range(1, wide + 1):
        push(near_out.at[1], near_mass.at[(around - 1 - h) % around], 3, neighbour(h))
        push(near_out.at[1], near_mass.at[(around - 1 + h) % around], 3, neighbour(-h))
    near_mass[around - 1] = near_out[1]

    for c in range(runs):
        columns = slice(c * width, (c + 1) * width)
        value = across(lined[:, columns], pair[:, columns])
        for j in range(CLOSE):
            top = value[2 * ROWS * j : 2 * ROWS * j + ROWS]
            low = value[2 * ROWS * j + ROWS : 2 * ROWS * (j + 1)]
            pieces[c, j] = (
                top[:, 0:clusters] + top[:, clusters:] + low[:, 0:clusters] + low[:, clusters:]
            )
    places = [(c, j) for c in range(runs) for j in range(CLOSE)]
    tail_slot = last[0] - first[0]
    alone = jnp.where(tail_slot > 0, 1.0, 0.0)
    shrink = jnp.where(head | tail, 0.0, ridge / (mass + ridge))
    first_moment = jnp.zeros((ROWS, clusters), f32)
    tail_moment = jnp.zeros((ROWS, clusters), f32)
    whole = jnp.zeros((ROWS, clusters), f32)
    right = jnp.zeros((ROWS, clusters), f32)
    for c in range(runs):
        base = base_of(c)
        for j in range(CLOSE):
            piece = pieces[c, j]
            line = jnp.sum(jnp.where(slot == base + j, shrink, 0.0), axis=0, keepdims=True)
            right = right + line * piece
            tail_moment = tail_moment + jnp.where(base + j == tail_slot, 1.0, 0.0) * piece
            whole = whole + piece
            if j == 0:
                first_moment = first_moment + jnp.where(base == 0, 1.0, 0.0) * piece
    for t in range(near):
        inner = slice(t * rows_each, (t + 1) * rows_each)
        sums_out[t, 0] = right[inner]
        sums_out[t, 1] = first_moment[inner]
        sums_out[t, 2] = tail_moment[inner] * alone
        cent_out[t] = whole[inner]
    for r in range(1, near):
        push(sums_out.at[lax.rem(rank + r, near)], sum_in.at[r - 1], 5, mate(r))
    for r in range(1, near):
        push(cent_out.at[lax.rem(rank + r, near)], cent_in.at[r - 1], 4, mate(r))
    ends_out[0] = first_moment[0:56]
    ends_out[1] = tail_moment[0:56]
    arrived(near_mass.at[pl.ds(0, around - 1)], 3)
    full_mass = completed(
        mass, {i: near_mass[(around - 1 + h) % around] for i, h in enumerate(offsets)}
    )
    end_mass = jnp.zeros((16, clusters), f32)
    for p in range(-reach, near + reach):
        both = near_mass[lax.rem(p + (2 * around - 1) - rank, around)]
        one, two = ids[p + reach : p + reach + 1], ids[16 + p + reach : 17 + p + reach]
        end_mass = end_mass + jnp.where(own_ids == one, both[0:1], 0.0)
        end_mass = end_mass + jnp.where((own_ids == two) & (two != one), both[1:2], 0.0)
    end_shrink = own_ridge / (end_mass + own_ridge)
    for t in range(near):
        shrinks[t, 0:1, :] = end_shrink[t : t + 1]
        shrinks[t, 1:2, :] = end_shrink[8 + t : 9 + t]
    arrived(sum_in, 5)
    sum_tile = jnp.zeros((rows_each, clusters), f32)
    for r in range(near):
        by = shrinks[lax.rem(rank + near - r, near)]
        got = sums_out[rank] if r == 0 else sum_in[r - 1]
        sum_tile = sum_tile + got[0] + got[1] * by[0:1] + got[2] * by[1:2]
    tile_out[2] = sum_tile
    for r in range(1, ny):
        push(tile_out.at[2], sum_y.at[r - 1], 8, along_y(r))
    arrived(cent_in, 4)
    cent_tile = cent_out[rank]
    for r in range(near - 1):
        cent_tile = cent_tile + cent_in[r]
    tile_out[0] = cent_tile
    arrived(sum_y, 8)
    for r in range(ny - 1):
        sum_tile = sum_tile + sum_y[r]
    tile_out[3] = sum_tile
    for r in range(1, nz):
        push(tile_out.at[3], sum_z.at[r - 1], 12, along_z(r))
    for r in range(1, ny):
        push(tile_out.at[0], cent_y.at[r - 1], 7, along_y(r))
    for i, h in enumerate(offsets):
        push(ends_out.at[int(h > 0)], near_moments.at[len(offsets) - 1 - i], 6, neighbour(h))
    arrived(cent_y, 7)
    for r in range(ny - 1):
        cent_tile = cent_tile + cent_y[r]
    tile_out[1] = cent_tile
    for r in range(1, nz):
        push(tile_out.at[1], cent_z.at[r - 1], 11, along_z(r))
    moments = []
    for s in range(SLOTS):
        moment = jnp.zeros((ROWS, clusters), f32)
        for c, j in places:
            if j <= s <= CLOSE * c + j:
                moment = moment + jnp.where(base_of(c) + j == s, 1.0, 0.0) * pieces[c, j]
        moments.append(moment)

    arrived(sum_z, 12)
    full_sums[1, 0] = sum_tile + jnp.sum(sum_z[...], axis=0)
    for r in range(1, near):
        push(full_sums.at[1, 0], full_sums.at[1, r], 10, mate(r))
    arrived(near_moments, 6)
    before = jnp.zeros((56, clusters), f32)
    after = jnp.zeros((56, clusters), f32)
    for i, h in enumerate(offsets):
        if h < 0:
            before = before + behind[h] * near_moments[i]
        else:
            after = after + ahead[h] * near_moments[i]
    for s in range(SLOTS):
        moment = moments[s][0:56] + after * tail[s : s + 1].astype(f32)
        full_moments[s] = moment + before if s == 0 else moment

    arrived(cent_z, 11)
    for r in range(nz - 1):
        cent_tile = cent_tile + cent_z[r]
    full_sums[0, 0] = cent_tile
    for r in range(1, near):
        push(full_sums.at[0, 0], full_sums.at[0, r], 9, mate(r))

    def gathered(which):
        return jnp.concatenate(
            [full_sums[which, lax.rem(rank + (near - t), near)] for t in range(near)], axis=0
        )

    arrived(full_sums.at[1, pl.ds(1, near - 1)], 10)
    right = gathered(1)
    intercept = (right / (1.0 + right[pcs : pcs + 1]))[0:56]
    for s in range(SLOTS):
        moment = full_moments[s]
        line = full_mass[s : s + 1]
        slope = (moment - line * intercept) / (line + ridge[s : s + 1])
        c1, c2 = two_pieces(jnp.concatenate([slope, jnp.zeros((8, clusters), f32)], axis=0))
        slopes[ROWS * s : ROWS * (s + 1), :] = jnp.concatenate([c1, c1, c2], axis=1)

    arrived(full_sums.at[0, pl.ds(1, near - 1)], 9)
    centre = gathered(0)
    centre = (centre / (1.0 + centre[pcs : pcs + 1])).T
    owned = cent_ref.shape[0]
    cells_at = lax.div(me, nx)
    row = lax.broadcasted_iota(jnp.int32, (clusters, ROWS), 0)
    for j in range(owned):
        line = jnp.sum(jnp.where(row == cells_at * owned + j, centre, 0.0), axis=0, keepdims=True)
        cent_ref[j : j + 1, :] = line[:, 0:pcs]

    left(line_a, 0)
    left(near_counts, 1)
    left(line_b, 2)
    left(near_mass.at[pl.ds(0, around - 1)], 3)
    left(cent_in, 4)
    left(sum_in, 5)
    left(near_moments, 6)
    left(cent_y, 7)
    left(sum_y, 8)
    left(sum_z, 12)
    left(cent_z, 11)
    left(full_sums.at[0, pl.ds(1, near - 1)], 9)
    left(full_sums.at[1, pl.ds(1, near - 1)], 10)


def correct_kernel(
    zf, pair, slopes, starts_ref, cent_ref, out_hbm, cent_hbm, held, starts, out_sems
):
    pcs, cells = zf.shape
    clusters = pair.shape[0] // 2
    loads = out_sems.shape[0] - 1
    part = cells // loads
    cent = pltpu.make_async_copy(cent_ref, cent_hbm, out_sems.at[loads])
    cent.start()
    begin = [jnp.max(starts_ref[s : s + 1, :]) for s in range(SLOTS)]
    for s in range(SLOTS):
        starts[s] = begin[s]
    lane = lax.broadcasted_iota(jnp.int32, (1, TILE), 1)

    def slope_of(j):
        return slopes[pl.ds(pl.multiple_of(j * ROWS, ROWS), ROWS), :]

    def slots_of(t):
        base = jnp.int32(0)
        final = jnp.int32(0)
        border = jnp.int32(2 * cells)
        for s in range(1, SLOTS):
            base = base + jnp.where(begin[s] <= t * TILE, 1, 0)
            final = final + jnp.where(begin[s] < (t + 1) * TILE, 1, 0)
            border = jnp.where(begin[s] > t * TILE, jnp.minimum(border, begin[s]), border)
        return base, final, border

    def send_out(i):
        columns = pl.ds(i * part, part)
        return pltpu.make_async_copy(
            held.at[:, columns], out_hbm.at[:, columns], out_sems.at[i]
        )

    beyond = jnp.int32(0)
    for i in range(loads):
        for t in range(i * part // TILE, (i + 1) * part // TILE):
            columns = slice(t * TILE, (t + 1) * TILE)
            base, final, border = slots_of(t)
            beyond = jnp.maximum(beyond, final - base)
            following = jnp.minimum(base + 1, SLOTS - 1)
            both = pair[:, columns]
            both = jnp.concatenate([both, both[0:clusters]], axis=0)
            moved = plain(jnp.concatenate([slope_of(base), slope_of(following)], axis=0), both)
            moved = jnp.where(lane < border - t * TILE, moved[0:ROWS], moved[ROWS:])
            held[:, columns] = zf[:, columns] - moved[0:pcs]
        send_out(i).start()
    for i in range(loads):
        send_out(i).wait()
    cent.wait()

    @pl.when(beyond > 1)
    def _():
        def tile_of(t, carry):
            columns = pl.ds(pl.multiple_of(t * TILE, TILE), TILE)
            base, final, border = slots_of(t)

            def more(j, carry):
                both = pair[:, columns]
                both = jnp.concatenate([both, both[0:clusters]], axis=0)
                other = zf[:, columns] - plain(slope_of(j), both)[0:pcs]
                held[:, columns] = jnp.where(
                    lane >= starts[j] - t * TILE, other, held[:, columns]
                )
                return carry

            lax.fori_loop(base + 2, final + 1, more, 0)
            return carry

        lax.fori_loop(0, cells // TILE, tile_of, 0)
        for i in range(loads):
            send_out(i).start()
        for i in range(loads):
            send_out(i).wait()


def narrow_body(
    shape, latent_coordinates, group_means, entropy_scaling, sample_shrinkage_lambda, sample_population
):
    pcs, cells = latent_coordinates.shape
    clusters = group_means.shape[0]
    batches = sample_population.shape[0]
    nz, ny, nc, nx = shape
    near, far = nc * nx, nz * ny
    rows_each = ROWS // near
    reach = (MOST - 2) // cells + 1
    owned = clusters // (nz * ny * nc)
    vmem = pl.BlockSpec(memory_space=pltpu.VMEM)
    tile = (rows_each, clusters)
    scratch = [
        pltpu.VMEM((pcs, clusters), f32),
        pltpu.VMEM((1, clusters), f32),
        pltpu.VMEM((1, batches), f32),
        pltpu.VMEM((1, batches), jnp.int32),
        pltpu.VMEM((2 * ROWS, cells), bf16),
        pltpu.VMEM((clusters, cells), f32),
        pltpu.VMEM((2 * ROWS * CLOSE, cells), bf16),
        pltpu.VMEM((clusters, clusters), f32),
        pltpu.VMEM((cells // 512, CLOSE, ROWS, clusters), f32),
        pltpu.VMEM((2, 2, clusters), f32),
        pltpu.VMEM((2 * reach, 2, clusters), f32),
        pltpu.VMEM((2 * (near - 1 + reach) + 1, 2, clusters), f32),
        pltpu.VMEM((2 * reach, 56, clusters), f32),
        pltpu.VMEM((2, 56, clusters), f32),
        pltpu.VMEM((SLOTS, 56, clusters), f32),
        pltpu.VMEM((2, 1, clusters), f32),
        pltpu.VMEM((near * ny - 1, 1, clusters), f32),
        pltpu.VMEM((nz - 1, 1, clusters), f32),
        pltpu.VMEM((near, 3, *tile), f32),
        pltpu.VMEM((near - 1, 3, *tile), f32),
        pltpu.VMEM((near, *tile), f32),
        pltpu.VMEM((near - 1, *tile), f32),
        pltpu.VMEM((near, 2, clusters), f32),
        pltpu.VMEM((ny - 1, *tile), f32),
        pltpu.VMEM((nz - 1, *tile), f32),
        pltpu.VMEM((4, *tile), f32),
        pltpu.VMEM((ny - 1, *tile), f32),
        pltpu.VMEM((nz - 1, *tile), f32),
        pltpu.VMEM((2, near, *tile), f32),
        pltpu.SemaphoreType.DMA((4,)),
        pltpu.SemaphoreType.DMA((cells // 512,)),
        pltpu.SemaphoreType.DMA((13,)),
        pltpu.SemaphoreType.DMA((13,)),
    ]
    return pl.pallas_call(
        functools.partial(step_kernel, shape, float(cells * near * far)),
        out_shape=(
            pltpu.VMEM((pcs, cells), f32),
            pltpu.VMEM((2 * clusters, cells), bf16),
            pltpu.VMEM((SLOTS * ROWS, 3 * clusters), bf16),
            pltpu.VMEM((SLOTS, 128), jnp.int32),
            pltpu.VMEM((1, 128), jnp.int32),
            pltpu.VMEM((owned, pcs), f32),
        ),
        in_specs=[pl.BlockSpec(memory_space=pl.ANY)] * 5,
        out_specs=(vmem,) * 6,
        scratch_shapes=scratch,
        compiler_params=pltpu.CompilerParams(
            collective_id=0, has_side_effects=True, vmem_limit_bytes=44 * 1024 * 1024
        ),
    )(
        latent_coordinates[None],
        group_means.T,
        entropy_scaling.reshape(1, clusters),
        sample_shrinkage_lambda.reshape(1, batches),
        sample_population.reshape(1, batches),
    )


def corrected_by(kept, pair, slopes, starts, new_centroids):
    pcs, cells = kept.shape
    vmem = pl.BlockSpec(memory_space=pltpu.VMEM)
    anywhere = pl.BlockSpec(memory_space=pl.ANY)
    return pl.pallas_call(
        correct_kernel,
        out_shape=(pltpu.HBM((pcs, cells), f32), pltpu.HBM(new_centroids.shape, f32)),
        in_specs=[vmem] * 5,
        out_specs=(anywhere, anywhere),
        scratch_shapes=[
            pltpu.VMEM((pcs, cells), f32),
            pltpu.SMEM((SLOTS,), jnp.int32),
            pltpu.SemaphoreType.DMA((5,)),
        ],
        compiler_params=pltpu.CompilerParams(vmem_limit_bytes=16 * 1024 * 1024),
    )(
        kept,
        pair,
        slopes,
        starts,
        new_centroids,
    )


def body(
    shape, latent_coordinates, group_means, entropy_scaling, sample_shrinkage_lambda, sample_population
):
    arguments = (
        latent_coordinates,
        group_means,
        entropy_scaling,
        sample_shrinkage_lambda,
        sample_population,
    )
    kept, pair, slopes, starts, flag, new_centroids = narrow_body(shape, *arguments)
    return lax.cond(
        flag[0, 0] == 0,
        lambda: corrected_by(kept, pair, slopes, starts, new_centroids),
        lambda: wide_body(*arguments),
    )


def solution(mesh):
    shape = (mesh.shape["cells"] // 8, 4, 2, mesh.shape["grp"])
    finer = Mesh(mesh.devices.reshape(shape), ("cells_0", "cells_1", "cells_2", "grp"))
    return jax.shard_map(
        functools.partial(body, shape),
        mesh=finer,
        in_specs=(P(None, CELLS_GRP), P(), P(), P(), P()),
        out_specs=(P(None, CELLS_GRP), P(CELLS, None)),
        check_vma=False,
    )
```

```python
import functools

import jax
import jax.numpy as jnp
from jax import lax
from jax.experimental import pallas as pl
from jax.experimental.pallas import tpu as pltpu
from jax.sharding import Mesh
from jax.sharding import PartitionSpec as P

CELLS = ("cells_0", "cells_1", "cells_2")
CELLS_GRP = ("cells_0", "cells_1", "cells_2", "grp")


diversity = 2.0
intercept_ridge = 1.0
highest = lax.Precision.HIGHEST


def split_up(array, dim, size):
    dims = array.shape
    parts = array.reshape(*dims[:dim], size, dims[dim] // size, *dims[dim + 1 :])
    return jnp.moveaxis(parts, dim, 0)


def summed_on_arrival(array, axis, dim):
    size = lax.axis_size(axis)
    parts = lax.all_to_all(split_up(array, dim, size), axis, 0, 0, tiled=True)
    return jnp.sum(parts, axis=0)


def sum_in_two_steps(array, axes, dim):
    far, near = axes
    parts = split_up(array, dim, lax.axis_size(far))
    nearer = summed_on_arrival(parts, near, dim + 1)
    arrived = lax.all_to_all(nearer, far, split_axis=0, concat_axis=0, tiled=True)
    return arrived.sum(axis=0)


def filled_up(lines, size):
    spare = -len(lines) % size
    return jnp.pad(lines, [(0, spare)] + [(0, 0)] * (lines.ndim - 1))


def sent_to_all(array, axis):
    size = lax.axis_size(axis)
    return lax.all_to_all(
        jnp.broadcast_to(array[None], (size, *array.shape)), axis, 0, 0, tiled=True
    )


def joined_along(parts, dim):
    parts = jnp.moveaxis(parts, 0, dim)
    dims = parts.shape
    return parts.reshape(*dims[:dim], dims[dim] * dims[dim + 1], *dims[dim + 2 :])


def gather_axes(array, axes, dim):
    far, near = axes
    leading = sent_to_all(array, far)
    parts = jnp.swapaxes(sent_to_all(leading, near), 0, 1)
    return joined_along(parts.reshape(-1, *array.shape), dim)


def total_of(array, axes):
    lines = array.reshape(-1)
    own = sum_in_two_steps(
        filled_up(lines, lax.axis_size(axes[0]) * lax.axis_size(axes[1])), axes, 0
    )
    whole = gather_axes(own, axes, 0)
    return whole[: len(lines)].reshape(array.shape)


def from_behind(block, axis, distance):
    devices = range(lax.axis_size(axis))
    route = [(i - distance, i) for i in devices if i - distance in devices]
    return lax.ppermute(block, axis, route)


def by_axis(array, axes):
    return functools.reduce(lax.psum, axes, array)


def observation_affinity(latent_coordinates, group_means, entropy_scaling):
    pairwise_dots = jnp.dot(
        group_means, latent_coordinates, precision=highest, preferred_element_type=jnp.float32
    )
    quadratic_lengths = jnp.sum(group_means * group_means, axis=1)
    return (2.0 * pairwise_dots - quadratic_lengths[:, None]) / (2.0 * entropy_scaling[:, None])


def probabilistic_responsibility(group_affinity):
    top = jnp.max(group_affinity, axis=0, keepdims=True)
    raised = jnp.exp(group_affinity - top)
    return raised / jnp.sum(raised, axis=0, keepdims=True)


def batch_parts(moments, ridge):
    mass = moments[:, 0, :]
    sums = moments[:, 1:, :]
    shrink = ridge[None, :] / (mass + ridge[None, :])
    weight = jnp.sum(mass * shrink, axis=1)
    right_side = jnp.sum(sums * shrink[:, None, :], axis=2)
    return (weight, right_side, jnp.sum(mass, axis=1), jnp.sum(sums, axis=2))


def slopes_of(moments, ridge, weight, right_side):
    mass = moments[:, 0, :]
    sums = moments[:, 1:, :]
    intercept = right_side / (intercept_ridge + weight)[:, None]
    return (sums - mass[:, None, :] * intercept[:, :, None]) / (mass + ridge[None, :])[:, None, :]


def wide_body(
    latent_coordinates, group_means, entropy_scaling, sample_shrinkage_lambda, sample_population
):
    local_cells = latent_coordinates.shape[1]
    num_pcs = latent_coordinates.shape[0]
    clusters = group_means.shape[0]
    batches = sample_population.shape[0]
    owned = clusters // lax.axis_size(CELLS)
    offset = (lax.axis_index(CELLS) * lax.axis_size("grp") + lax.axis_index("grp")) * local_cells
    batch_ends = jnp.cumsum(sample_population)
    batch_starts = batch_ends - sample_population
    cells_total = jnp.sum(sample_population).astype(jnp.float32)
    position = offset + lax.iota(jnp.int32, local_cells)
    batch_of = jnp.sum((batch_ends[:, None] <= position[None, :]).astype(jnp.int32), axis=0)
    first_batch = batch_of[0]
    last_batch = batch_of[local_cells - 1]
    group_affinity = observation_affinity(latent_coordinates, group_means, entropy_scaling)
    expected_occupancy = probabilistic_responsibility(group_affinity)

    def count_step(batch_id, running):
        in_batch = (batch_of == batch_id).astype(jnp.float32)
        single_observation = jnp.dot(
            expected_occupancy, in_batch, precision=highest, preferred_element_type=jnp.float32
        )
        return lax.dynamic_update_slice(
            running, single_observation[:, None], (jnp.int32(0), batch_id)
        )

    counts = lax.fori_loop(
        first_batch, last_batch + 1, count_step, jnp.zeros((clusters, batches), jnp.float32)
    )
    counts = total_of(counts, (("cells_0", "cells_1"), ("cells_2", "grp")))
    totals = jnp.sum(counts, axis=1)
    expected = sample_population.astype(jnp.float32)[None, :] * totals[:, None] / cells_total
    penalty = diversity * jnp.log((counts + 1.0) / (expected + 1.0))

    def penalty_step(batch_id, running):
        in_batch = (batch_of == batch_id).astype(jnp.float32)
        column = lax.dynamic_index_in_dim(penalty, batch_id, 1, keepdims=True)
        return running + column * in_batch[None, :]

    cell_penalty = lax.fori_loop(
        first_batch, last_batch + 1, penalty_step, jnp.zeros((clusters, local_cells), jnp.float32)
    )
    assign = probabilistic_responsibility(group_affinity - cell_penalty)
    augmented = jnp.concatenate(
        [jnp.ones((1, local_cells), jnp.float32), latent_coordinates], axis=0
    )

    def moment_step(batch_id, running):
        in_batch = (batch_of == batch_id).astype(jnp.float32)
        contiguous_portion = jnp.einsum(
            "kn,dn->kd", assign * in_batch[None, :], augmented, precision=highest
        )
        return lax.dynamic_update_slice(
            running, contiguous_portion[:, :, None], (jnp.int32(0), jnp.int32(0), batch_id)
        )

    moments = lax.fori_loop(
        first_batch,
        last_batch + 1,
        moment_step,
        jnp.zeros((clusters, num_pcs + 1, batches), jnp.float32),
    )
    devices_flat = lax.axis_size(CELLS) * lax.axis_size("grp")
    most_cells = 2 * local_cells * devices_flat // batches
    reach = (most_cells - 2) // local_cells + 1
    begins_here = (batch_starts >= offset) & (batch_starts < offset + local_cells)
    owner_mask = begins_here.astype(jnp.float32)
    head_owned = begins_here[first_batch]
    head_column = lax.dynamic_index_in_dim(moments, first_batch, 2, keepdims=False)
    sent_stats = jnp.where(head_owned, 0.0, 1.0) * head_column
    sent_tag = jnp.where(head_owned, 0.0, first_batch.astype(jnp.float32) + 1.0) * jnp.ones(
        (1,), jnp.float32
    )
    completed = moments
    for hop in range(1, reach + 1):
        got_stats, got_tag = from_behind((sent_stats, sent_tag), CELLS_GRP, -hop)
        got_id = jnp.maximum(got_tag[0].astype(jnp.int32) - 1, 0)
        accept = jnp.where((got_tag[0] > 0.5) & begins_here[got_id], 1.0, 0.0)
        single_observation = (
            lax.dynamic_index_in_dim(completed, got_id, 2, keepdims=False) + accept * got_stats
        )
        completed = lax.dynamic_update_slice(
            completed, single_observation[:, :, None], (jnp.int32(0), jnp.int32(0), got_id)
        )
    completed = completed * owner_mask[None, None, :]
    weight, right_side, mass_total, moment_total = jax.tree.map(
        lambda part: by_axis(part, CELLS_GRP), batch_parts(completed, sample_shrinkage_lambda)
    )
    coefficients = slopes_of(completed, sample_shrinkage_lambda, weight, right_side)
    every_centroid = moment_total / (1.0 + mass_total)[:, None]
    new_centroids = lax.dynamic_slice_in_dim(
        every_centroid, lax.axis_index(CELLS) * owned, owned, 0
    )
    tail_owned = begins_here[last_batch]
    tail_column = lax.dynamic_index_in_dim(coefficients, last_batch, 2, keepdims=False)
    tail_send = jnp.where(tail_owned, 1.0, 0.0) * tail_column
    tail_tag = jnp.where(tail_owned, last_batch.astype(jnp.float32) + 1.0, 0.0) * jnp.ones(
        (1,), jnp.float32
    )
    head_fix = jnp.zeros_like(tail_column)
    for hop in range(1, reach + 1):
        got_coef, got_tag = from_behind((tail_send, tail_tag), CELLS_GRP, hop)
        match = got_tag[0] == first_batch.astype(jnp.float32) + 1.0
        head_fix = jnp.where(match, got_coef, head_fix)
    own_head = lax.dynamic_index_in_dim(coefficients, first_batch, 2, keepdims=False)
    head_final = jnp.where(head_owned, own_head, head_fix)
    coefficients = lax.dynamic_update_slice(
        coefficients, head_final[:, :, None], (jnp.int32(0), jnp.int32(0), first_batch)
    )

    def correct_step(batch_id, running):
        in_batch = (batch_of == batch_id).astype(jnp.float32)
        slope_table = lax.dynamic_index_in_dim(coefficients, batch_id, 2, keepdims=False)
        moved = jnp.einsum("kd,kn->dn", slope_table, assign * in_batch[None, :], precision=highest)
        return running + moved

    corrected = lax.fori_loop(first_batch, last_batch + 1, correct_step, jnp.zeros_like(latent_coordinates))
    return (latent_coordinates - corrected, new_centroids)


SLOTS = 8
ROWS = 64
MOST = 10485
LOGICAL = pl.DeviceIdType.LOGICAL
TILE = 256
CLOSE = 4
bf16, f32 = jnp.bfloat16, jnp.float32


def two_pieces(value):
    first = value.astype(bf16)
    return first, (value - first.astype(f32)).astype(bf16)


def across(left, right):
    return lax.dot_general(left, right, (((1,), (1,)), ((), ())), preferred_element_type=f32)


def plain(left, right):
    return jnp.dot(left, right, preferred_element_type=f32)


def step_kernel(
    shape,
    cells_all,
    z_hbm,
    means_hbm,
    soft_hbm,
    ridge_hbm,
    pop_hbm,
    zf,
    pair,
    slopes,
    starts_ref,
    flag_ref,
    cent_ref,
    means_ref,
    soft_ref,
    ridge_ref,
    pop_ref,
    zc,
    ex,
    lined,
    means_wide,
    pieces,
    near_out,
    near_counts,
    near_mass,
    near_moments,
    ends_out,
    full_moments,
    line_out,
    line_a,
    line_b,
    sums_out,
    sum_in,
    cent_out,
    cent_in,
    shrinks,
    cent_rows,
    cent_far,
    cent_full,
    tile_out,
    tile_in,
    full_sums,
    small_sems,
    load_sems,
    send_sems,
    recv_sems,
):
    nz, ny, nc, nx = shape
    near = nc * nx
    far = nz * ny
    count = near * far
    cells = zf.shape[1]
    pcs, clusters = means_ref.shape
    batches = pop_ref.shape[1]
    rows_each = ROWS // near
    width = 512
    reach = (MOST - 2) // cells + 1
    offsets = [h for h in range(-reach, reach + 1) if h]
    me = (
        (lax.axis_index("cells_0") * ny + lax.axis_index("cells_1")) * nc
        + lax.axis_index("cells_2")
    ) * nx + lax.axis_index("grp")
    rank = lax.rem(me, near)
    block = lax.div(me, near)

    def mate(r):
        return block * near + lax.rem(rank + r, near)

    plane = near * ny
    in_plane = lax.rem(me, plane)

    def beside(r):
        return me - in_plane + lax.rem(in_plane + r, plane)

    def peer(r):
        return lax.rem(block + r, far) * near + rank

    def along_z(r):
        return lax.rem(block + r * ny, far) * near + rank

    def neighbour(h):
        return lax.rem(me + (h + count), count)

    def push(src, dst, which, q):
        pltpu.make_async_remote_copy(
            src_ref=src,
            dst_ref=dst,
            send_sem=send_sems.at[which],
            recv_sem=recv_sems.at[which],
            device_id=q,
            device_id_type=LOGICAL,
        ).start()

    def arrived(buffer, which):
        pltpu.make_async_copy(buffer, buffer, recv_sems.at[which]).wait()

    def left(buffer, which):
        pltpu.make_async_copy(buffer, buffer, send_sems.at[which]).wait()

    small = [
        pltpu.make_async_copy(src, dst, small_sems.at[i])
        for i, (src, dst) in enumerate(
            (
                (pop_hbm, pop_ref),
                (means_hbm, means_ref),
                (soft_hbm, soft_ref),
                (ridge_hbm, ridge_ref),
            )
        )
    ]
    for copy in small:
        copy.start()
    for i in range(cells // width):
        columns = pl.ds(i * width, width)
        pltpu.make_async_copy(z_hbm.at[0, :, columns], zf.at[:, columns], load_sems.at[i]).start()

    barrier = pltpu.get_barrier_semaphore()
    greeted = [along_z(r) for r in range(1, nz)] + [beside(r) for r in range(1, plane)]
    greeted = greeted + [neighbour(h) for h in offsets]
    for q in greeted:
        pl.semaphore_signal(barrier, inc=1, device_id=q, device_id_type=LOGICAL)

    for copy in small:
        copy.wait()

    means_wide[...] = jnp.zeros_like(means_wide)
    means_wide[0:pcs, :] = means_ref[...]
    g = means_wide[...].T
    square = lax.broadcasted_iota(jnp.int32, (clusters, clusters), 0)
    lane = lax.broadcasted_iota(jnp.int32, (clusters, clusters), 1)
    soft = jnp.sum(jnp.where(square == lane, soft_ref[...], 0.0), axis=1, keepdims=True)
    offset_of = -0.5 * jnp.sum(g * g, axis=1, keepdims=True) / soft
    weights = jnp.where(lane == pcs, offset_of, g / soft)
    w1 = weights.astype(bf16).astype(f32)
    w2 = (weights - w1).astype(bf16).astype(f32)
    o1 = offset_of.astype(bf16).astype(f32)
    o2 = (offset_of - o1).astype(bf16).astype(f32)
    w1 = jnp.where(lane == pcs + 1, offset_of - o1 - o2, w1)
    w1 = (w1 + pltpu.roll(w1, ROWS, 1)).astype(bf16)
    w2 = (w2 + pltpu.roll(w2, ROWS, 1)).astype(bf16)
    weights = jnp.concatenate([w1, w2], axis=1)

    pop = pop_ref[...]
    up = lax.broadcasted_iota(jnp.int32, (batches, batches), 0)
    down = lax.broadcasted_iota(jnp.int32, (batches, batches), 1)
    column = jnp.sum(jnp.where(up == down, pop, 0), axis=1, keepdims=True)
    ends = jnp.sum(jnp.where(up <= down, column, 0), axis=0, keepdims=True)
    half = lax.broadcasted_iota(jnp.int32, (16, 1), 0)
    device = me + lax.rem(half, 8) - reach
    limit = device * cells + jnp.where(half >= 8, cells - 1, 0)
    spot = jnp.sum(jnp.where(ends <= limit, 1, 0), axis=1, keepdims=True)
    spot = jnp.where(device < 0, -9, spot)
    first = {h: spot[h + reach : h + reach + 1] for h in offsets + [0]}
    last = {h: spot[8 + h + reach : 9 + h + reach] for h in offsets + [0]}
    slot = lax.broadcasted_iota(jnp.int32, (SLOTS, 1), 0)
    batch_id = first[0] + slot
    batch_lane = lax.broadcasted_iota(jnp.int32, (SLOTS, batches), 1)
    chosen = batch_lane == batch_id
    held = jnp.sum(jnp.where(chosen, pop, 0), axis=1, keepdims=True)
    ridge = jnp.sum(jnp.where(chosen, ridge_ref[...], 0.0), axis=1, keepdims=True)
    ridge = jnp.where(batch_id < batches, ridge, 1.0)
    stop = jnp.sum(jnp.where(batch_lane <= batch_id, pop, 0), axis=1, keepdims=True) - me * cells
    start = stop - held
    held = held.astype(f32)
    starts_ref[...] = jnp.broadcast_to(jnp.where(batch_id < batches, start, 2 * cells), (SLOTS, 128))
    tail = slot == last[0] - first[0]
    head = slot == 0
    behind = {h: (last[h] == first[0]).astype(f32) for h in offsets if h < 0}
    ahead = {h: (first[h] == last[0]).astype(f32) for h in offsets if h > 0}

    wide = near - 1 + reach
    row32 = lax.broadcasted_iota(jnp.int32, (32, 1), 0)
    device = block * near + lax.rem(row32, 16) - reach
    limit = device * cells + jnp.where(row32 >= 16, cells - 1, 0)
    ids = jnp.sum(jnp.where(ends <= limit, 1, 0), axis=1, keepdims=True)
    ids = jnp.where(device < 0, -9, ids)
    limit = (block * near + lax.rem(half, 8)) * cells + jnp.where(half >= 8, cells - 1, 0)
    own_ids = jnp.sum(jnp.where(ends <= limit, 1, 0), axis=1, keepdims=True)
    own_lane = lax.broadcasted_iota(jnp.int32, (16, batches), 1)
    own_ridge = jnp.sum(jnp.where(own_lane == own_ids, ridge_ref[...], 0.0), axis=1, keepdims=True)

    crowded = jnp.zeros((1, 1), jnp.int32)
    for inner, room in ((SLOTS - 1, cells), (CLOSE - 1, width)):
        window = jnp.sum(
            jnp.where((up >= down) & (up < down + inner), column, 0), axis=0, keepdims=True
        )
        window = jnp.where((window < room - 1) & (batch_lane[0:1] <= batches - inner), 1, 0)
        crowded = crowded + jnp.sum(window, axis=1, keepdims=True)
    flag_ref[...] = jnp.broadcast_to(crowded, (1, 128))

    def inside(c, width, times):
        position = lax.broadcasted_iota(jnp.int32, (SLOTS * times, width), 1) + c * width
        low = jnp.concatenate([start] * times, axis=0)
        high = jnp.concatenate([stop] * times, axis=0)
        return ((position >= low) & (position < high)).astype(f32)

    def completed(own, buffer):
        before = jnp.zeros((1, clusters), f32)
        after = jnp.zeros((1, clusters), f32)
        for i, h in enumerate(offsets):
            if h < 0:
                before = before + behind[h] * buffer[i][1:2]
            else:
                after = after + ahead[h] * buffer[i][0:1]
        return own + jnp.where(head, before, 0.0) + jnp.where(tail, after, 0.0)

    def tail_of(value):
        return jnp.sum(jnp.where(tail, value, 0.0), axis=0, keepdims=True)

    def greeted_rows(which, value):
        near_out[which, 0:1, :] = value[0:1]
        near_out[which, 1:2, :] = tail_of(value)

    runs = cells // width

    def base_of(c):
        return jnp.sum(
            jnp.where((start <= c * width) & (slot > 0) & (batch_id < batches), 1, 0),
            axis=0,
            keepdims=True,
        )


    for i in range(runs):
        columns = pl.ds(i * width, width)
        pltpu.make_async_copy(z_hbm.at[0, :, columns], zf.at[:, columns], load_sems.at[i]).wait()
    z1, z2 = two_pieces(
        jnp.concatenate(
            [
                zf[...],
                jnp.ones((2, cells), f32),
                jnp.zeros((ROWS - 2 - pcs, cells), f32),
            ],
            axis=0,
        )
    )
    zc[0:ROWS, :] = z1
    zc[ROWS : 2 * ROWS, :] = z2
    score = plain(weights, jnp.concatenate([z1, z2, z1, z2], axis=0))
    raised = jnp.exp(score - jnp.max(score, axis=0, keepdims=True))
    ex[...] = raised
    p1, p2 = two_pieces(raised * (1.0 / jnp.sum(raised, axis=0, keepdims=True)))
    mask = inside(0, cells, 2).astype(bf16)
    total = across(mask, jnp.concatenate([p1, p2], axis=0))
    counts = total[0:SLOTS, 0:clusters] + total[0:SLOTS, clusters : 2 * clusters]
    own_total = jnp.sum(counts, axis=0, keepdims=True)
    greeted_rows(0, counts)
    line_out[0] = own_total
    pl.semaphore_wait(barrier, len(greeted))
    for r in range(1, plane):
        push(line_out.at[0], line_a.at[r - 1], 0, beside(r))
    for i, h in enumerate(offsets):
        push(near_out.at[0], near_counts.at[len(offsets) - 1 - i], 1, neighbour(h))

    def line_up(c):
        columns = slice(c * width, (c + 1) * width)
        mask = inside(c, width, 1)
        kind = jnp.sum(mask * slot.astype(f32), axis=0, keepdims=True)
        kind = kind - base_of(c).astype(f32)
        z = zc[:, columns]
        for j in range(CLOSE):
            lined[2 * ROWS * j : 2 * ROWS * (j + 1), columns] = z * (kind == j).astype(
                f32
            ).astype(bf16)

    for c in range(runs // 2):
        line_up(c)
    arrived(line_a, 0)
    plane_total = own_total + jnp.sum(line_a[...], axis=0)
    line_out[1] = plane_total
    for r in range(1, nz):
        push(line_out.at[1], line_b.at[r - 1], 2, along_z(r))
    for c in range(runs // 2, runs):
        line_up(c)
    arrived(near_counts, 1)
    full_counts = completed(counts, [near_counts[i] for i in range(len(offsets))])
    arrived(line_b, 2)
    totals = plane_total + jnp.sum(line_b[...], axis=0)
    expected = held * totals * (1.0 / cells_all)
    ratio = (expected + 1.0) / (full_counts + 1.0)
    factor = ratio * ratio
    f1 = factor.astype(bf16).astype(f32)
    f2 = (factor - f1).astype(bf16).astype(f32)
    f3 = factor - f1 - f2
    factor = jnp.concatenate([f1, f2, f3, jnp.zeros_like(f3)], axis=0).T.astype(bf16)

    mask = inside(0, cells, 4).astype(bf16)
    weighed = ex[...] * plain(factor, mask)
    a1, a2 = two_pieces(weighed * (1.0 / jnp.sum(weighed, axis=0, keepdims=True)))
    both = jnp.concatenate([a1, a2], axis=0)
    pair[...] = both
    total = across(mask[0 : 2 * SLOTS], both)
    mass = total[0:SLOTS, 0:clusters] + total[0:SLOTS, clusters : 2 * clusters]
    greeted_rows(1, mass)
    around = 2 * wide + 1
    for h in range(1, wide + 1):
        push(near_out.at[1], near_mass.at[(around - 1 - h) % around], 3, neighbour(h))
        push(near_out.at[1], near_mass.at[(around - 1 + h) % around], 3, neighbour(-h))
    near_mass[around - 1] = near_out[1]

    for c in range(runs):
        columns = slice(c * width, (c + 1) * width)
        value = across(lined[:, columns], pair[:, columns])
        for j in range(CLOSE):
            top = value[2 * ROWS * j : 2 * ROWS * j + ROWS]
            low = value[2 * ROWS * j + ROWS : 2 * ROWS * (j + 1)]
            pieces[c, j] = (
                top[:, 0:clusters] + top[:, clusters:] + low[:, 0:clusters] + low[:, clusters:]
            )
    places = [(c, j) for c in range(runs) for j in range(CLOSE)]
    tail_slot = last[0] - first[0]
    alone = jnp.where(tail_slot > 0, 1.0, 0.0)
    shrink = jnp.where(head | tail, 0.0, ridge / (mass + ridge))
    first_moment = jnp.zeros((ROWS, clusters), f32)
    tail_moment = jnp.zeros((ROWS, clusters), f32)
    whole = jnp.zeros((ROWS, clusters), f32)
    right = jnp.zeros((ROWS, clusters), f32)
    for c in range(runs):
        base = base_of(c)
        for j in range(CLOSE):
            piece = pieces[c, j]
            line = jnp.sum(jnp.where(slot == base + j, shrink, 0.0), axis=0, keepdims=True)
            right = right + line * piece
            tail_moment = tail_moment + jnp.where(base + j == tail_slot, 1.0, 0.0) * piece
            whole = whole + piece
            if j == 0:
                first_moment = first_moment + jnp.where(base == 0, 1.0, 0.0) * piece
    for t in range(near):
        inner = slice(t * rows_each, (t + 1) * rows_each)
        sums_out[t, 0] = right[inner]
        sums_out[t, 1] = first_moment[inner]
        sums_out[t, 2] = tail_moment[inner] * alone
        cent_out[t] = whole[inner]
    for r in range(1, near):
        push(sums_out.at[lax.rem(rank + r, near)], sum_in.at[r - 1], 5, mate(r))
    ends_out[0] = first_moment[0:56]
    ends_out[1] = tail_moment[0:56]
    arrived(near_mass.at[pl.ds(0, around - 1)], 3)
    full_mass = completed(
        mass, {i: near_mass[(around - 1 + h) % around] for i, h in enumerate(offsets)}
    )
    end_mass = jnp.zeros((16, clusters), f32)
    for p in range(-reach, near + reach):
        both = near_mass[lax.rem(p + (2 * around - 1) - rank, around)]
        one, two = ids[p + reach : p + reach + 1], ids[16 + p + reach : 17 + p + reach]
        end_mass = end_mass + jnp.where(own_ids == one, both[0:1], 0.0)
        end_mass = end_mass + jnp.where((own_ids == two) & (two != one), both[1:2], 0.0)
    end_shrink = own_ridge / (end_mass + own_ridge)
    for r in range(1, near):
        push(cent_out.at[lax.rem(rank + r, near)], cent_in.at[r - 1], 4, mate(r))
    for t in range(near):
        shrinks[t, 0:1, :] = end_shrink[t : t + 1]
        shrinks[t, 1:2, :] = end_shrink[8 + t : 9 + t]
    arrived(sum_in, 5)
    sum_tile = jnp.zeros((rows_each, clusters), f32)
    for r in range(near):
        by = shrinks[lax.rem(rank + near - r, near)]
        got = sums_out[rank] if r == 0 else sum_in[r - 1]
        sum_tile = sum_tile + got[0] + got[1] * by[0:1] + got[2] * by[1:2]
    tile_out[2] = sum_tile
    for r in range(1, far):
        push(tile_out.at[2], tile_in.at[r - 1], 8, peer(r))
    for i, h in enumerate(offsets):
        push(ends_out.at[int(h > 0)], near_moments.at[len(offsets) - 1 - i], 6, neighbour(h))
    arrived(cent_in, 4)
    cent_tile = cent_out[rank]
    for r in range(near - 1):
        cent_tile = cent_tile + cent_in[r]
    owned = clusters // far
    spread = jnp.concatenate(
        [jnp.broadcast_to(cent_tile[d : d + 1], (owned, clusters)) for d in range(rows_each)],
        axis=0,
    )
    row_at = lax.broadcasted_iota(jnp.int32, spread.shape, 0)
    lane_at = lax.broadcasted_iota(jnp.int32, spread.shape, 1)
    spread = jnp.where(lax.rem(lane_at, owned) == lax.rem(row_at, owned), spread, 0.0)
    spread = jnp.concatenate(
        [spread, jnp.zeros((clusters - spread.shape[0], clusters), f32)], axis=0
    )
    taken = lax.div(lax.broadcasted_iota(jnp.int32, (far, clusters), 1), owned)
    taken = taken == lax.broadcasted_iota(jnp.int32, (far, clusters), 0)
    by_block = lax.dot_general(
        taken.astype(f32),
        spread,
        (((1,), (1,)), ((), ())),
        precision=highest,
        preferred_element_type=f32,
    )
    for t in range(far):
        cent_rows[t] = by_block[t : t + 1]
    for r in range(1, far):
        push(cent_rows.at[lax.rem(block + r, far)], cent_far.at[r - 1], 7, peer(r))
    moments = []
    for s in range(SLOTS):
        moment = jnp.zeros((ROWS, clusters), f32)
        for c, j in places:
            if j <= s <= CLOSE * c + j:
                moment = moment + jnp.where(base_of(c) + j == s, 1.0, 0.0) * pieces[c, j]
        moments.append(moment)

    arrived(tile_in, 8)
    full_sums[1, 0] = sum_tile + jnp.sum(tile_in[...], axis=0)
    for r in range(1, near):
        push(full_sums.at[1, 0], full_sums.at[1, r], 10, mate(r))
    arrived(cent_far, 7)
    cent_full[0] = cent_rows[block] + jnp.sum(cent_far[...], axis=0)
    for r in range(1, near):
        push(cent_full.at[0], cent_full.at[r], 9, mate(r))
    arrived(near_moments, 6)
    before = jnp.zeros((56, clusters), f32)
    after = jnp.zeros((56, clusters), f32)
    for i, h in enumerate(offsets):
        if h < 0:
            before = before + behind[h] * near_moments[i]
        else:
            after = after + ahead[h] * near_moments[i]
    for s in range(SLOTS):
        moment = moments[s][0:56] + after * tail[s : s + 1].astype(f32)
        full_moments[s] = moment + before if s == 0 else moment


    def gathered(which):
        return jnp.concatenate(
            [full_sums[which, lax.rem(rank + (near - t), near)] for t in range(near)], axis=0
        )

    arrived(full_sums.at[1, pl.ds(1, near - 1)], 10)
    right = gathered(1)
    intercept = (right / (1.0 + right[pcs : pcs + 1]))[0:56]
    for s in range(SLOTS):
        moment = full_moments[s]
        line = full_mass[s : s + 1]
        slope = (moment - line * intercept) / (line + ridge[s : s + 1])
        c1, c2 = two_pieces(jnp.concatenate([slope, jnp.zeros((8, clusters), f32)], axis=0))
        slopes[ROWS * s : ROWS * (s + 1), :] = jnp.concatenate([c1, c1, c2], axis=1)

    arrived(cent_full.at[pl.ds(1, near - 1)], 9)
    rows = jnp.concatenate(
        [cent_full[lax.rem(rank + (near - t), near)] for t in range(near)], axis=0
    )
    from_lane = lax.broadcasted_iota(jnp.int32, (clusters, ROWS), 0)
    to_lane = lax.broadcasted_iota(jnp.int32, (clusters, ROWS), 1)
    tile_at = lax.broadcasted_iota(jnp.int32, (near, ROWS), 0)
    mine = tile_at == lax.div(lax.broadcasted_iota(jnp.int32, (near, ROWS), 1), rows_each)
    core = lax.div(rank, nx)
    each = cent_ref.shape[0]
    for j in range(each):
        picked = from_lane == lax.rem(to_lane, rows_each) * owned + core * each + j
        line = jnp.dot(
            rows, picked.astype(f32), precision=highest, preferred_element_type=f32
        )
        line = jnp.sum(jnp.where(mine, line, 0.0), axis=0, keepdims=True)
        cent_ref[j : j + 1, :] = (line / (1.0 + line[:, pcs : pcs + 1]))[:, 0:pcs]

    left(line_a, 0)
    left(near_counts, 1)
    left(line_b, 2)
    left(near_mass.at[pl.ds(0, around - 1)], 3)
    left(cent_in, 4)
    left(sum_in, 5)
    left(near_moments, 6)
    left(cent_far, 7)
    left(tile_in, 8)
    left(cent_full.at[pl.ds(1, near - 1)], 9)
    left(full_sums.at[1, pl.ds(1, near - 1)], 10)


def correct_kernel(
    zf, pair, slopes, starts_ref, cent_ref, out_hbm, cent_hbm, held, starts, out_sems
):
    pcs, cells = zf.shape
    clusters = pair.shape[0] // 2
    loads = out_sems.shape[0] - 1
    part = cells // loads
    cent = pltpu.make_async_copy(cent_ref, cent_hbm, out_sems.at[loads])
    cent.start()
    begin = [jnp.max(starts_ref[s : s + 1, :]) for s in range(SLOTS)]
    for s in range(SLOTS):
        starts[s] = begin[s]
    lane = lax.broadcasted_iota(jnp.int32, (1, TILE), 1)

    def slope_of(j):
        return slopes[pl.ds(pl.multiple_of(j * ROWS, ROWS), ROWS), :]

    def slots_of(t):
        base = jnp.int32(0)
        final = jnp.int32(0)
        border = jnp.int32(2 * cells)
        for s in range(1, SLOTS):
            base = base + jnp.where(begin[s] <= t * TILE, 1, 0)
            final = final + jnp.where(begin[s] < (t + 1) * TILE, 1, 0)
            border = jnp.where(begin[s] > t * TILE, jnp.minimum(border, begin[s]), border)
        return base, final, border

    def send_out(i):
        columns = pl.ds(i * part, part)
        return pltpu.make_async_copy(
            held.at[:, columns], out_hbm.at[:, columns], out_sems.at[i]
        )

    beyond = jnp.int32(0)
    for i in range(loads):
        for t in range(i * part // TILE, (i + 1) * part // TILE):
            columns = slice(t * TILE, (t + 1) * TILE)
            base, final, border = slots_of(t)
            beyond = jnp.maximum(beyond, final - base)
            following = jnp.minimum(base + 1, SLOTS - 1)
            both = pair[:, columns]
            both = jnp.concatenate([both, both[0:clusters]], axis=0)
            moved = plain(jnp.concatenate([slope_of(base), slope_of(following)], axis=0), both)
            moved = jnp.where(lane < border - t * TILE, moved[0:ROWS], moved[ROWS:])
            held[:, columns] = zf[:, columns] - moved[0:pcs]
        send_out(i).start()
    for i in range(loads):
        send_out(i).wait()
    cent.wait()

    @pl.when(beyond > 1)
    def _():
        def tile_of(t, carry):
            columns = pl.ds(pl.multiple_of(t * TILE, TILE), TILE)
            base, final, border = slots_of(t)

            def more(j, carry):
                both = pair[:, columns]
                both = jnp.concatenate([both, both[0:clusters]], axis=0)
                other = zf[:, columns] - plain(slope_of(j), both)[0:pcs]
                held[:, columns] = jnp.where(
                    lane >= starts[j] - t * TILE, other, held[:, columns]
                )
                return carry

            lax.fori_loop(base + 2, final + 1, more, 0)
            return carry

        lax.fori_loop(0, cells // TILE, tile_of, 0)
        for i in range(loads):
            send_out(i).start()
        for i in range(loads):
            send_out(i).wait()


def narrow_body(
    shape, latent_coordinates, group_means, entropy_scaling, sample_shrinkage_lambda, sample_population
):
    pcs, cells = latent_coordinates.shape
    clusters = group_means.shape[0]
    batches = sample_population.shape[0]
    nz, ny, nc, nx = shape
    near, far = nc * nx, nz * ny
    rows_each = ROWS // near
    reach = (MOST - 2) // cells + 1
    owned = clusters // (nz * ny * nc)
    vmem = pl.BlockSpec(memory_space=pltpu.VMEM)
    tile = (rows_each, clusters)
    scratch = [
        pltpu.VMEM((pcs, clusters), f32),
        pltpu.VMEM((1, clusters), f32),
        pltpu.VMEM((1, batches), f32),
        pltpu.VMEM((1, batches), jnp.int32),
        pltpu.VMEM((2 * ROWS, cells), bf16),
        pltpu.VMEM((clusters, cells), f32),
        pltpu.VMEM((2 * ROWS * CLOSE, cells), bf16),
        pltpu.VMEM((clusters, clusters), f32),
        pltpu.VMEM((cells // 512, CLOSE, ROWS, clusters), f32),
        pltpu.VMEM((2, 2, clusters), f32),
        pltpu.VMEM((2 * reach, 2, clusters), f32),
        pltpu.VMEM((2 * (near - 1 + reach) + 1, 2, clusters), f32),
        pltpu.VMEM((2 * reach, 56, clusters), f32),
        pltpu.VMEM((2, 56, clusters), f32),
        pltpu.VMEM((SLOTS, 56, clusters), f32),
        pltpu.VMEM((2, 1, clusters), f32),
        pltpu.VMEM((near * ny - 1, 1, clusters), f32),
        pltpu.VMEM((nz - 1, 1, clusters), f32),
        pltpu.VMEM((near, 3, *tile), f32),
        pltpu.VMEM((near - 1, 3, *tile), f32),
        pltpu.VMEM((near, *tile), f32),
        pltpu.VMEM((near - 1, *tile), f32),
        pltpu.VMEM((near, 2, clusters), f32),
        pltpu.VMEM((far, 1, clusters), f32),
        pltpu.VMEM((far - 1, 1, clusters), f32),
        pltpu.VMEM((near, 1, clusters), f32),
        pltpu.VMEM((3, *tile), f32),
        pltpu.VMEM((far - 1, *tile), f32),
        pltpu.VMEM((2, near, *tile), f32),
        pltpu.SemaphoreType.DMA((4,)),
        pltpu.SemaphoreType.DMA((cells // 512,)),
        pltpu.SemaphoreType.DMA((12,)),
        pltpu.SemaphoreType.DMA((12,)),
    ]
    return pl.pallas_call(
        functools.partial(step_kernel, shape, float(cells * near * far)),
        out_shape=(
            pltpu.VMEM((pcs, cells), f32),
            pltpu.VMEM((2 * clusters, cells), bf16),
            pltpu.VMEM((SLOTS * ROWS, 3 * clusters), bf16),
            pltpu.VMEM((SLOTS, 128), jnp.int32),
            pltpu.VMEM((1, 128), jnp.int32),
            pltpu.VMEM((owned, pcs), f32),
        ),
        in_specs=[pl.BlockSpec(memory_space=pl.ANY)] * 5,
        out_specs=(vmem,) * 6,
        scratch_shapes=scratch,
        compiler_params=pltpu.CompilerParams(
            collective_id=0, has_side_effects=True, vmem_limit_bytes=44 * 1024 * 1024
        ),
    )(
        latent_coordinates[None],
        group_means.T,
        entropy_scaling.reshape(1, clusters),
        sample_shrinkage_lambda.reshape(1, batches),
        sample_population.reshape(1, batches),
    )


def corrected_by(kept, pair, slopes, starts, new_centroids):
    pcs, cells = kept.shape
    vmem = pl.BlockSpec(memory_space=pltpu.VMEM)
    anywhere = pl.BlockSpec(memory_space=pl.ANY)
    return pl.pallas_call(
        correct_kernel,
        out_shape=(pltpu.HBM((pcs, cells), f32), pltpu.HBM(new_centroids.shape, f32)),
        in_specs=[vmem] * 5,
        out_specs=(anywhere, anywhere),
        scratch_shapes=[
            pltpu.VMEM((pcs, cells), f32),
            pltpu.SMEM((SLOTS,), jnp.int32),
            pltpu.SemaphoreType.DMA((5,)),
        ],
        compiler_params=pltpu.CompilerParams(vmem_limit_bytes=16 * 1024 * 1024),
    )(
        kept,
        pair,
        slopes,
        starts,
        new_centroids,
    )


def body(
    shape, latent_coordinates, group_means, entropy_scaling, sample_shrinkage_lambda, sample_population
):
    arguments = (
        latent_coordinates,
        group_means,
        entropy_scaling,
        sample_shrinkage_lambda,
        sample_population,
    )
    kept, pair, slopes, starts, flag, new_centroids = narrow_body(shape, *arguments)
    return lax.cond(
        flag[0, 0] == 0,
        lambda: corrected_by(kept, pair, slopes, starts, new_centroids),
        lambda: wide_body(*arguments),
    )


def solution(mesh):
    shape = (mesh.shape["cells"] // 8, 4, 2, mesh.shape["grp"])
    finer = Mesh(mesh.devices.reshape(shape), ("cells_0", "cells_1", "cells_2", "grp"))
    return jax.shard_map(
        functools.partial(body, shape),
        mesh=finer,
        in_specs=(P(None, CELLS_GRP), P(), P(), P(), P()),
        out_specs=(P(None, CELLS_GRP), P(CELLS, None)),
        check_vma=False,
    )
```

```python
import functools

import jax
import jax.numpy as jnp
from jax import lax
from jax.experimental import pallas as pl
from jax.experimental.pallas import tpu as pltpu
from jax.sharding import Mesh
from jax.sharding import PartitionSpec as P

CELLS = ("cells_0", "cells_1", "cells_2")
CELLS_GRP = ("cells_0", "cells_1", "cells_2", "grp")


diversity = 2.0
intercept_ridge = 1.0
highest = lax.Precision.HIGHEST


def split_up(array, dim, size):
    dims = array.shape
    parts = array.reshape(*dims[:dim], size, dims[dim] // size, *dims[dim + 1 :])
    return jnp.moveaxis(parts, dim, 0)


def summed_on_arrival(array, axis, dim):
    size = lax.axis_size(axis)
    parts = lax.all_to_all(split_up(array, dim, size), axis, 0, 0, tiled=True)
    return jnp.sum(parts, axis=0)


def sum_in_two_steps(array, axes, dim):
    far, near = axes
    parts = split_up(array, dim, lax.axis_size(far))
    nearer = summed_on_arrival(parts, near, dim + 1)
    arrived = lax.all_to_all(nearer, far, split_axis=0, concat_axis=0, tiled=True)
    return arrived.sum(axis=0)


def filled_up(lines, size):
    spare = -len(lines) % size
    return jnp.pad(lines, [(0, spare)] + [(0, 0)] * (lines.ndim - 1))


def sent_to_all(array, axis):
    size = lax.axis_size(axis)
    return lax.all_to_all(
        jnp.broadcast_to(array[None], (size, *array.shape)), axis, 0, 0, tiled=True
    )


def joined_along(parts, dim):
    parts = jnp.moveaxis(parts, 0, dim)
    dims = parts.shape
    return parts.reshape(*dims[:dim], dims[dim] * dims[dim + 1], *dims[dim + 2 :])


def gather_axes(array, axes, dim):
    far, near = axes
    leading = sent_to_all(array, far)
    parts = jnp.swapaxes(sent_to_all(leading, near), 0, 1)
    return joined_along(parts.reshape(-1, *array.shape), dim)


def total_of(array, axes):
    lines = array.reshape(-1)
    own = sum_in_two_steps(
        filled_up(lines, lax.axis_size(axes[0]) * lax.axis_size(axes[1])), axes, 0
    )
    whole = gather_axes(own, axes, 0)
    return whole[: len(lines)].reshape(array.shape)


def from_behind(block, axis, distance):
    devices = range(lax.axis_size(axis))
    route = [(i - distance, i) for i in devices if i - distance in devices]
    return lax.ppermute(block, axis, route)


def by_axis(array, axes):
    return functools.reduce(lax.psum, axes, array)


def observation_affinity(latent_coordinates, group_means, entropy_scaling):
    pairwise_dots = jnp.dot(
        group_means, latent_coordinates, precision=highest, preferred_element_type=jnp.float32
    )
    quadratic_lengths = jnp.sum(group_means * group_means, axis=1)
    return (2.0 * pairwise_dots - quadratic_lengths[:, None]) / (2.0 * entropy_scaling[:, None])


def probabilistic_responsibility(group_affinity):
    top = jnp.max(group_affinity, axis=0, keepdims=True)
    raised = jnp.exp(group_affinity - top)
    return raised / jnp.sum(raised, axis=0, keepdims=True)


def batch_parts(moments, ridge):
    mass = moments[:, 0, :]
    sums = moments[:, 1:, :]
    shrink = ridge[None, :] / (mass + ridge[None, :])
    weight = jnp.sum(mass * shrink, axis=1)
    right_side = jnp.sum(sums * shrink[:, None, :], axis=2)
    return (weight, right_side, jnp.sum(mass, axis=1), jnp.sum(sums, axis=2))


def slopes_of(moments, ridge, weight, right_side):
    mass = moments[:, 0, :]
    sums = moments[:, 1:, :]
    intercept = right_side / (intercept_ridge + weight)[:, None]
    return (sums - mass[:, None, :] * intercept[:, :, None]) / (mass + ridge[None, :])[:, None, :]


def wide_body(
    latent_coordinates, group_means, entropy_scaling, sample_shrinkage_lambda, sample_population
):
    local_cells = latent_coordinates.shape[1]
    num_pcs = latent_coordinates.shape[0]
    clusters = group_means.shape[0]
    batches = sample_population.shape[0]
    owned = clusters // lax.axis_size(CELLS)
    offset = (lax.axis_index(CELLS) * lax.axis_size("grp") + lax.axis_index("grp")) * local_cells
    batch_ends = jnp.cumsum(sample_population)
    batch_starts = batch_ends - sample_population
    cells_total = jnp.sum(sample_population).astype(jnp.float32)
    position = offset + lax.iota(jnp.int32, local_cells)
    batch_of = jnp.sum((batch_ends[:, None] <= position[None, :]).astype(jnp.int32), axis=0)
    first_batch = batch_of[0]
    last_batch = batch_of[local_cells - 1]
    group_affinity = observation_affinity(latent_coordinates, group_means, entropy_scaling)
    expected_occupancy = probabilistic_responsibility(group_affinity)

    def count_step(batch_id, running):
        in_batch = (batch_of == batch_id).astype(jnp.float32)
        single_observation = jnp.dot(
            expected_occupancy, in_batch, precision=highest, preferred_element_type=jnp.float32
        )
        return lax.dynamic_update_slice(
            running, single_observation[:, None], (jnp.int32(0), batch_id)
        )

    counts = lax.fori_loop(
        first_batch, last_batch + 1, count_step, jnp.zeros((clusters, batches), jnp.float32)
    )
    counts = total_of(counts, (("cells_0", "cells_1"), ("cells_2", "grp")))
    totals = jnp.sum(counts, axis=1)
    expected = sample_population.astype(jnp.float32)[None, :] * totals[:, None] / cells_total
    penalty = diversity * jnp.log((counts + 1.0) / (expected + 1.0))

    def penalty_step(batch_id, running):
        in_batch = (batch_of == batch_id).astype(jnp.float32)
        column = lax.dynamic_index_in_dim(penalty, batch_id, 1, keepdims=True)
        return running + column * in_batch[None, :]

    cell_penalty = lax.fori_loop(
        first_batch, last_batch + 1, penalty_step, jnp.zeros((clusters, local_cells), jnp.float32)
    )
    assign = probabilistic_responsibility(group_affinity - cell_penalty)
    augmented = jnp.concatenate(
        [jnp.ones((1, local_cells), jnp.float32), latent_coordinates], axis=0
    )

    def moment_step(batch_id, running):
        in_batch = (batch_of == batch_id).astype(jnp.float32)
        contiguous_portion = jnp.einsum(
            "kn,dn->kd", assign * in_batch[None, :], augmented, precision=highest
        )
        return lax.dynamic_update_slice(
            running, contiguous_portion[:, :, None], (jnp.int32(0), jnp.int32(0), batch_id)
        )

    moments = lax.fori_loop(
        first_batch,
        last_batch + 1,
        moment_step,
        jnp.zeros((clusters, num_pcs + 1, batches), jnp.float32),
    )
    devices_flat = lax.axis_size(CELLS) * lax.axis_size("grp")
    most_cells = 2 * local_cells * devices_flat // batches
    reach = (most_cells - 2) // local_cells + 1
    begins_here = (batch_starts >= offset) & (batch_starts < offset + local_cells)
    owner_mask = begins_here.astype(jnp.float32)
    head_owned = begins_here[first_batch]
    head_column = lax.dynamic_index_in_dim(moments, first_batch, 2, keepdims=False)
    sent_stats = jnp.where(head_owned, 0.0, 1.0) * head_column
    sent_tag = jnp.where(head_owned, 0.0, first_batch.astype(jnp.float32) + 1.0) * jnp.ones(
        (1,), jnp.float32
    )
    completed = moments
    for hop in range(1, reach + 1):
        got_stats, got_tag = from_behind((sent_stats, sent_tag), CELLS_GRP, -hop)
        got_id = jnp.maximum(got_tag[0].astype(jnp.int32) - 1, 0)
        accept = jnp.where((got_tag[0] > 0.5) & begins_here[got_id], 1.0, 0.0)
        single_observation = (
            lax.dynamic_index_in_dim(completed, got_id, 2, keepdims=False) + accept * got_stats
        )
        completed = lax.dynamic_update_slice(
            completed, single_observation[:, :, None], (jnp.int32(0), jnp.int32(0), got_id)
        )
    completed = completed * owner_mask[None, None, :]
    weight, right_side, mass_total, moment_total = jax.tree.map(
        lambda part: by_axis(part, CELLS_GRP), batch_parts(completed, sample_shrinkage_lambda)
    )
    coefficients = slopes_of(completed, sample_shrinkage_lambda, weight, right_side)
    every_centroid = moment_total / (1.0 + mass_total)[:, None]
    new_centroids = lax.dynamic_slice_in_dim(
        every_centroid, lax.axis_index(CELLS) * owned, owned, 0
    )
    tail_owned = begins_here[last_batch]
    tail_column = lax.dynamic_index_in_dim(coefficients, last_batch, 2, keepdims=False)
    tail_send = jnp.where(tail_owned, 1.0, 0.0) * tail_column
    tail_tag = jnp.where(tail_owned, last_batch.astype(jnp.float32) + 1.0, 0.0) * jnp.ones(
        (1,), jnp.float32
    )
    head_fix = jnp.zeros_like(tail_column)
    for hop in range(1, reach + 1):
        got_coef, got_tag = from_behind((tail_send, tail_tag), CELLS_GRP, hop)
        match = got_tag[0] == first_batch.astype(jnp.float32) + 1.0
        head_fix = jnp.where(match, got_coef, head_fix)
    own_head = lax.dynamic_index_in_dim(coefficients, first_batch, 2, keepdims=False)
    head_final = jnp.where(head_owned, own_head, head_fix)
    coefficients = lax.dynamic_update_slice(
        coefficients, head_final[:, :, None], (jnp.int32(0), jnp.int32(0), first_batch)
    )

    def correct_step(batch_id, running):
        in_batch = (batch_of == batch_id).astype(jnp.float32)
        slope_table = lax.dynamic_index_in_dim(coefficients, batch_id, 2, keepdims=False)
        moved = jnp.einsum("kd,kn->dn", slope_table, assign * in_batch[None, :], precision=highest)
        return running + moved

    corrected = lax.fori_loop(first_batch, last_batch + 1, correct_step, jnp.zeros_like(latent_coordinates))
    return (latent_coordinates - corrected, new_centroids)


SLOTS = 8
ROWS = 64
MOST = 10485
LOGICAL = pl.DeviceIdType.LOGICAL
TILE = 256
CLOSE = 4
bf16, f32 = jnp.bfloat16, jnp.float32


def two_pieces(value):
    first = value.astype(bf16)
    return first, (value - first.astype(f32)).astype(bf16)


def across(left, right):
    return lax.dot_general(left, right, (((1,), (1,)), ((), ())), preferred_element_type=f32)


def plain(left, right):
    return jnp.dot(left, right, preferred_element_type=f32)


def step_kernel(
    shape,
    cells_all,
    z_hbm,
    means_hbm,
    soft_hbm,
    ridge_hbm,
    pop_hbm,
    zf,
    pair,
    slopes,
    starts_ref,
    flag_ref,
    cent_ref,
    means_ref,
    soft_ref,
    ridge_ref,
    pop_ref,
    zc,
    ex,
    lined,
    means_wide,
    pieces,
    near_out,
    near_counts,
    near_mass,
    near_moments,
    ends_out,
    full_moments,
    line_out,
    line_a,
    line_b,
    sums_out,
    sum_in,
    cent_out,
    cent_in,
    shrinks,
    cent_rows,
    cent_far,
    cent_full,
    tile_out,
    tile_in,
    full_sums,
    small_sems,
    load_sems,
    send_sems,
    recv_sems,
):
    nz, ny, nc, nx = shape
    near = nc * nx
    far = nz * ny
    count = near * far
    cells = zf.shape[1]
    pcs, clusters = means_ref.shape
    batches = pop_ref.shape[1]
    rows_each = ROWS // near
    width = 512
    reach = (MOST - 2) // cells + 1
    offsets = [h for h in range(-reach, reach + 1) if h]
    me = (
        (lax.axis_index("cells_0") * ny + lax.axis_index("cells_1")) * nc
        + lax.axis_index("cells_2")
    ) * nx + lax.axis_index("grp")
    rank = lax.rem(me, near)
    block = lax.div(me, near)

    def mate(r):
        return block * near + lax.rem(rank + r, near)

    plane = near * ny
    in_plane = lax.rem(me, plane)

    def beside(r):
        return me - in_plane + lax.rem(in_plane + r, plane)

    def peer(r):
        return lax.rem(block + r, far) * near + rank

    def along_z(r):
        return lax.rem(block + r * ny, far) * near + rank

    def neighbour(h):
        return lax.rem(me + (h + count), count)

    def push(src, dst, which, q):
        pltpu.make_async_remote_copy(
            src_ref=src,
            dst_ref=dst,
            send_sem=send_sems.at[which],
            recv_sem=recv_sems.at[which],
            device_id=q,
            device_id_type=LOGICAL,
        ).start()

    def arrived(buffer, which):
        pltpu.make_async_copy(buffer, buffer, recv_sems.at[which]).wait()

    def left(buffer, which):
        pltpu.make_async_copy(buffer, buffer, send_sems.at[which]).wait()

    small = [
        pltpu.make_async_copy(src, dst, small_sems.at[i])
        for i, (src, dst) in enumerate(
            (
                (pop_hbm, pop_ref),
                (means_hbm, means_ref),
                (soft_hbm, soft_ref),
                (ridge_hbm, ridge_ref),
            )
        )
    ]
    for copy in small:
        copy.start()
    for i in range(cells // width):
        columns = pl.ds(i * width, width)
        pltpu.make_async_copy(z_hbm.at[0, :, columns], zf.at[:, columns], load_sems.at[i]).start()

    barrier = pltpu.get_barrier_semaphore()
    greeted = [along_z(r) for r in range(1, nz)] + [beside(r) for r in range(1, plane)]
    greeted = greeted + [neighbour(h) for h in offsets]
    for q in greeted:
        pl.semaphore_signal(barrier, inc=1, device_id=q, device_id_type=LOGICAL)

    for copy in small:
        copy.wait()

    means_wide[...] = jnp.zeros_like(means_wide)
    means_wide[0:pcs, :] = means_ref[...]
    g = means_wide[...].T
    square = lax.broadcasted_iota(jnp.int32, (clusters, clusters), 0)
    lane = lax.broadcasted_iota(jnp.int32, (clusters, clusters), 1)
    soft = jnp.sum(jnp.where(square == lane, soft_ref[...], 0.0), axis=1, keepdims=True)
    offset_of = -0.5 * jnp.sum(g * g, axis=1, keepdims=True) / soft
    weights = jnp.where(lane == pcs, offset_of, g / soft)
    w1 = weights.astype(bf16).astype(f32)
    w2 = (weights - w1).astype(bf16).astype(f32)
    o1 = offset_of.astype(bf16).astype(f32)
    o2 = (offset_of - o1).astype(bf16).astype(f32)
    w1 = jnp.where(lane == pcs + 1, offset_of - o1 - o2, w1)
    w1 = (w1 + pltpu.roll(w1, ROWS, 1)).astype(bf16)
    w2 = (w2 + pltpu.roll(w2, ROWS, 1)).astype(bf16)
    weights = jnp.concatenate([w1, w2], axis=1)

    pop = pop_ref[...]
    up = lax.broadcasted_iota(jnp.int32, (batches, batches), 0)
    down = lax.broadcasted_iota(jnp.int32, (batches, batches), 1)
    column = jnp.sum(jnp.where(up == down, pop, 0), axis=1, keepdims=True)
    ends = jnp.sum(jnp.where(up <= down, column, 0), axis=0, keepdims=True)
    half = lax.broadcasted_iota(jnp.int32, (16, 1), 0)
    device = me + lax.rem(half, 8) - reach
    limit = device * cells + jnp.where(half >= 8, cells - 1, 0)
    spot = jnp.sum(jnp.where(ends <= limit, 1, 0), axis=1, keepdims=True)
    spot = jnp.where(device < 0, -9, spot)
    first = {h: spot[h + reach : h + reach + 1] for h in offsets + [0]}
    last = {h: spot[8 + h + reach : 9 + h + reach] for h in offsets + [0]}
    slot = lax.broadcasted_iota(jnp.int32, (SLOTS, 1), 0)
    batch_id = first[0] + slot
    batch_lane = lax.broadcasted_iota(jnp.int32, (SLOTS, batches), 1)
    chosen = batch_lane == batch_id
    held = jnp.sum(jnp.where(chosen, pop, 0), axis=1, keepdims=True)
    ridge = jnp.sum(jnp.where(chosen, ridge_ref[...], 0.0), axis=1, keepdims=True)
    ridge = jnp.where(batch_id < batches, ridge, 1.0)
    stop = jnp.sum(jnp.where(batch_lane <= batch_id, pop, 0), axis=1, keepdims=True) - me * cells
    start = stop - held
    held = held.astype(f32)
    starts_ref[...] = jnp.broadcast_to(jnp.where(batch_id < batches, start, 2 * cells), (SLOTS, 128))
    tail = slot == last[0] - first[0]
    head = slot == 0
    behind = {h: (last[h] == first[0]).astype(f32) for h in offsets if h < 0}
    ahead = {h: (first[h] == last[0]).astype(f32) for h in offsets if h > 0}

    wide = near - 1 + reach
    row32 = lax.broadcasted_iota(jnp.int32, (32, 1), 0)
    device = block * near + lax.rem(row32, 16) - reach
    limit = device * cells + jnp.where(row32 >= 16, cells - 1, 0)
    ids = jnp.sum(jnp.where(ends <= limit, 1, 0), axis=1, keepdims=True)
    ids = jnp.where(device < 0, -9, ids)
    limit = (block * near + lax.rem(half, 8)) * cells + jnp.where(half >= 8, cells - 1, 0)
    own_ids = jnp.sum(jnp.where(ends <= limit, 1, 0), axis=1, keepdims=True)
    own_lane = lax.broadcasted_iota(jnp.int32, (16, batches), 1)
    own_ridge = jnp.sum(jnp.where(own_lane == own_ids, ridge_ref[...], 0.0), axis=1, keepdims=True)

    crowded = jnp.zeros((1, 1), jnp.int32)
    for inner, room in ((SLOTS - 1, cells), (CLOSE - 1, width)):
        window = jnp.sum(
            jnp.where((up >= down) & (up < down + inner), column, 0), axis=0, keepdims=True
        )
        window = jnp.where((window < room - 1) & (batch_lane[0:1] <= batches - inner), 1, 0)
        crowded = crowded + jnp.sum(window, axis=1, keepdims=True)
    flag_ref[...] = jnp.broadcast_to(crowded, (1, 128))

    def inside(c, width, times):
        position = lax.broadcasted_iota(jnp.int32, (SLOTS * times, width), 1) + c * width
        low = jnp.concatenate([start] * times, axis=0)
        high = jnp.concatenate([stop] * times, axis=0)
        return ((position >= low) & (position < high)).astype(f32)

    def completed(own, buffer):
        before = jnp.zeros((1, clusters), f32)
        after = jnp.zeros((1, clusters), f32)
        for i, h in enumerate(offsets):
            if h < 0:
                before = before + behind[h] * buffer[i][1:2]
            else:
                after = after + ahead[h] * buffer[i][0:1]
        return own + jnp.where(head, before, 0.0) + jnp.where(tail, after, 0.0)

    def tail_of(value):
        return jnp.sum(jnp.where(tail, value, 0.0), axis=0, keepdims=True)

    def greeted_rows(which, value):
        near_out[which, 0:1, :] = value[0:1]
        near_out[which, 1:2, :] = tail_of(value)

    runs = cells // width

    def base_of(c):
        return jnp.sum(
            jnp.where((start <= c * width) & (slot > 0) & (batch_id < batches), 1, 0),
            axis=0,
            keepdims=True,
        )


    for i in range(runs):
        columns = pl.ds(i * width, width)
        pltpu.make_async_copy(z_hbm.at[0, :, columns], zf.at[:, columns], load_sems.at[i]).wait()
    z1, z2 = two_pieces(
        jnp.concatenate(
            [
                zf[...],
                jnp.ones((2, cells), f32),
                jnp.zeros((ROWS - 2 - pcs, cells), f32),
            ],
            axis=0,
        )
    )
    zc[0:ROWS, :] = z1
    zc[ROWS : 2 * ROWS, :] = z2
    score = plain(weights, jnp.concatenate([z1, z2, z1, z2], axis=0))
    raised = jnp.exp(score - jnp.max(score, axis=0, keepdims=True))
    ex[...] = raised
    p1, p2 = two_pieces(raised * (1.0 / jnp.sum(raised, axis=0, keepdims=True)))
    mask = inside(0, cells, 2).astype(bf16)
    total = across(mask, jnp.concatenate([p1, p2], axis=0))
    counts = total[0:SLOTS, 0:clusters] + total[0:SLOTS, clusters : 2 * clusters]
    own_total = jnp.sum(counts, axis=0, keepdims=True)
    greeted_rows(0, counts)
    line_out[0] = own_total
    pl.semaphore_wait(barrier, len(greeted))
    for r in range(1, plane):
        push(line_out.at[0], line_a.at[r - 1], 0, beside(r))
    for i, h in enumerate(offsets):
        push(near_out.at[0], near_counts.at[len(offsets) - 1 - i], 1, neighbour(h))

    def line_up(c):
        columns = slice(c * width, (c + 1) * width)
        mask = inside(c, width, 1)
        kind = jnp.sum(mask * slot.astype(f32), axis=0, keepdims=True)
        kind = kind - base_of(c).astype(f32)
        z = zc[:, columns]
        for j in range(CLOSE):
            lined[2 * ROWS * j : 2 * ROWS * (j + 1), columns] = z * (kind == j).astype(
                f32
            ).astype(bf16)

    for c in range(runs // 2):
        line_up(c)
    arrived(line_a, 0)
    plane_total = own_total + jnp.sum(line_a[...], axis=0)
    line_out[1] = plane_total
    for r in range(1, nz):
        push(line_out.at[1], line_b.at[r - 1], 2, along_z(r))
    for c in range(runs // 2, runs):
        line_up(c)
    arrived(near_counts, 1)
    full_counts = completed(counts, [near_counts[i] for i in range(len(offsets))])
    arrived(line_b, 2)
    totals = plane_total + jnp.sum(line_b[...], axis=0)
    expected = held * totals * (1.0 / cells_all)
    ratio = (expected + 1.0) / (full_counts + 1.0)
    factor = ratio * ratio
    f1 = factor.astype(bf16).astype(f32)
    f2 = (factor - f1).astype(bf16).astype(f32)
    f3 = factor - f1 - f2
    factor = jnp.concatenate([f1, f2, f3, jnp.zeros_like(f3)], axis=0).T.astype(bf16)

    mask = inside(0, cells, 4).astype(bf16)
    weighed = ex[...] * plain(factor, mask)
    a1, a2 = two_pieces(weighed * (1.0 / jnp.sum(weighed, axis=0, keepdims=True)))
    both = jnp.concatenate([a1, a2], axis=0)
    pair[...] = both
    total = across(mask[0 : 2 * SLOTS], both)
    mass = total[0:SLOTS, 0:clusters] + total[0:SLOTS, clusters : 2 * clusters]
    greeted_rows(1, mass)
    around = 2 * wide + 1
    for h in range(1, wide + 1):
        push(near_out.at[1], near_mass.at[(around - 1 - h) % around], 3, neighbour(h))
        push(near_out.at[1], near_mass.at[(around - 1 + h) % around], 3, neighbour(-h))
    near_mass[around - 1] = near_out[1]

    for c in range(runs):
        columns = slice(c * width, (c + 1) * width)
        value = across(lined[:, columns], pair[:, columns])
        for j in range(CLOSE):
            top = value[2 * ROWS * j : 2 * ROWS * j + ROWS]
            low = value[2 * ROWS * j + ROWS : 2 * ROWS * (j + 1)]
            pieces[c, j] = (
                top[:, 0:clusters] + top[:, clusters:] + low[:, 0:clusters] + low[:, clusters:]
            )
    places = [(c, j) for c in range(runs) for j in range(CLOSE)]
    tail_slot = last[0] - first[0]
    alone = jnp.where(tail_slot > 0, 1.0, 0.0)
    shrink = jnp.where(head | tail, 0.0, ridge / (mass + ridge))
    first_moment = jnp.zeros((ROWS, clusters), f32)
    tail_moment = jnp.zeros((ROWS, clusters), f32)
    whole = jnp.zeros((ROWS, clusters), f32)
    right = jnp.zeros((ROWS, clusters), f32)
    for c in range(runs):
        base = base_of(c)
        for j in range(CLOSE):
            piece = pieces[c, j]
            line = jnp.sum(jnp.where(slot == base + j, shrink, 0.0), axis=0, keepdims=True)
            right = right + line * piece
            tail_moment = tail_moment + jnp.where(base + j == tail_slot, 1.0, 0.0) * piece
            whole = whole + piece
            if j == 0:
                first_moment = first_moment + jnp.where(base == 0, 1.0, 0.0) * piece
    for t in range(near):
        inner = slice(t * rows_each, (t + 1) * rows_each)
        sums_out[t, 0] = right[inner]
        sums_out[t, 1] = first_moment[inner]
        sums_out[t, 2] = tail_moment[inner] * alone
        cent_out[t] = whole[inner]
    for r in range(1, near):
        push(sums_out.at[lax.rem(rank + r, near)], sum_in.at[r - 1], 5, mate(r))
    for r in range(1, near):
        push(cent_out.at[lax.rem(rank + r, near)], cent_in.at[r - 1], 4, mate(r))
    ends_out[0] = first_moment[0:56]
    ends_out[1] = tail_moment[0:56]
    arrived(near_mass.at[pl.ds(0, around - 1)], 3)
    full_mass = completed(
        mass, {i: near_mass[(around - 1 + h) % around] for i, h in enumerate(offsets)}
    )
    end_mass = jnp.zeros((16, clusters), f32)
    for p in range(-reach, near + reach):
        both = near_mass[lax.rem(p + (2 * around - 1) - rank, around)]
        one, two = ids[p + reach : p + reach + 1], ids[16 + p + reach : 17 + p + reach]
        end_mass = end_mass + jnp.where(own_ids == one, both[0:1], 0.0)
        end_mass = end_mass + jnp.where((own_ids == two) & (two != one), both[1:2], 0.0)
    end_shrink = own_ridge / (end_mass + own_ridge)
    for t in range(near):
        shrinks[t, 0:1, :] = end_shrink[t : t + 1]
        shrinks[t, 1:2, :] = end_shrink[8 + t : 9 + t]
    arrived(sum_in, 5)
    sum_tile = jnp.zeros((rows_each, clusters), f32)
    for r in range(near):
        by = shrinks[lax.rem(rank + near - r, near)]
        got = sums_out[rank] if r == 0 else sum_in[r - 1]
        sum_tile = sum_tile + got[0] + got[1] * by[0:1] + got[2] * by[1:2]
    tile_out[2] = sum_tile
    for r in range(1, far):
        push(tile_out.at[2], tile_in.at[r - 1], 8, peer(r))
    for i, h in enumerate(offsets):
        push(ends_out.at[int(h > 0)], near_moments.at[len(offsets) - 1 - i], 6, neighbour(h))
    arrived(cent_in, 4)
    cent_tile = cent_out[rank]
    for r in range(near - 1):
        cent_tile = cent_tile + cent_in[r]
    owned = clusters // far
    spread = jnp.concatenate(
        [jnp.broadcast_to(cent_tile[d : d + 1], (owned, clusters)) for d in range(rows_each)],
        axis=0,
    )
    row_at = lax.broadcasted_iota(jnp.int32, spread.shape, 0)
    lane_at = lax.broadcasted_iota(jnp.int32, spread.shape, 1)
    spread = jnp.where(lax.rem(lane_at, owned) == lax.rem(row_at, owned), spread, 0.0)
    spread = jnp.concatenate(
        [spread, jnp.zeros((clusters - spread.shape[0], clusters), f32)], axis=0
    )
    taken = lax.div(lax.broadcasted_iota(jnp.int32, (far, clusters), 1), owned)
    taken = taken == lax.broadcasted_iota(jnp.int32, (far, clusters), 0)
    by_block = lax.dot_general(
        taken.astype(f32),
        spread,
        (((1,), (1,)), ((), ())),
        precision=highest,
        preferred_element_type=f32,
    )
    for t in range(far):
        cent_rows[t] = by_block[t : t + 1]
    for r in range(1, far):
        push(cent_rows.at[lax.rem(block + r, far)], cent_far.at[r - 1], 7, peer(r))
    moments = []
    for s in range(SLOTS):
        moment = jnp.zeros((ROWS, clusters), f32)
        for c, j in places:
            if j <= s <= CLOSE * c + j:
                moment = moment + jnp.where(base_of(c) + j == s, 1.0, 0.0) * pieces[c, j]
        moments.append(moment)

    arrived(cent_far, 7)
    cent_full[0] = cent_rows[block] + jnp.sum(cent_far[...], axis=0)
    for r in range(1, near):
        push(cent_full.at[0], cent_full.at[r], 9, mate(r))
    arrived(tile_in, 8)
    full_sums[1, 0] = sum_tile + jnp.sum(tile_in[...], axis=0)
    for r in range(1, near):
        push(full_sums.at[1, 0], full_sums.at[1, r], 10, mate(r))
    arrived(near_moments, 6)
    before = jnp.zeros((56, clusters), f32)
    after = jnp.zeros((56, clusters), f32)
    for i, h in enumerate(offsets):
        if h < 0:
            before = before + behind[h] * near_moments[i]
        else:
            after = after + ahead[h] * near_moments[i]
    for s in range(SLOTS):
        moment = moments[s][0:56] + after * tail[s : s + 1].astype(f32)
        full_moments[s] = moment + before if s == 0 else moment


    def gathered(which):
        return jnp.concatenate(
            [full_sums[which, lax.rem(rank + (near - t), near)] for t in range(near)], axis=0
        )

    arrived(cent_full.at[pl.ds(1, near - 1)], 9)
    rows = jnp.concatenate(
        [cent_full[lax.rem(rank + (near - t), near)] for t in range(near)], axis=0
    )
    from_lane = lax.broadcasted_iota(jnp.int32, (clusters, ROWS), 0)
    to_lane = lax.broadcasted_iota(jnp.int32, (clusters, ROWS), 1)
    tile_at = lax.broadcasted_iota(jnp.int32, (near, ROWS), 0)
    mine = tile_at == lax.div(lax.broadcasted_iota(jnp.int32, (near, ROWS), 1), rows_each)
    core = lax.div(rank, nx)
    each = cent_ref.shape[0]
    for j in range(each):
        picked = from_lane == lax.rem(to_lane, rows_each) * owned + core * each + j
        line = jnp.dot(
            rows, picked.astype(f32), precision=highest, preferred_element_type=f32
        )
        line = jnp.sum(jnp.where(mine, line, 0.0), axis=0, keepdims=True)
        cent_ref[j : j + 1, :] = (line / (1.0 + line[:, pcs : pcs + 1]))[:, 0:pcs]

    arrived(full_sums.at[1, pl.ds(1, near - 1)], 10)
    right = gathered(1)
    intercept = (right / (1.0 + right[pcs : pcs + 1]))[0:56]
    for s in range(SLOTS):
        moment = full_moments[s]
        line = full_mass[s : s + 1]
        slope = (moment - line * intercept) / (line + ridge[s : s + 1])
        c1, c2 = two_pieces(jnp.concatenate([slope, jnp.zeros((8, clusters), f32)], axis=0))
        slopes[ROWS * s : ROWS * (s + 1), :] = jnp.concatenate([c1, c1, c2], axis=1)

    left(line_a, 0)
    left(near_counts, 1)
    left(line_b, 2)
    left(near_mass.at[pl.ds(0, around - 1)], 3)
    left(cent_in, 4)
    left(sum_in, 5)
    left(near_moments, 6)
    left(cent_far, 7)
    left(tile_in, 8)
    left(cent_full.at[pl.ds(1, near - 1)], 9)
    left(full_sums.at[1, pl.ds(1, near - 1)], 10)


def correct_kernel(
    zf, pair, slopes, starts_ref, cent_ref, out_hbm, cent_hbm, held, starts, out_sems
):
    pcs, cells = zf.shape
    clusters = pair.shape[0] // 2
    loads = out_sems.shape[0] - 1
    part = cells // loads
    cent = pltpu.make_async_copy(cent_ref, cent_hbm, out_sems.at[loads])
    cent.start()
    begin = [jnp.max(starts_ref[s : s + 1, :]) for s in range(SLOTS)]
    for s in range(SLOTS):
        starts[s] = begin[s]
    lane = lax.broadcasted_iota(jnp.int32, (1, TILE), 1)

    def slope_of(j):
        return slopes[pl.ds(pl.multiple_of(j * ROWS, ROWS), ROWS), :]

    def slots_of(t):
        base = jnp.int32(0)
        final = jnp.int32(0)
        border = jnp.int32(2 * cells)
        for s in range(1, SLOTS):
            base = base + jnp.where(begin[s] <= t * TILE, 1, 0)
            final = final + jnp.where(begin[s] < (t + 1) * TILE, 1, 0)
            border = jnp.where(begin[s] > t * TILE, jnp.minimum(border, begin[s]), border)
        return base, final, border

    def send_out(i):
        columns = pl.ds(i * part, part)
        return pltpu.make_async_copy(
            held.at[:, columns], out_hbm.at[:, columns], out_sems.at[i]
        )

    beyond = jnp.int32(0)
    for i in range(loads):
        for t in range(i * part // TILE, (i + 1) * part // TILE):
            columns = slice(t * TILE, (t + 1) * TILE)
            base, final, border = slots_of(t)
            beyond = jnp.maximum(beyond, final - base)
            following = jnp.minimum(base + 1, SLOTS - 1)
            both = pair[:, columns]
            both = jnp.concatenate([both, both[0:clusters]], axis=0)
            moved = plain(jnp.concatenate([slope_of(base), slope_of(following)], axis=0), both)
            moved = jnp.where(lane < border - t * TILE, moved[0:ROWS], moved[ROWS:])
            held[:, columns] = zf[:, columns] - moved[0:pcs]
        send_out(i).start()
    for i in range(loads):
        send_out(i).wait()
    cent.wait()

    @pl.when(beyond > 1)
    def _():
        def tile_of(t, carry):
            columns = pl.ds(pl.multiple_of(t * TILE, TILE), TILE)
            base, final, border = slots_of(t)

            def more(j, carry):
                both = pair[:, columns]
                both = jnp.concatenate([both, both[0:clusters]], axis=0)
                other = zf[:, columns] - plain(slope_of(j), both)[0:pcs]
                held[:, columns] = jnp.where(
                    lane >= starts[j] - t * TILE, other, held[:, columns]
                )
                return carry

            lax.fori_loop(base + 2, final + 1, more, 0)
            return carry

        lax.fori_loop(0, cells // TILE, tile_of, 0)
        for i in range(loads):
            send_out(i).start()
        for i in range(loads):
            send_out(i).wait()


def narrow_body(
    shape, latent_coordinates, group_means, entropy_scaling, sample_shrinkage_lambda, sample_population
):
    pcs, cells = latent_coordinates.shape
    clusters = group_means.shape[0]
    batches = sample_population.shape[0]
    nz, ny, nc, nx = shape
    near, far = nc * nx, nz * ny
    rows_each = ROWS // near
    reach = (MOST - 2) // cells + 1
    owned = clusters // (nz * ny * nc)
    vmem = pl.BlockSpec(memory_space=pltpu.VMEM)
    tile = (rows_each, clusters)
    scratch = [
        pltpu.VMEM((pcs, clusters), f32),
        pltpu.VMEM((1, clusters), f32),
        pltpu.VMEM((1, batches), f32),
        pltpu.VMEM((1, batches), jnp.int32),
        pltpu.VMEM((2 * ROWS, cells), bf16),
        pltpu.VMEM((clusters, cells), f32),
        pltpu.VMEM((2 * ROWS * CLOSE, cells), bf16),
        pltpu.VMEM((clusters, clusters), f32),
        pltpu.VMEM((cells // 512, CLOSE, ROWS, clusters), f32),
        pltpu.VMEM((2, 2, clusters), f32),
        pltpu.VMEM((2 * reach, 2, clusters), f32),
        pltpu.VMEM((2 * (near - 1 + reach) + 1, 2, clusters), f32),
        pltpu.VMEM((2 * reach, 56, clusters), f32),
        pltpu.VMEM((2, 56, clusters), f32),
        pltpu.VMEM((SLOTS, 56, clusters), f32),
        pltpu.VMEM((2, 1, clusters), f32),
        pltpu.VMEM((near * ny - 1, 1, clusters), f32),
        pltpu.VMEM((nz - 1, 1, clusters), f32),
        pltpu.VMEM((near, 3, *tile), f32),
        pltpu.VMEM((near - 1, 3, *tile), f32),
        pltpu.VMEM((near, *tile), f32),
        pltpu.VMEM((near - 1, *tile), f32),
        pltpu.VMEM((near, 2, clusters), f32),
        pltpu.VMEM((far, 1, clusters), f32),
        pltpu.VMEM((far - 1, 1, clusters), f32),
        pltpu.VMEM((near, 1, clusters), f32),
        pltpu.VMEM((3, *tile), f32),
        pltpu.VMEM((far - 1, *tile), f32),
        pltpu.VMEM((2, near, *tile), f32),
        pltpu.SemaphoreType.DMA((4,)),
        pltpu.SemaphoreType.DMA((cells // 512,)),
        pltpu.SemaphoreType.DMA((12,)),
        pltpu.SemaphoreType.DMA((12,)),
    ]
    return pl.pallas_call(
        functools.partial(step_kernel, shape, float(cells * near * far)),
        out_shape=(
            pltpu.VMEM((pcs, cells), f32),
            pltpu.VMEM((2 * clusters, cells), bf16),
            pltpu.VMEM((SLOTS * ROWS, 3 * clusters), bf16),
            pltpu.VMEM((SLOTS, 128), jnp.int32),
            pltpu.VMEM((1, 128), jnp.int32),
            pltpu.VMEM((owned, pcs), f32),
        ),
        in_specs=[pl.BlockSpec(memory_space=pl.ANY)] * 5,
        out_specs=(vmem,) * 6,
        scratch_shapes=scratch,
        compiler_params=pltpu.CompilerParams(
            collective_id=0, has_side_effects=True, vmem_limit_bytes=44 * 1024 * 1024
        ),
    )(
        latent_coordinates[None],
        group_means.T,
        entropy_scaling.reshape(1, clusters),
        sample_shrinkage_lambda.reshape(1, batches),
        sample_population.reshape(1, batches),
    )


def corrected_by(kept, pair, slopes, starts, new_centroids):
    pcs, cells = kept.shape
    vmem = pl.BlockSpec(memory_space=pltpu.VMEM)
    anywhere = pl.BlockSpec(memory_space=pl.ANY)
    return pl.pallas_call(
        correct_kernel,
        out_shape=(pltpu.HBM((pcs, cells), f32), pltpu.HBM(new_centroids.shape, f32)),
        in_specs=[vmem] * 5,
        out_specs=(anywhere, anywhere),
        scratch_shapes=[
            pltpu.VMEM((pcs, cells), f32),
            pltpu.SMEM((SLOTS,), jnp.int32),
            pltpu.SemaphoreType.DMA((5,)),
        ],
        compiler_params=pltpu.CompilerParams(vmem_limit_bytes=16 * 1024 * 1024),
    )(
        kept,
        pair,
        slopes,
        starts,
        new_centroids,
    )


def body(
    shape, latent_coordinates, group_means, entropy_scaling, sample_shrinkage_lambda, sample_population
):
    arguments = (
        latent_coordinates,
        group_means,
        entropy_scaling,
        sample_shrinkage_lambda,
        sample_population,
    )
    kept, pair, slopes, starts, flag, new_centroids = narrow_body(shape, *arguments)
    return lax.cond(
        flag[0, 0] == 0,
        lambda: corrected_by(kept, pair, slopes, starts, new_centroids),
        lambda: wide_body(*arguments),
    )


def solution(mesh):
    shape = (mesh.shape["cells"] // 8, 4, 2, mesh.shape["grp"])
    finer = Mesh(mesh.devices.reshape(shape), ("cells_0", "cells_1", "cells_2", "grp"))
    return jax.shard_map(
        functools.partial(body, shape),
        mesh=finer,
        in_specs=(P(None, CELLS_GRP), P(), P(), P(), P()),
        out_specs=(P(None, CELLS_GRP), P(CELLS, None)),
        check_vma=False,
    )
```

```python
import functools

import jax
import jax.numpy as jnp
from jax import lax
from jax.experimental import pallas as pl
from jax.experimental.pallas import tpu as pltpu
from jax.sharding import Mesh
from jax.sharding import PartitionSpec as P

CELLS = ("cells_0", "cells_1", "cells_2")
CELLS_GRP = ("cells_0", "cells_1", "cells_2", "grp")


diversity = 2.0
intercept_ridge = 1.0
highest = lax.Precision.HIGHEST


def split_up(array, dim, size):
    dims = array.shape
    parts = array.reshape(*dims[:dim], size, dims[dim] // size, *dims[dim + 1 :])
    return jnp.moveaxis(parts, dim, 0)


def summed_on_arrival(array, axis, dim):
    size = lax.axis_size(axis)
    parts = lax.all_to_all(split_up(array, dim, size), axis, 0, 0, tiled=True)
    return jnp.sum(parts, axis=0)


def sum_in_two_steps(array, axes, dim):
    far, near = axes
    parts = split_up(array, dim, lax.axis_size(far))
    nearer = summed_on_arrival(parts, near, dim + 1)
    arrived = lax.all_to_all(nearer, far, split_axis=0, concat_axis=0, tiled=True)
    return arrived.sum(axis=0)


def filled_up(lines, size):
    spare = -len(lines) % size
    return jnp.pad(lines, [(0, spare)] + [(0, 0)] * (lines.ndim - 1))


def sent_to_all(array, axis):
    size = lax.axis_size(axis)
    return lax.all_to_all(
        jnp.broadcast_to(array[None], (size, *array.shape)), axis, 0, 0, tiled=True
    )


def joined_along(parts, dim):
    parts = jnp.moveaxis(parts, 0, dim)
    dims = parts.shape
    return parts.reshape(*dims[:dim], dims[dim] * dims[dim + 1], *dims[dim + 2 :])


def gather_axes(array, axes, dim):
    far, near = axes
    leading = sent_to_all(array, far)
    parts = jnp.swapaxes(sent_to_all(leading, near), 0, 1)
    return joined_along(parts.reshape(-1, *array.shape), dim)


def total_of(array, axes):
    lines = array.reshape(-1)
    own = sum_in_two_steps(
        filled_up(lines, lax.axis_size(axes[0]) * lax.axis_size(axes[1])), axes, 0
    )
    whole = gather_axes(own, axes, 0)
    return whole[: len(lines)].reshape(array.shape)


def from_behind(block, axis, distance):
    devices = range(lax.axis_size(axis))
    route = [(i - distance, i) for i in devices if i - distance in devices]
    return lax.ppermute(block, axis, route)


def by_axis(array, axes):
    return functools.reduce(lax.psum, axes, array)


def observation_affinity(latent_coordinates, group_means, entropy_scaling):
    pairwise_dots = jnp.dot(
        group_means, latent_coordinates, precision=highest, preferred_element_type=jnp.float32
    )
    quadratic_lengths = jnp.sum(group_means * group_means, axis=1)
    return (2.0 * pairwise_dots - quadratic_lengths[:, None]) / (2.0 * entropy_scaling[:, None])


def probabilistic_responsibility(group_affinity):
    top = jnp.max(group_affinity, axis=0, keepdims=True)
    raised = jnp.exp(group_affinity - top)
    return raised / jnp.sum(raised, axis=0, keepdims=True)


def batch_parts(moments, ridge):
    mass = moments[:, 0, :]
    sums = moments[:, 1:, :]
    shrink = ridge[None, :] / (mass + ridge[None, :])
    weight = jnp.sum(mass * shrink, axis=1)
    right_side = jnp.sum(sums * shrink[:, None, :], axis=2)
    return (weight, right_side, jnp.sum(mass, axis=1), jnp.sum(sums, axis=2))


def slopes_of(moments, ridge, weight, right_side):
    mass = moments[:, 0, :]
    sums = moments[:, 1:, :]
    intercept = right_side / (intercept_ridge + weight)[:, None]
    return (sums - mass[:, None, :] * intercept[:, :, None]) / (mass + ridge[None, :])[:, None, :]


def wide_body(
    latent_coordinates, group_means, entropy_scaling, sample_shrinkage_lambda, sample_population
):
    local_cells = latent_coordinates.shape[1]
    num_pcs = latent_coordinates.shape[0]
    clusters = group_means.shape[0]
    batches = sample_population.shape[0]
    owned = clusters // lax.axis_size(CELLS)
    offset = (lax.axis_index(CELLS) * lax.axis_size("grp") + lax.axis_index("grp")) * local_cells
    batch_ends = jnp.cumsum(sample_population)
    batch_starts = batch_ends - sample_population
    cells_total = jnp.sum(sample_population).astype(jnp.float32)
    position = offset + lax.iota(jnp.int32, local_cells)
    batch_of = jnp.sum((batch_ends[:, None] <= position[None, :]).astype(jnp.int32), axis=0)
    first_batch = batch_of[0]
    last_batch = batch_of[local_cells - 1]
    group_affinity = observation_affinity(latent_coordinates, group_means, entropy_scaling)
    expected_occupancy = probabilistic_responsibility(group_affinity)

    def count_step(batch_id, running):
        in_batch = (batch_of == batch_id).astype(jnp.float32)
        single_observation = jnp.dot(
            expected_occupancy, in_batch, precision=highest, preferred_element_type=jnp.float32
        )
        return lax.dynamic_update_slice(
            running, single_observation[:, None], (jnp.int32(0), batch_id)
        )

    counts = lax.fori_loop(
        first_batch, last_batch + 1, count_step, jnp.zeros((clusters, batches), jnp.float32)
    )
    counts = total_of(counts, (("cells_0", "cells_1"), ("cells_2", "grp")))
    totals = jnp.sum(counts, axis=1)
    expected = sample_population.astype(jnp.float32)[None, :] * totals[:, None] / cells_total
    penalty = diversity * jnp.log((counts + 1.0) / (expected + 1.0))

    def penalty_step(batch_id, running):
        in_batch = (batch_of == batch_id).astype(jnp.float32)
        column = lax.dynamic_index_in_dim(penalty, batch_id, 1, keepdims=True)
        return running + column * in_batch[None, :]

    cell_penalty = lax.fori_loop(
        first_batch, last_batch + 1, penalty_step, jnp.zeros((clusters, local_cells), jnp.float32)
    )
    assign = probabilistic_responsibility(group_affinity - cell_penalty)
    augmented = jnp.concatenate(
        [jnp.ones((1, local_cells), jnp.float32), latent_coordinates], axis=0
    )

    def moment_step(batch_id, running):
        in_batch = (batch_of == batch_id).astype(jnp.float32)
        contiguous_portion = jnp.einsum(
            "kn,dn->kd", assign * in_batch[None, :], augmented, precision=highest
        )
        return lax.dynamic_update_slice(
            running, contiguous_portion[:, :, None], (jnp.int32(0), jnp.int32(0), batch_id)
        )

    moments = lax.fori_loop(
        first_batch,
        last_batch + 1,
        moment_step,
        jnp.zeros((clusters, num_pcs + 1, batches), jnp.float32),
    )
    devices_flat = lax.axis_size(CELLS) * lax.axis_size("grp")
    most_cells = 2 * local_cells * devices_flat // batches
    reach = (most_cells - 2) // local_cells + 1
    begins_here = (batch_starts >= offset) & (batch_starts < offset + local_cells)
    owner_mask = begins_here.astype(jnp.float32)
    head_owned = begins_here[first_batch]
    head_column = lax.dynamic_index_in_dim(moments, first_batch, 2, keepdims=False)
    sent_stats = jnp.where(head_owned, 0.0, 1.0) * head_column
    sent_tag = jnp.where(head_owned, 0.0, first_batch.astype(jnp.float32) + 1.0) * jnp.ones(
        (1,), jnp.float32
    )
    completed = moments
    for hop in range(1, reach + 1):
        got_stats, got_tag = from_behind((sent_stats, sent_tag), CELLS_GRP, -hop)
        got_id = jnp.maximum(got_tag[0].astype(jnp.int32) - 1, 0)
        accept = jnp.where((got_tag[0] > 0.5) & begins_here[got_id], 1.0, 0.0)
        single_observation = (
            lax.dynamic_index_in_dim(completed, got_id, 2, keepdims=False) + accept * got_stats
        )
        completed = lax.dynamic_update_slice(
            completed, single_observation[:, :, None], (jnp.int32(0), jnp.int32(0), got_id)
        )
    completed = completed * owner_mask[None, None, :]
    weight, right_side, mass_total, moment_total = jax.tree.map(
        lambda part: by_axis(part, CELLS_GRP), batch_parts(completed, sample_shrinkage_lambda)
    )
    coefficients = slopes_of(completed, sample_shrinkage_lambda, weight, right_side)
    every_centroid = moment_total / (1.0 + mass_total)[:, None]
    new_centroids = lax.dynamic_slice_in_dim(
        every_centroid, lax.axis_index(CELLS) * owned, owned, 0
    )
    tail_owned = begins_here[last_batch]
    tail_column = lax.dynamic_index_in_dim(coefficients, last_batch, 2, keepdims=False)
    tail_send = jnp.where(tail_owned, 1.0, 0.0) * tail_column
    tail_tag = jnp.where(tail_owned, last_batch.astype(jnp.float32) + 1.0, 0.0) * jnp.ones(
        (1,), jnp.float32
    )
    head_fix = jnp.zeros_like(tail_column)
    for hop in range(1, reach + 1):
        got_coef, got_tag = from_behind((tail_send, tail_tag), CELLS_GRP, hop)
        match = got_tag[0] == first_batch.astype(jnp.float32) + 1.0
        head_fix = jnp.where(match, got_coef, head_fix)
    own_head = lax.dynamic_index_in_dim(coefficients, first_batch, 2, keepdims=False)
    head_final = jnp.where(head_owned, own_head, head_fix)
    coefficients = lax.dynamic_update_slice(
        coefficients, head_final[:, :, None], (jnp.int32(0), jnp.int32(0), first_batch)
    )

    def correct_step(batch_id, running):
        in_batch = (batch_of == batch_id).astype(jnp.float32)
        slope_table = lax.dynamic_index_in_dim(coefficients, batch_id, 2, keepdims=False)
        moved = jnp.einsum("kd,kn->dn", slope_table, assign * in_batch[None, :], precision=highest)
        return running + moved

    corrected = lax.fori_loop(first_batch, last_batch + 1, correct_step, jnp.zeros_like(latent_coordinates))
    return (latent_coordinates - corrected, new_centroids)


SLOTS = 8
ROWS = 64
MOST = 10485
LOGICAL = pl.DeviceIdType.LOGICAL
TILE = 256
CLOSE = 4
bf16, f32 = jnp.bfloat16, jnp.float32


def wrapped(value, size):
    return value & (size - 1) if size & (size - 1) == 0 else lax.rem(value, size)


def two_pieces(value):
    first = value.astype(bf16)
    return first, (value - first.astype(f32)).astype(bf16)


def across(left, right):
    return lax.dot_general(left, right, (((1,), (1,)), ((), ())), preferred_element_type=f32)


def plain(left, right):
    return jnp.dot(left, right, preferred_element_type=f32)


def step_kernel(
    shape,
    cells_all,
    z_hbm,
    means_hbm,
    soft_hbm,
    ridge_hbm,
    pop_hbm,
    zf,
    pair,
    slopes,
    starts_ref,
    flag_ref,
    cent_ref,
    means_ref,
    soft_ref,
    ridge_ref,
    pop_ref,
    zc,
    ex,
    lined,
    means_wide,
    pieces,
    near_out,
    near_counts,
    near_mass,
    near_moments,
    ends_out,
    full_moments,
    line_out,
    line_a,
    line_b,
    sums_out,
    sum_in,
    cent_out,
    cent_in,
    shrinks,
    cent_rows,
    cent_far,
    cent_full,
    tile_out,
    tile_in,
    full_sums,
    small_sems,
    load_sems,
    send_sems,
    recv_sems,
):
    nz, ny, nc, nx = shape
    near = nc * nx
    far = nz * ny
    count = near * far
    cells = zf.shape[1]
    pcs, clusters = means_ref.shape
    batches = pop_ref.shape[1]
    rows_each = ROWS // near
    width = 512
    reach = (MOST - 2) // cells + 1
    offsets = [h for h in range(-reach, reach + 1) if h]
    me = (
        (lax.axis_index("cells_0") * ny + lax.axis_index("cells_1")) * nc
        + lax.axis_index("cells_2")
    ) * nx + lax.axis_index("grp")
    rank = wrapped(me, near)
    block = lax.div(me, near)

    def mate(r):
        return block * near + wrapped(rank + r, near)

    plane = near * ny
    in_plane = wrapped(me, plane)

    def beside(r):
        return me - in_plane + wrapped(in_plane + r, plane)

    def peer(r):
        return wrapped(block + r, far) * near + rank

    def along_z(r):
        return wrapped(block + r * ny, far) * near + rank

    def neighbour(h):
        return wrapped(me + (h + count), count)

    def push(src, dst, which, q):
        pltpu.make_async_remote_copy(
            src_ref=src,
            dst_ref=dst,
            send_sem=send_sems.at[which],
            recv_sem=recv_sems.at[which],
            device_id=q,
            device_id_type=LOGICAL,
        ).start()

    def arrived(buffer, which):
        pltpu.make_async_copy(buffer, buffer, recv_sems.at[which]).wait()

    def left(buffer, which):
        pltpu.make_async_copy(buffer, buffer, send_sems.at[which]).wait()

    small = [
        pltpu.make_async_copy(src, dst, small_sems.at[i])
        for i, (src, dst) in enumerate(
            (
                (pop_hbm, pop_ref),
                (means_hbm, means_ref),
                (soft_hbm, soft_ref),
                (ridge_hbm, ridge_ref),
            )
        )
    ]
    for copy in small:
        copy.start()
    for i in range(cells // width):
        columns = pl.ds(i * width, width)
        pltpu.make_async_copy(z_hbm.at[0, :, columns], zf.at[:, columns], load_sems.at[i]).start()

    barrier = pltpu.get_barrier_semaphore()
    greeted = [along_z(r) for r in range(1, nz)] + [beside(r) for r in range(1, plane)]
    greeted = greeted + [neighbour(h) for h in offsets]
    for q in greeted:
        pl.semaphore_signal(barrier, inc=1, device_id=q, device_id_type=LOGICAL)

    for copy in small:
        copy.wait()

    means_wide[...] = jnp.zeros_like(means_wide)
    means_wide[0:pcs, :] = means_ref[...]
    g = means_wide[...].T
    square = lax.broadcasted_iota(jnp.int32, (clusters, clusters), 0)
    lane = lax.broadcasted_iota(jnp.int32, (clusters, clusters), 1)
    soft = jnp.sum(jnp.where(square == lane, soft_ref[...], 0.0), axis=1, keepdims=True)
    offset_of = -0.5 * jnp.sum(g * g, axis=1, keepdims=True) / soft
    weights = jnp.where(lane == pcs, offset_of, g / soft)
    w1 = weights.astype(bf16).astype(f32)
    w2 = (weights - w1).astype(bf16).astype(f32)
    o1 = offset_of.astype(bf16).astype(f32)
    o2 = (offset_of - o1).astype(bf16).astype(f32)
    w1 = jnp.where(lane == pcs + 1, offset_of - o1 - o2, w1)
    w1 = (w1 + pltpu.roll(w1, ROWS, 1)).astype(bf16)
    w2 = (w2 + pltpu.roll(w2, ROWS, 1)).astype(bf16)
    weights = jnp.concatenate([w1, w2], axis=1)

    pop = pop_ref[...]
    up = lax.broadcasted_iota(jnp.int32, (batches, batches), 0)
    down = lax.broadcasted_iota(jnp.int32, (batches, batches), 1)
    column = jnp.sum(jnp.where(up == down, pop, 0), axis=1, keepdims=True)
    ends = jnp.sum(jnp.where(up <= down, column, 0), axis=0, keepdims=True)
    half = lax.broadcasted_iota(jnp.int32, (16, 1), 0)
    device = me + lax.rem(half, 8) - reach
    limit = device * cells + jnp.where(half >= 8, cells - 1, 0)
    spot = jnp.sum(jnp.where(ends <= limit, 1, 0), axis=1, keepdims=True)
    spot = jnp.where(device < 0, -9, spot)
    first = {h: spot[h + reach : h + reach + 1] for h in offsets + [0]}
    last = {h: spot[8 + h + reach : 9 + h + reach] for h in offsets + [0]}
    slot = lax.broadcasted_iota(jnp.int32, (SLOTS, 1), 0)
    batch_id = first[0] + slot
    batch_lane = lax.broadcasted_iota(jnp.int32, (SLOTS, batches), 1)
    chosen = batch_lane == batch_id
    held = jnp.sum(jnp.where(chosen, pop, 0), axis=1, keepdims=True)
    ridge = jnp.sum(jnp.where(chosen, ridge_ref[...], 0.0), axis=1, keepdims=True)
    ridge = jnp.where(batch_id < batches, ridge, 1.0)
    stop = jnp.sum(jnp.where(batch_lane <= batch_id, pop, 0), axis=1, keepdims=True) - me * cells
    start = stop - held
    held = held.astype(f32)
    starts_ref[...] = jnp.broadcast_to(jnp.where(batch_id < batches, start, 2 * cells), (SLOTS, 128))
    tail = slot == last[0] - first[0]
    head = slot == 0
    behind = {h: (last[h] == first[0]).astype(f32) for h in offsets if h < 0}
    ahead = {h: (first[h] == last[0]).astype(f32) for h in offsets if h > 0}

    wide = near - 1 + reach
    row32 = lax.broadcasted_iota(jnp.int32, (32, 1), 0)
    device = block * near + lax.rem(row32, 16) - reach
    limit = device * cells + jnp.where(row32 >= 16, cells - 1, 0)
    ids = jnp.sum(jnp.where(ends <= limit, 1, 0), axis=1, keepdims=True)
    ids = jnp.where(device < 0, -9, ids)
    limit = (block * near + lax.rem(half, 8)) * cells + jnp.where(half >= 8, cells - 1, 0)
    own_ids = jnp.sum(jnp.where(ends <= limit, 1, 0), axis=1, keepdims=True)
    own_lane = lax.broadcasted_iota(jnp.int32, (16, batches), 1)
    own_ridge = jnp.sum(jnp.where(own_lane == own_ids, ridge_ref[...], 0.0), axis=1, keepdims=True)

    crowded = jnp.zeros((1, 1), jnp.int32)
    for inner, room in ((SLOTS - 1, cells), (CLOSE - 1, width)):
        window = jnp.sum(
            jnp.where((up >= down) & (up < down + inner), column, 0), axis=0, keepdims=True
        )
        window = jnp.where((window < room - 1) & (batch_lane[0:1] <= batches - inner), 1, 0)
        crowded = crowded + jnp.sum(window, axis=1, keepdims=True)
    flag_ref[...] = jnp.broadcast_to(crowded, (1, 128))

    def inside(c, width, times):
        position = lax.broadcasted_iota(jnp.int32, (SLOTS * times, width), 1) + c * width
        low = jnp.concatenate([start] * times, axis=0)
        high = jnp.concatenate([stop] * times, axis=0)
        return ((position >= low) & (position < high)).astype(f32)

    def completed(own, buffer):
        before = jnp.zeros((1, clusters), f32)
        after = jnp.zeros((1, clusters), f32)
        for i, h in enumerate(offsets):
            if h < 0:
                before = before + behind[h] * buffer[i][1:2]
            else:
                after = after + ahead[h] * buffer[i][0:1]
        return own + jnp.where(head, before, 0.0) + jnp.where(tail, after, 0.0)

    def tail_of(value):
        return jnp.sum(jnp.where(tail, value, 0.0), axis=0, keepdims=True)

    def greeted_rows(which, value):
        near_out[which, 0:1, :] = value[0:1]
        near_out[which, 1:2, :] = tail_of(value)

    runs = cells // width

    def base_of(c):
        return jnp.sum(
            jnp.where((start <= c * width) & (slot > 0) & (batch_id < batches), 1, 0),
            axis=0,
            keepdims=True,
        )


    for i in range(runs):
        columns = pl.ds(i * width, width)
        pltpu.make_async_copy(z_hbm.at[0, :, columns], zf.at[:, columns], load_sems.at[i]).wait()
    z1, z2 = two_pieces(
        jnp.concatenate(
            [
                zf[...],
                jnp.ones((2, cells), f32),
                jnp.zeros((ROWS - 2 - pcs, cells), f32),
            ],
            axis=0,
        )
    )
    zc[0:ROWS, :] = z1
    zc[ROWS : 2 * ROWS, :] = z2
    score = plain(weights, jnp.concatenate([z1, z2, z1, z2], axis=0))
    raised = jnp.exp(score - jnp.max(score, axis=0, keepdims=True))
    ex[...] = raised
    p1, p2 = two_pieces(raised * (1.0 / jnp.sum(raised, axis=0, keepdims=True)))
    mask = inside(0, cells, 2).astype(bf16)
    total = across(mask, jnp.concatenate([p1, p2], axis=0))
    counts = total[0:SLOTS, 0:clusters] + total[0:SLOTS, clusters : 2 * clusters]
    own_total = jnp.sum(counts, axis=0, keepdims=True)
    greeted_rows(0, counts)
    line_out[0] = own_total
    pl.semaphore_wait(barrier, len(greeted))
    for r in range(1, plane):
        push(line_out.at[0], line_a.at[r - 1], 0, beside(r))
    for i, h in enumerate(offsets):
        push(near_out.at[0], near_counts.at[len(offsets) - 1 - i], 1, neighbour(h))

    def line_up(c):
        columns = slice(c * width, (c + 1) * width)
        mask = inside(c, width, 1)
        kind = jnp.sum(mask * slot.astype(f32), axis=0, keepdims=True)
        kind = kind - base_of(c).astype(f32)
        z = zc[:, columns]
        for j in range(CLOSE):
            lined[2 * ROWS * j : 2 * ROWS * (j + 1), columns] = z * (kind == j).astype(
                f32
            ).astype(bf16)

    for c in range(runs // 2):
        line_up(c)
    arrived(line_a, 0)
    plane_total = own_total + jnp.sum(line_a[...], axis=0)
    line_out[1] = plane_total
    for r in range(1, nz):
        push(line_out.at[1], line_b.at[r - 1], 2, along_z(r))
    for c in range(runs // 2, runs):
        line_up(c)
    arrived(near_counts, 1)
    full_counts = completed(counts, [near_counts[i] for i in range(len(offsets))])
    arrived(line_b, 2)
    totals = plane_total + jnp.sum(line_b[...], axis=0)
    expected = held * totals * (1.0 / cells_all)
    ratio = (expected + 1.0) / (full_counts + 1.0)
    factor = ratio * ratio
    f1 = factor.astype(bf16).astype(f32)
    f2 = (factor - f1).astype(bf16).astype(f32)
    f3 = factor - f1 - f2
    factor = jnp.concatenate([f1, f2, f3, jnp.zeros_like(f3)], axis=0).T.astype(bf16)

    mask = inside(0, cells, 4).astype(bf16)
    weighed = ex[...] * plain(factor, mask)
    a1, a2 = two_pieces(weighed * (1.0 / jnp.sum(weighed, axis=0, keepdims=True)))
    both = jnp.concatenate([a1, a2], axis=0)
    pair[...] = both
    total = across(mask[0 : 2 * SLOTS], both)
    mass = total[0:SLOTS, 0:clusters] + total[0:SLOTS, clusters : 2 * clusters]
    greeted_rows(1, mass)
    around = 2 * wide + 1
    for h in range(1, wide + 1):
        push(near_out.at[1], near_mass.at[(around - 1 - h) % around], 3, neighbour(h))
        push(near_out.at[1], near_mass.at[(around - 1 + h) % around], 3, neighbour(-h))
    near_mass[around - 1] = near_out[1]

    for c in range(runs):
        columns = slice(c * width, (c + 1) * width)
        value = across(lined[:, columns], pair[:, columns])
        for j in range(CLOSE):
            top = value[2 * ROWS * j : 2 * ROWS * j + ROWS]
            low = value[2 * ROWS * j + ROWS : 2 * ROWS * (j + 1)]
            pieces[c, j] = (
                top[:, 0:clusters] + top[:, clusters:] + low[:, 0:clusters] + low[:, clusters:]
            )
    places = [(c, j) for c in range(runs) for j in range(CLOSE)]
    tail_slot = last[0] - first[0]
    alone = jnp.where(tail_slot > 0, 1.0, 0.0)
    shrink = jnp.where(head | tail, 0.0, ridge / (mass + ridge))
    first_moment = jnp.zeros((ROWS, clusters), f32)
    tail_moment = jnp.zeros((ROWS, clusters), f32)
    whole = jnp.zeros((ROWS, clusters), f32)
    right = jnp.zeros((ROWS, clusters), f32)
    for c in range(runs):
        base = base_of(c)
        for j in range(CLOSE):
            piece = pieces[c, j]
            line = jnp.sum(jnp.where(slot == base + j, shrink, 0.0), axis=0, keepdims=True)
            right = right + line * piece
            tail_moment = tail_moment + jnp.where(base + j == tail_slot, 1.0, 0.0) * piece
            whole = whole + piece
            if j == 0:
                first_moment = first_moment + jnp.where(base == 0, 1.0, 0.0) * piece
    for t in range(near):
        inner = slice(t * rows_each, (t + 1) * rows_each)
        sums_out[t, 0] = right[inner]
        sums_out[t, 1] = first_moment[inner]
        sums_out[t, 2] = tail_moment[inner] * alone
        cent_out[t] = whole[inner]
    for r in range(1, near):
        push(sums_out.at[wrapped(rank + r, near)], sum_in.at[r - 1], 5, mate(r))
    for r in range(1, near):
        push(cent_out.at[wrapped(rank + r, near)], cent_in.at[r - 1], 4, mate(r))
    ends_out[0] = first_moment[0:56]
    ends_out[1] = tail_moment[0:56]
    arrived(near_mass.at[pl.ds(0, around - 1)], 3)
    full_mass = completed(
        mass, {i: near_mass[(around - 1 + h) % around] for i, h in enumerate(offsets)}
    )
    end_mass = jnp.zeros((16, clusters), f32)
    for p in range(-reach, near + reach):
        both = near_mass[lax.rem(p + (2 * around - 1) - rank, around)]
        one, two = ids[p + reach : p + reach + 1], ids[16 + p + reach : 17 + p + reach]
        end_mass = end_mass + jnp.where(own_ids == one, both[0:1], 0.0)
        end_mass = end_mass + jnp.where((own_ids == two) & (two != one), both[1:2], 0.0)
    end_shrink = own_ridge / (end_mass + own_ridge)
    for t in range(near):
        shrinks[t, 0:1, :] = end_shrink[t : t + 1]
        shrinks[t, 1:2, :] = end_shrink[8 + t : 9 + t]
    arrived(sum_in, 5)
    sum_tile = jnp.zeros((rows_each, clusters), f32)
    for r in range(near):
        by = shrinks[wrapped(rank + near - r, near)]
        got = sums_out[rank] if r == 0 else sum_in[r - 1]
        sum_tile = sum_tile + got[0] + got[1] * by[0:1] + got[2] * by[1:2]
    tile_out[2] = sum_tile
    for r in range(1, far):
        push(tile_out.at[2], tile_in.at[r - 1], 8, peer(r))
    for i, h in enumerate(offsets):
        push(ends_out.at[int(h > 0)], near_moments.at[len(offsets) - 1 - i], 6, neighbour(h))
    arrived(cent_in, 4)
    cent_tile = cent_out[rank]
    for r in range(near - 1):
        cent_tile = cent_tile + cent_in[r]
    owned = clusters // far
    spread = jnp.concatenate(
        [jnp.broadcast_to(cent_tile[d : d + 1], (owned, clusters)) for d in range(rows_each)],
        axis=0,
    )
    row_at = lax.broadcasted_iota(jnp.int32, spread.shape, 0)
    lane_at = lax.broadcasted_iota(jnp.int32, spread.shape, 1)
    spread = jnp.where(lax.rem(lane_at, owned) == lax.rem(row_at, owned), spread, 0.0)
    spread = jnp.concatenate(
        [spread, jnp.zeros((clusters - spread.shape[0], clusters), f32)], axis=0
    )
    taken = lax.div(lax.broadcasted_iota(jnp.int32, (far, clusters), 1), owned)
    taken = taken == lax.broadcasted_iota(jnp.int32, (far, clusters), 0)
    by_block = lax.dot_general(
        taken.astype(f32),
        spread,
        (((1,), (1,)), ((), ())),
        precision=highest,
        preferred_element_type=f32,
    )
    for t in range(far):
        cent_rows[t] = by_block[t : t + 1]
    for r in range(1, far):
        push(cent_rows.at[wrapped(block + r, far)], cent_far.at[r - 1], 7, peer(r))
    moments = []
    for s in range(SLOTS):
        moment = jnp.zeros((ROWS, clusters), f32)
        for c, j in places:
            if j <= s <= CLOSE * c + j:
                moment = moment + jnp.where(base_of(c) + j == s, 1.0, 0.0) * pieces[c, j]
        moments.append(moment)

    arrived(cent_far, 7)
    cent_full[0] = cent_rows[block] + jnp.sum(cent_far[...], axis=0)
    for r in range(1, near):
        push(cent_full.at[0], cent_full.at[r], 9, mate(r))
    arrived(tile_in, 8)
    full_sums[1, 0] = sum_tile + jnp.sum(tile_in[...], axis=0)
    for r in range(1, near):
        push(full_sums.at[1, 0], full_sums.at[1, r], 10, mate(r))
    arrived(near_moments, 6)
    before = jnp.zeros((56, clusters), f32)
    after = jnp.zeros((56, clusters), f32)
    for i, h in enumerate(offsets):
        if h < 0:
            before = before + behind[h] * near_moments[i]
        else:
            after = after + ahead[h] * near_moments[i]
    for s in range(SLOTS):
        moment = moments[s][0:56] + after * tail[s : s + 1].astype(f32)
        full_moments[s] = moment + before if s == 0 else moment


    def gathered(which):
        return jnp.concatenate(
            [full_sums[which, wrapped(rank + (near - t), near)] for t in range(near)], axis=0
        )

    arrived(cent_full.at[pl.ds(1, near - 1)], 9)
    rows = jnp.concatenate(
        [cent_full[wrapped(rank + (near - t), near)] for t in range(near)], axis=0
    )
    from_lane = lax.broadcasted_iota(jnp.int32, (clusters, ROWS), 0)
    to_lane = lax.broadcasted_iota(jnp.int32, (clusters, ROWS), 1)
    tile_at = lax.broadcasted_iota(jnp.int32, (near, ROWS), 0)
    mine = tile_at == lax.div(lax.broadcasted_iota(jnp.int32, (near, ROWS), 1), rows_each)
    core = lax.div(rank, nx)
    each = cent_ref.shape[0]
    for j in range(each):
        picked = from_lane == lax.rem(to_lane, rows_each) * owned + core * each + j
        line = jnp.dot(
            rows, picked.astype(f32), precision=highest, preferred_element_type=f32
        )
        line = jnp.sum(jnp.where(mine, line, 0.0), axis=0, keepdims=True)
        cent_ref[j : j + 1, :] = (line / (1.0 + line[:, pcs : pcs + 1]))[:, 0:pcs]

    arrived(full_sums.at[1, pl.ds(1, near - 1)], 10)
    right = gathered(1)
    intercept = (right / (1.0 + right[pcs : pcs + 1]))[0:56]
    for s in range(SLOTS):
        moment = full_moments[s]
        line = full_mass[s : s + 1]
        slope = (moment - line * intercept) / (line + ridge[s : s + 1])
        c1, c2 = two_pieces(jnp.concatenate([slope, jnp.zeros((8, clusters), f32)], axis=0))
        slopes[ROWS * s : ROWS * (s + 1), :] = jnp.concatenate([c1, c1, c2], axis=1)

    left(line_a, 0)
    left(near_counts, 1)
    left(line_b, 2)
    left(near_mass.at[pl.ds(0, around - 1)], 3)
    left(cent_in, 4)
    left(sum_in, 5)
    left(near_moments, 6)
    left(cent_far, 7)
    left(tile_in, 8)
    left(cent_full.at[pl.ds(1, near - 1)], 9)
    left(full_sums.at[1, pl.ds(1, near - 1)], 10)


def correct_kernel(
    zf, pair, slopes, starts_ref, cent_ref, out_hbm, cent_hbm, held, starts, out_sems
):
    pcs, cells = zf.shape
    clusters = pair.shape[0] // 2
    loads = out_sems.shape[0] - 1
    part = cells // loads
    cent = pltpu.make_async_copy(cent_ref, cent_hbm, out_sems.at[loads])
    cent.start()
    begin = [jnp.max(starts_ref[s : s + 1, :]) for s in range(SLOTS)]
    for s in range(SLOTS):
        starts[s] = begin[s]
    lane = lax.broadcasted_iota(jnp.int32, (1, TILE), 1)

    def slope_of(j):
        return slopes[pl.ds(pl.multiple_of(j * ROWS, ROWS), ROWS), :]

    def slots_of(t):
        base = jnp.int32(0)
        final = jnp.int32(0)
        border = jnp.int32(2 * cells)
        for s in range(1, SLOTS):
            base = base + jnp.where(begin[s] <= t * TILE, 1, 0)
            final = final + jnp.where(begin[s] < (t + 1) * TILE, 1, 0)
            border = jnp.where(begin[s] > t * TILE, jnp.minimum(border, begin[s]), border)
        return base, final, border

    def send_out(i):
        columns = pl.ds(i * part, part)
        return pltpu.make_async_copy(
            held.at[:, columns], out_hbm.at[:, columns], out_sems.at[i]
        )

    beyond = jnp.int32(0)
    for i in range(loads):
        for t in range(i * part // TILE, (i + 1) * part // TILE):
            columns = slice(t * TILE, (t + 1) * TILE)
            base, final, border = slots_of(t)
            beyond = jnp.maximum(beyond, final - base)
            following = jnp.minimum(base + 1, SLOTS - 1)
            both = pair[:, columns]
            both = jnp.concatenate([both, both[0:clusters]], axis=0)
            moved = plain(jnp.concatenate([slope_of(base), slope_of(following)], axis=0), both)
            moved = jnp.where(lane < border - t * TILE, moved[0:ROWS], moved[ROWS:])
            held[:, columns] = zf[:, columns] - moved[0:pcs]
        send_out(i).start()
    for i in range(loads):
        send_out(i).wait()
    cent.wait()

    @pl.when(beyond > 1)
    def _():
        def tile_of(t, carry):
            columns = pl.ds(pl.multiple_of(t * TILE, TILE), TILE)
            base, final, border = slots_of(t)

            def more(j, carry):
                both = pair[:, columns]
                both = jnp.concatenate([both, both[0:clusters]], axis=0)
                other = zf[:, columns] - plain(slope_of(j), both)[0:pcs]
                held[:, columns] = jnp.where(
                    lane >= starts[j] - t * TILE, other, held[:, columns]
                )
                return carry

            lax.fori_loop(base + 2, final + 1, more, 0)
            return carry

        lax.fori_loop(0, cells // TILE, tile_of, 0)
        for i in range(loads):
            send_out(i).start()
        for i in range(loads):
            send_out(i).wait()


def narrow_body(
    shape, latent_coordinates, group_means, entropy_scaling, sample_shrinkage_lambda, sample_population
):
    pcs, cells = latent_coordinates.shape
    clusters = group_means.shape[0]
    batches = sample_population.shape[0]
    nz, ny, nc, nx = shape
    near, far = nc * nx, nz * ny
    rows_each = ROWS // near
    reach = (MOST - 2) // cells + 1
    owned = clusters // (nz * ny * nc)
    vmem = pl.BlockSpec(memory_space=pltpu.VMEM)
    tile = (rows_each, clusters)
    scratch = [
        pltpu.VMEM((pcs, clusters), f32),
        pltpu.VMEM((1, clusters), f32),
        pltpu.VMEM((1, batches), f32),
        pltpu.VMEM((1, batches), jnp.int32),
        pltpu.VMEM((2 * ROWS, cells), bf16),
        pltpu.VMEM((clusters, cells), f32),
        pltpu.VMEM((2 * ROWS * CLOSE, cells), bf16),
        pltpu.VMEM((clusters, clusters), f32),
        pltpu.VMEM((cells // 512, CLOSE, ROWS, clusters), f32),
        pltpu.VMEM((2, 2, clusters), f32),
        pltpu.VMEM((2 * reach, 2, clusters), f32),
        pltpu.VMEM((2 * (near - 1 + reach) + 1, 2, clusters), f32),
        pltpu.VMEM((2 * reach, 56, clusters), f32),
        pltpu.VMEM((2, 56, clusters), f32),
        pltpu.VMEM((SLOTS, 56, clusters), f32),
        pltpu.VMEM((2, 1, clusters), f32),
        pltpu.VMEM((near * ny - 1, 1, clusters), f32),
        pltpu.VMEM((nz - 1, 1, clusters), f32),
        pltpu.VMEM((near, 3, *tile), f32),
        pltpu.VMEM((near - 1, 3, *tile), f32),
        pltpu.VMEM((near, *tile), f32),
        pltpu.VMEM((near - 1, *tile), f32),
        pltpu.VMEM((near, 2, clusters), f32),
        pltpu.VMEM((far, 1, clusters), f32),
        pltpu.VMEM((far - 1, 1, clusters), f32),
        pltpu.VMEM((near, 1, clusters), f32),
        pltpu.VMEM((3, *tile), f32),
        pltpu.VMEM((far - 1, *tile), f32),
        pltpu.VMEM((2, near, *tile), f32),
        pltpu.SemaphoreType.DMA((4,)),
        pltpu.SemaphoreType.DMA((cells // 512,)),
        pltpu.SemaphoreType.DMA((12,)),
        pltpu.SemaphoreType.DMA((12,)),
    ]
    return pl.pallas_call(
        functools.partial(step_kernel, shape, float(cells * near * far)),
        out_shape=(
            pltpu.VMEM((pcs, cells), f32),
            pltpu.VMEM((2 * clusters, cells), bf16),
            pltpu.VMEM((SLOTS * ROWS, 3 * clusters), bf16),
            pltpu.VMEM((SLOTS, 128), jnp.int32),
            pltpu.VMEM((1, 128), jnp.int32),
            pltpu.VMEM((owned, pcs), f32),
        ),
        in_specs=[pl.BlockSpec(memory_space=pl.ANY)] * 5,
        out_specs=(vmem,) * 6,
        scratch_shapes=scratch,
        compiler_params=pltpu.CompilerParams(
            collective_id=0, has_side_effects=True, vmem_limit_bytes=44 * 1024 * 1024
        ),
    )(
        latent_coordinates[None],
        group_means.T,
        entropy_scaling.reshape(1, clusters),
        sample_shrinkage_lambda.reshape(1, batches),
        sample_population.reshape(1, batches),
    )


def corrected_by(kept, pair, slopes, starts, new_centroids):
    pcs, cells = kept.shape
    vmem = pl.BlockSpec(memory_space=pltpu.VMEM)
    anywhere = pl.BlockSpec(memory_space=pl.ANY)
    return pl.pallas_call(
        correct_kernel,
        out_shape=(pltpu.HBM((pcs, cells), f32), pltpu.HBM(new_centroids.shape, f32)),
        in_specs=[vmem] * 5,
        out_specs=(anywhere, anywhere),
        scratch_shapes=[
            pltpu.VMEM((pcs, cells), f32),
            pltpu.SMEM((SLOTS,), jnp.int32),
            pltpu.SemaphoreType.DMA((9,)),
        ],
        compiler_params=pltpu.CompilerParams(vmem_limit_bytes=16 * 1024 * 1024),
    )(
        kept,
        pair,
        slopes,
        starts,
        new_centroids,
    )


def body(
    shape, latent_coordinates, group_means, entropy_scaling, sample_shrinkage_lambda, sample_population
):
    arguments = (
        latent_coordinates,
        group_means,
        entropy_scaling,
        sample_shrinkage_lambda,
        sample_population,
    )
    kept, pair, slopes, starts, flag, new_centroids = narrow_body(shape, *arguments)
    return lax.cond(
        flag[0, 0] == 0,
        lambda: corrected_by(kept, pair, slopes, starts, new_centroids),
        lambda: wide_body(*arguments),
    )


def solution(mesh):
    shape = (mesh.shape["cells"] // 8, 4, 2, mesh.shape["grp"])
    finer = Mesh(mesh.devices.reshape(shape), ("cells_0", "cells_1", "cells_2", "grp"))
    return jax.shard_map(
        functools.partial(body, shape),
        mesh=finer,
        in_specs=(P(None, CELLS_GRP), P(), P(), P(), P()),
        out_specs=(P(None, CELLS_GRP), P(CELLS, None)),
        check_vma=False,
    )
```
